8 devices in a mesh: dp: 1 (over z), ch: 2 (over y), wd: 4 (over x, core).
Axes of the slice: x: 2, y: 2, z: 1, core: 2. Of those that a mesh axis runs over, the one named last changes fastest.
Arguments:
- resid_in: bfloat16 [16384, 2048], P('dp', 'wd')
- seg_pos: int32 [4, 4096], P('dp')
- gain_temporal: bfloat16 [2048], P('wd')
- w_x: bfloat16 [2048, 2560], P('wd', 'ch')
- bias_x: bfloat16 [2560], P('ch')
- w_y: bfloat16 [2048, 2560], P('wd', 'ch')
- bias_y: bfloat16 [2560], P('ch')
- conv_w: bfloat16 [4, 2560], P(None, 'ch')
- conv_bias: bfloat16 [2560], P('ch')
- lam_param: float32 [2560], P('ch')
- rgate_w: bfloat16 [10, 256, 256], P('ch')
- rgate_b: bfloat16 [2560], P('ch')
- igate_w: bfloat16 [10, 256, 256], P('ch')
- igate_b: bfloat16 [2560], P('ch')
- w_o: bfloat16 [2560, 2048], P('ch', 'wd')
- bias_o: bfloat16 [2048], P('wd')
- gain_mlp: bfloat16 [2048], P('wd')
- w_g: bfloat16 [2048, 6144], P('wd', 'ch')
- bias_g: bfloat16 [6144], P('ch')
- w_u: bfloat16 [2048, 6144], P('wd', 'ch')
- bias_u: bfloat16 [6144], P('ch')
- w_d: bfloat16 [6144, 2048], P('ch', 'wd')
- bias_d: bfloat16 [2048], P('wd')
Outputs:
- output: bfloat16 [16384, 2048], P('dp', 'wd')
All inputs are finite; a program needn't handle non-finite values.
Results may differ from the reference program's by a relative error of at most 0.0129377.
Values are sent between devices in bfloat16 or wider.
A program may use at most 1 GiB of HBM per device.

```python
import jax
import jax.numpy as jnp
from jax import lax

D = 2048
D_RNN = 2560
F = 6144
BLOCKS = 10
B = 4
T = 4096
CONV_WIDTH = 4
BLOCK_WIDTH = D_RNN // BLOCKS
EPS = 1e-6


def normal_draw(key, shape, scale):
    return (jax.random.normal(key, shape, jnp.float32) * scale).astype(jnp.bfloat16)


def doc_positions(key):
    cuts = jax.random.randint(key, (B, 4), 0, T)
    steps = jnp.arange(T, dtype=jnp.int32)
    starts = jnp.any(steps[None, :, None] == cuts[:, None, :], axis=2) | (steps == 0)[None, :]
    last_start = lax.cummax(jnp.where(starts, steps[None, :], 0), axis=1)
    return (steps[None, :] - last_start).astype(jnp.int32)


def setup_inputs(seed: int = 0, part: int = 0) -> dict:
    root = jax.random.key(seed)
    part_key = jax.random.fold_in(root, part)
    keys = jax.random.split(root, 24)
    col_ramp = 0.5 + 1.5 * jnp.arange(D, dtype=jnp.float32) / D
    noise = jax.random.normal(jax.random.fold_in(part_key, 0), (B * T, D), jnp.float32)
    decay_target = jax.random.uniform(keys[9], (D_RNN,), jnp.float32, 0.9, 0.999)
    sigma_lam = decay_target ** 0.125
    return {
        'resid_in': (noise * col_ramp).astype(jnp.bfloat16),
        'seg_pos': doc_positions(jax.random.fold_in(part_key, 1)),
        'gain_temporal': normal_draw(keys[0], (D,), 0.5),
        'w_x': normal_draw(keys[1], (D, D_RNN), D ** -0.5),
        'bias_x': normal_draw(keys[2], (D_RNN,), 0.5),
        'w_y': normal_draw(keys[3], (D, D_RNN), D ** -0.5),
        'bias_y': normal_draw(keys[4], (D_RNN,), 0.5),
        'conv_w': normal_draw(keys[5], (CONV_WIDTH, D_RNN), 0.5),
        'conv_bias': normal_draw(keys[6], (D_RNN,), 0.5),
        'lam_param': jnp.log(sigma_lam / (1.0 - sigma_lam)),
        'rgate_w': normal_draw(keys[7], (BLOCKS, BLOCK_WIDTH, BLOCK_WIDTH), BLOCK_WIDTH ** -0.5),
        'rgate_b': normal_draw(keys[8], (D_RNN,), 1.0),
        'igate_w': normal_draw(keys[10], (BLOCKS, BLOCK_WIDTH, BLOCK_WIDTH), BLOCK_WIDTH ** -0.5),
        'igate_b': normal_draw(keys[11], (D_RNN,), 1.0),
        'w_o': normal_draw(keys[12], (D_RNN, D), 1.5 * D_RNN ** -0.5),
        'bias_o': normal_draw(keys[13], (D,), 0.5),
        'gain_mlp': normal_draw(keys[14], (D,), 0.5),
        'w_g': normal_draw(keys[15], (D, F), D ** -0.5),
        'bias_g': normal_draw(keys[16], (F,), 0.5),
        'w_u': normal_draw(keys[17], (D, F), D ** -0.5),
        'bias_u': normal_draw(keys[18], (F,), 0.5),
        'w_d': normal_draw(keys[19], (F, D), 1.5 * F ** -0.5),
        'bias_d': normal_draw(keys[20], (D,), 0.5),
    }


def rms_scale(vals, gain):
    mean_sq = jnp.mean(vals * vals, axis=-1, keepdims=True)
    return (vals * lax.rsqrt(mean_sq + EPS) * (1.0 + gain.astype(jnp.float32))).astype(jnp.bfloat16)


def conv_mix(vals, positions, conv_w, conv_bias):
    vals32 = vals.astype(jnp.float32)
    taps = conv_w.astype(jnp.float32)
    total = conv_bias.astype(jnp.float32) + vals32 * taps[0]
    for shift in range(1, CONV_WIDTH):
        moved = jnp.pad(vals32[:-shift], ((shift, 0), (0, 0)))
        total = total + jnp.where((positions >= shift)[:, None], moved, 0.0) * taps[shift]
    return total.astype(jnp.bfloat16)


def combine(left, right):
    return left[0] * right[0], right[0] * left[1] + right[1]


def rg_lru(conv_out, positions, lam_param, rgate_w, rgate_b, igate_w, igate_b):
    grouped = conv_out.astype(jnp.float32).reshape(T, BLOCKS, BLOCK_WIDTH)
    rate = jax.nn.sigmoid(jnp.einsum('tbi,bij->tbj', grouped, rgate_w.astype(jnp.float32)).reshape(T, D_RNN) + rgate_b.astype(jnp.float32))
    inflow = jax.nn.sigmoid(jnp.einsum('tbi,bij->tbj', grouped, igate_w.astype(jnp.float32)).reshape(T, D_RNN) + igate_b.astype(jnp.float32))
    log_a = -8.0 * rate * jax.nn.softplus(-lam_param.astype(jnp.float32))
    reset = (positions == 0)[:, None]
    decay = jnp.where(reset, 0.0, jnp.exp(log_a))
    scale = jnp.where(reset, 1.0, jnp.sqrt(-jnp.expm1(2.0 * log_a)))
    drive = scale * inflow * conv_out.astype(jnp.float32)
    return lax.associative_scan(combine, (decay, drive), axis=0)[1]


def reference(resid_in, seg_pos, gain_temporal, w_x, bias_x, w_y, bias_y, conv_w, conv_bias, lam_param, rgate_w, rgate_b, igate_w, igate_b, w_o, bias_o, gain_mlp, w_g, bias_g, w_u, bias_u, w_d, bias_d):
    def one_sequence(pair):
        seq_x, positions = pair
        resid32 = seq_x.astype(jnp.float32)
        normed = rms_scale(resid32, gain_temporal)
        y_branch = jax.nn.gelu(jnp.dot(normed, w_y, preferred_element_type=jnp.float32) + bias_y.astype(jnp.float32), approximate=True).astype(jnp.bfloat16)
        u_branch = (jnp.dot(normed, w_x, preferred_element_type=jnp.float32) + bias_x.astype(jnp.float32)).astype(jnp.bfloat16)
        conv_out = conv_mix(u_branch, positions, conv_w, conv_bias)
        hidden = rg_lru(conv_out, positions, lam_param, rgate_w, rgate_b, igate_w, igate_b)
        mixed = (hidden * y_branch.astype(jnp.float32)).astype(jnp.bfloat16)
        resid = resid32 + jnp.dot(mixed, w_o, preferred_element_type=jnp.float32) + bias_o.astype(jnp.float32)
        normed2 = rms_scale(resid, gain_mlp)
        gate = jax.nn.gelu(jnp.dot(normed2, w_g, preferred_element_type=jnp.float32) + bias_g.astype(jnp.float32), approximate=True)
        upper = jnp.dot(normed2, w_u, preferred_element_type=jnp.float32) + bias_u.astype(jnp.float32)
        inner = (gate * upper).astype(jnp.bfloat16)
        return (resid + jnp.dot(inner, w_d, preferred_element_type=jnp.float32) + bias_d.astype(jnp.float32)).astype(jnp.bfloat16)
    per_seq = lax.map(one_sequence, (resid_in.reshape(B, T, D), seg_pos))
    return per_seq.reshape(B * T, D)
```

```python
import functools

import jax
import jax.numpy as jnp
from jax import lax
from jax.experimental import pallas as pl
from jax.experimental.pallas import tpu as pltpu
from jax.sharding import PartitionSpec as P

MESH = pl.DeviceIdType.MESH
F32, BF16 = jnp.float32, jnp.bfloat16
EPS = 1e-6
LANES = 256
CHUNK = 256
ANY = pl.BlockSpec(memory_space=pl.ANY)
VMEM_LIMIT = 62 * 1024 * 1024


def gelu(v):
    return 0.5 * v * (1.0 + jnp.tanh(0.7978845608028654 * (v + 0.044715 * (v * v * v))))


def sigmoid(v):
    return 1.0 / (1.0 + jnp.exp(-v))


def shuffle_matrix(transposed):
    rows = lax.broadcasted_iota(jnp.int32, (CHUNK, CHUNK), 0)
    cols = lax.broadcasted_iota(jnp.int32, (CHUNK, CHUNK), 1)
    out, src = (cols, rows) if transposed else (rows, cols)
    return jnp.where((out % 8) * (CHUNK // 8) + out // 8 == src, 1.0, 0.0).astype(BF16)


def exchange_in(nwd, resid, gates, vch, vmlp, vwd, x_out, g_out, vch_out, vmlp_out, vwd_out,
                xbuf, gbuf, cbuf, fbuf, dbuf, ssem, rsem, lsem):
    ch, wd = lax.axis_index("ch"), lax.axis_index("wd")
    rows, width = xbuf.shape
    copies = []

    def send(src, dst, device, k):
        copies.append(pltpu.make_async_remote_copy(src_ref=src, dst_ref=dst, send_sem=ssem.at[k], recv_sem=rsem.at[k],
                                                   device_id=device, device_id_type=MESH))
        copies[-1].start()

    for p in (2, 1, 3):
        peer = lax.rem(wd + p, nwd)
        send(resid.at[pl.ds((ch * nwd + peer) * rows, rows)], x_out.at[:, pl.ds(wd * width, width)], (0, ch, peer), p - 1)
        send(vwd, vwd_out.at[wd], (0, ch, peer), 2 + p)
    other = (0, 1 - ch, wd)
    send(vch, vch_out.at[ch], other, 6)
    send(vmlp, vmlp_out.at[ch], other, 7)
    send(gates, g_out.at[ch], other, 8)
    own = [(resid.at[pl.ds((ch * nwd + wd) * rows, rows)], xbuf, x_out.at[:, pl.ds(wd * width, width)]),
           (gates, gbuf, g_out.at[ch]), (vch, cbuf, vch_out.at[ch]), (vmlp, fbuf, vmlp_out.at[ch]),
           (vwd, dbuf, vwd_out.at[wd])]
    ins = [pltpu.make_async_copy(s, b, lsem.at[i]) for i, (s, b, _) in enumerate(own)]
    outs = [pltpu.make_async_copy(b, d, lsem.at[len(own) + i]) for i, (_, b, d) in enumerate(own)]
    for c in ins:
        c.start()
    for c, d in zip(ins, outs):
        c.wait()
        d.start()
    for d in outs:
        d.wait()
    for c in copies:
        c.wait()


def exchange_out(nwd, pieces, blk, out, buf, ssem, rsem, fsem, gsem, lsem):
    ch, wd = lax.axis_index("ch"), lax.axis_index("wd")
    rows, width = buf.shape
    part = rows // pieces
    other = (0, 1 - ch, wd)
    direct, onward = {}, {}

    def remote(src, dst, device, s, r):
        return pltpu.make_async_remote_copy(src_ref=src, dst_ref=dst, send_sem=s, recv_sem=r, device_id=device,
                                            device_id_type=MESH)

    base = (ch * nwd + wd) * rows
    for k in range(pieces):
        piece = pl.ds(k * part, part)
        for p in (1, 2, 3):
            peer = lax.rem(wd + p, nwd)
            direct[p, k] = remote(blk.at[piece, pl.ds(peer * width, width)], out.at[pl.ds(base + k * part, part)],
                                  (0, ch, peer), ssem.at[p - 1, k], rsem.at[p - 1, k])
            direct[p, k].start()
        onward[0, k] = remote(blk.at[piece, pl.ds(wd * width, width)], out.at[pl.ds(base + k * part, part)],
                              other, fsem.at[0, k], gsem.at[0, k])
        onward[0, k].start()
    take = pltpu.make_async_copy(blk.at[:, pl.ds(wd * width, width)], buf, lsem.at[0])
    put = pltpu.make_async_copy(buf, out.at[pl.ds(base, rows)], lsem.at[1])
    take.start()
    take.wait()
    put.start()
    for k in range(pieces):
        for p in (1, 2, 3):
            came = lax.rem(wd + nwd - p, nwd)
            direct[p, k].wait_recv()
            here = pl.ds((ch * nwd + came) * rows + k * part, part)
            onward[p, k] = remote(out.at[here], out.at[here], other, fsem.at[p, k], gsem.at[p, k])
            onward[p, k].start()
    put.wait()
    for k in range(pieces):
        for p in (1, 2, 3):
            direct[p, k].wait_send()
    for c in onward.values():
        c.wait()


def temporal(x_ref, pos_ref, wy_ref, wx_ref, gate_ref, wo0_ref, wo1_ref, par_ref, vd_ref, res_out, m_out,
             n_s, acc_s, raw_s, u_s, h_s, prod_s, y_s, tail_s, h0_s, msg_out, msg_in, ssem, rsem, osem):
    j, blocks = pl.program_id(0), pl.num_programs(0)
    ch, wd = lax.axis_index("ch"), lax.axis_index("wd")
    core = lax.rem(wd, 2)
    tokens, model = n_s.shape
    steps = tokens // CHUNK
    groups = CHUNK // 8

    def message(i):
        return pltpu.make_async_remote_copy(src_ref=msg_out.at[i], dst_ref=msg_in.at[i], send_sem=ssem.at[i],
                                            recv_sem=rsem.at[i], device_id=(0, ch, wd + 1 - 2 * core), device_id_type=MESH)

    @pl.when(j == 0)
    def _():
        mix = shuffle_matrix(False)
        gain = 1.0 + vd_ref[0:1, :]
        bias = vd_ref[1:2, :]

        @pl.loop(0, steps)
        def _(c):
            rows = pl.ds(c * CHUNK, CHUNK)
            vals = jnp.dot(mix, x_ref[rows, :], preferred_element_type=F32)
            scale = lax.rsqrt(jnp.mean(vals * vals, axis=1, keepdims=True) + EPS)
            n_s[rows, :] = (vals * scale * gain).astype(BF16)
            acc_s[rows, :] = vals + bias

    def project(q, slot):
        vals = n_s[pl.ds(q * CHUNK, CHUNK), :]
        raw_s[slot, 0] = jnp.dot(vals, wy_ref[0].reshape(model, LANES), preferred_element_type=F32)
        raw_s[slot, 1] = jnp.dot(vals, wx_ref[0].reshape(model, LANES), preferred_element_type=F32)

    def row(i):
        return par_ref[0, i:i + 1, :]

    def recur(q, slot):
        rows = pl.ds(q * CHUNK, CHUNK)
        pos = pos_ref[rows, :]
        pos = jnp.concatenate([pos] * (LANES // pos.shape[1]), axis=1)
        y_s[...] = gelu(raw_s[slot, 0] + row(1)).astype(BF16)
        u = (raw_s[slot, 1] + row(0)).astype(BF16).astype(F32)
        u_s[24:, :] = u
        sub = lax.broadcasted_iota(jnp.int32, (8, LANES), 0)
        last = u[CHUNK - 24:, :]
        for k in range(3):
            edge = jnp.where(sub == 7, tail_s[k * 8:(k + 1) * 8, :], last[k * 8:(k + 1) * 8, :])
            u_s[k * 8:(k + 1) * 8, :] = pltpu.roll(edge, 1, 0)
        tail_s[...] = last
        c = row(2) + u * row(3)
        for k in range(1, 4):
            c = c + jnp.where(pos >= k, u_s[pl.ds(24 - 8 * k, CHUNK), :], 0.0) * row(3 + k)
        c16 = c.astype(BF16)
        pre = jnp.dot(c16, gate_ref[0], preferred_element_type=F32)
        rate = sigmoid(pre[:, :LANES] + row(8))
        inflow = sigmoid(pre[:, LANES:] + row(9))
        log_a = rate * row(7)
        a = jnp.exp(log_a)
        scale = jnp.sqrt(jnp.tanh(-log_a) * (1.0 + a * a))
        reset = pos == 0
        a = jnp.where(reset, 0.0, a)
        scale = jnp.where(reset, 1.0, scale)
        b = scale * inflow * c16.astype(F32)
        h, prod = b[0:8, :], a[0:8, :]
        h_s[0:8, :] = h
        prod_s[0:8, :] = prod
        for t in range(1, groups):
            at = a[t * 8:(t + 1) * 8, :]
            h = at * h + b[t * 8:(t + 1) * 8, :]
            prod = at * prod
            h_s[t * 8:(t + 1) * 8, :] = h
            prod_s[t * 8:(t + 1) * 8, :] = prod
        for k in (1, 2, 4):
            far = sub >= k
            h = jnp.where(far, h + prod * pltpu.roll(h, k, 0), h)
            prod = jnp.where(far, prod * pltpu.roll(prod, k, 0), prod)
        before = h0_s[...]
        ends = h + prod * before
        carry = jnp.where(sub == 0, before, pltpu.roll(ends, 1, 0))
        h0_s[...] = jnp.broadcast_to(ends[7:8, :], (8, LANES))
        hid = h_s[...].reshape(groups, 8, LANES) + prod_s[...].reshape(groups, 8, LANES) * carry[None]
        mixed = (hid.reshape(CHUNK, LANES) * y_s[...].astype(F32)).astype(BF16)
        for k in range(wo0_ref.shape[1]):
            for half, w in enumerate((wo0_ref, wo1_ref)):
                cols = pl.ds((2 * k + half) * LANES, LANES)
                acc_s[rows, cols] += jnp.dot(mixed, w[0, k], preferred_element_type=F32)

    project(0, 0)

    @pl.when(core == 0)
    def _():
        h0_s[...] = jnp.zeros_like(h0_s)
        tail_s[...] = jnp.zeros_like(tail_s)

    @pl.when(core == 1)
    def _():
        message(j).wait_recv()
        tail_s[...] = msg_in[j, 0:24, :]
        h0_s[...] = msg_in[j, 24:32, :]

    @pl.loop(0, steps - 1)
    def _(q):
        slot = lax.rem(q, 2)
        project(q + 1, 1 - slot)
        recur(q, slot)

    recur(steps - 1, (steps - 1) % 2)

    @pl.when(core == 0)
    def _():
        msg_out[j, 0:24, :] = tail_s[...]
        msg_out[j, 24:32, :] = h0_s[...]
        message(j).start()

    @pl.when(j == blocks - 1)
    def _():
        gain = 1.0 + vd_ref[2:3, :]
        bias = vd_ref[3:4, :]

        def put(c):
            rows = pl.ds(c * CHUNK, CHUNK)
            return (pltpu.make_async_copy(acc_s.at[rows], res_out.at[rows], osem.at[0, c]),
                    pltpu.make_async_copy(n_s.at[rows], m_out.at[rows], osem.at[1, c]))

        @pl.loop(0, steps)
        def _(c):
            rows = pl.ds(c * CHUNK, CHUNK)
            vals = acc_s[rows, :]
            scale = lax.rsqrt(jnp.mean(vals * vals, axis=1, keepdims=True) + EPS)
            n_s[rows, :] = (vals * scale * gain).astype(BF16)
            acc_s[rows, :] = vals + bias
            for d in put(c):
                d.start()

        @pl.loop(0, steps)
        def _(c):
            for d in put(c):
                d.wait()

        @pl.when(core == 0)
        def _():
            @pl.loop(0, blocks)
            def _(i):
                message(i).wait_send()


def mlp(final, m_hbm, acc_hbm, wg_ref, wu_ref, wd0_ref, wd1_ref, bias_ref, out, m_s, acc_s, act_s, isem, osem):
    f, tiles = pl.program_id(0), pl.num_programs(0)
    tokens, model = m_s.shape
    rows_up = act_s.shape[1]
    steps = tokens // rows_up

    def rows_of(i):
        return pl.ds(i * rows_up, rows_up)

    def take(i):
        return (pltpu.make_async_copy(m_hbm.at[rows_of(i)], m_s.at[rows_of(i)], isem.at[0, i]),
                pltpu.make_async_copy(acc_hbm.at[rows_of(i)], acc_s.at[rows_of(i)], isem.at[1, i]))

    def give(i):
        src = m_s if final else acc_s
        return pltpu.make_async_copy(src.at[rows_of(i)], out.at[rows_of(i)], osem.at[i])

    @pl.when(f == 0)
    def _():
        for i in range(steps):
            for d in take(i):
                d.start()

    def up(i, slot):
        vals = m_s[rows_of(i), :]
        for b in range(2):
            cols = slice(b * LANES, (b + 1) * LANES)
            part = slice(b * wg_ref.shape[2] // 2, (b + 1) * wg_ref.shape[2] // 2)
            gate = jnp.dot(vals, wg_ref[0, :, part, :].reshape(model, LANES), preferred_element_type=F32)
            upper = jnp.dot(vals, wu_ref[0, :, part, :].reshape(model, LANES), preferred_element_type=F32)
            act_s[slot, :, cols] = (gelu(gate + bias_ref[0, 0:1, cols]) * (upper + bias_ref[0, 1:2, cols])).astype(BF16)

    def down(i, slot):
        vals = act_s[slot]
        for k in range(wd0_ref.shape[1]):
            for half, w in enumerate((wd0_ref, wd1_ref)):
                cols = pl.ds((2 * k + half) * LANES, LANES)
                acc_s[rows_of(i), cols] += jnp.dot(vals, w[0, k], preferred_element_type=F32)

    @pl.when(f == 0)
    def _():
        take(0)[0].wait()

    up(0, 0)

    @pl.loop(1, steps)
    def _(i):
        @pl.when(f == 0)
        def _():
            take(i)[0].wait()
            take(i - 1)[1].wait()

        slot = lax.rem(i, 2)
        up(i, slot)
        down(i - 1, 1 - slot)
        if not final:
            @pl.when(f == tiles - 1)
            def _():
                give(i - 1).start()

    @pl.when(f == 0)
    def _():
        take(steps - 1)[1].wait()

    down(steps - 1, (steps - 1) % 2)

    @pl.when(f == tiles - 1)
    def _():
        if final:
            mix = shuffle_matrix(True)

            @pl.loop(0, steps)
            def _(i):
                for c in range(rows_up // CHUNK):
                    rows = pl.ds(i * rows_up + c * CHUNK, CHUNK)
                    m_s[rows, :] = jnp.dot(mix, acc_s[rows, :].astype(BF16), preferred_element_type=F32).astype(BF16)
                give(i).start()
        else:
            give(steps - 1).start()

        @pl.loop(0, steps)
        def _(i):
            give(i).wait()


def stack_columns(w):
    rows, cols = w.shape
    return [w[:, k * LANES:(k + 1) * LANES] for k in range(cols // LANES)]


def solution(mesh):
    nwd, nch = mesh.shape["wd"], mesh.shape["ch"]
    count = nwd * nch
    row_spec = P("dp", "wd")
    specs = (row_spec, P("dp", None), P("wd"), P("wd", "ch"), P("ch"), P("wd", "ch"), P("ch"), P(None, "ch"), P("ch"), P("ch"), P("ch", None, None), P("ch"), P("ch", None, None), P("ch"), P("ch", "wd"), P("wd"), P("wd"), P("wd", "ch"), P("ch"), P("wd", "ch"), P("ch"), P("ch", "wd"), P("wd"))
    CALLS = 3

    def gather(parts):
        packed = jnp.concatenate(parts, axis=0)
        full = lax.all_gather(packed, ("ch", "wd"))
        return full.reshape(nch, nwd, *packed.shape)

    def local_layer(resid_in, seg_pos, gain_temporal, w_x, bias_x, w_y, bias_y, conv_w, conv_bias, lam_param, rgate_w, rgate_b, igate_w, igate_b, w_o, bias_o, gain_mlp, w_g, bias_g, w_u, bias_u, w_d, bias_d):
        tokens, width = resid_in.shape
        model = width * nwd
        rows = tokens // count
        chan = w_x.shape[1]
        blocks = chan // LANES
        inner = w_g.shape[1]
        ch, wd = lax.axis_index("ch"), lax.axis_index("wd")

        w_in = gather(stack_columns(w_y) + stack_columns(w_x))
        w_back = gather(stack_columns(w_o))
        piece = inner // CALLS
        w_mlp = []
        for c in range(CALLS):
            cut = slice(c * piece, (c + 1) * piece)
            w_mlp.append(gather(stack_columns(w_g[:, cut]) + stack_columns(w_u[:, cut]) + stack_columns(w_d[cut])))

        gates = jnp.concatenate([rgate_w, igate_w], axis=2)
        per_chan = jnp.stack([bias_x, bias_y, conv_bias, *conv_w, -8.0 * jax.nn.softplus(-lam_param), rgate_b, igate_b]).astype(F32)
        per_chan = jnp.pad(per_chan, ((0, 16 - per_chan.shape[0]), (0, 0)))
        vch = per_chan.reshape(16, blocks, LANES).transpose(1, 0, 2)
        vmlp = jnp.pad(jnp.stack([bias_g, bias_u]).astype(F32), ((0, 6), (0, 0)))
        vwd = jnp.pad(jnp.stack([gain_temporal, bias_o, gain_mlp, bias_d]).astype(F32), ((0, 4), (0, 0)))
        x_full, gates_all, vch_all, vmlp_all, vwd_all = pl.pallas_call(
            functools.partial(exchange_in, nwd),
            out_shape=[jax.ShapeDtypeStruct((rows, model), BF16), jax.ShapeDtypeStruct((nch, *gates.shape), BF16),
                       jax.ShapeDtypeStruct((nch, *vch.shape), F32), jax.ShapeDtypeStruct((nch, *vmlp.shape), F32),
                       jax.ShapeDtypeStruct((nwd, *vwd.shape), F32)],
            in_specs=[ANY] * 5, out_specs=[ANY] * 5,
            scratch_shapes=[pltpu.VMEM((rows, width), BF16), pltpu.VMEM(gates.shape, BF16), pltpu.VMEM(vch.shape, F32),
                            pltpu.VMEM(vmlp.shape, F32), pltpu.VMEM(vwd.shape, F32),
                            pltpu.SemaphoreType.DMA((9,)), pltpu.SemaphoreType.DMA((9,)), pltpu.SemaphoreType.DMA((10,))],
            compiler_params=pltpu.CompilerParams(has_side_effects=True),
            cost_estimate=pl.CostEstimate(flops=100_000_000_000, bytes_accessed=16_000_000, transcendentals=0),
            name="exchange_in",
        )(resid_in, gates, vch, vmlp, vwd)
        gates_all = gates_all.reshape(nch * blocks, *gates.shape[1:])
        vch_all = vch_all.reshape(nch * blocks, *vch.shape[1:])
        vd_all = vwd_all.transpose(1, 0, 2).reshape(8, model)
        pos = lax.dynamic_index_in_dim(seg_pos.reshape(count, rows), ch * nwd + wd, 0, keepdims=False)
        pos = pos.reshape(rows // CHUNK, 8, CHUNK // 8).transpose(0, 2, 1).reshape(rows, 1)
        pos = jnp.broadcast_to(pos, (rows, 128))

        total = nch * blocks
        steps = rows // CHUNK

        def full(shape):
            return pl.BlockSpec(shape, lambda j: (0,) * len(shape), pipeline_mode=pl.Buffered(1))

        res, m = pl.pallas_call(
            temporal,
            grid=(total,),
            out_shape=[jax.ShapeDtypeStruct((rows, model), F32), jax.ShapeDtypeStruct((rows, model), BF16)],
            in_specs=[full((rows, model)), full((rows, 128)),
                      pl.BlockSpec((1, nwd, width, LANES), lambda j: (j // blocks, 0, j % blocks, 0)),
                      pl.BlockSpec((1, nwd, width, LANES), lambda j: (j // blocks, 0, blocks + j % blocks, 0)),
                      pl.BlockSpec((1, LANES, 2 * LANES), lambda j: (j, 0, 0)),
                      pl.BlockSpec((1, nwd, LANES, LANES), lambda j: (j // blocks, 0, j % blocks, 0)),
                      pl.BlockSpec((1, nwd, LANES, LANES), lambda j: (j // blocks, 0, blocks + j % blocks, 0)),
                      pl.BlockSpec((1, 16, LANES), lambda j: (j, 0, 0)),
                      full((8, model))],
            out_specs=[ANY, ANY],
            scratch_shapes=[pltpu.VMEM((rows, model), BF16), pltpu.VMEM((rows, model), F32),
                            pltpu.VMEM((2, 2, CHUNK, LANES), F32), pltpu.VMEM((CHUNK + 24, LANES), F32),
                            pltpu.VMEM((CHUNK, LANES), F32), pltpu.VMEM((CHUNK, LANES), F32),
                            pltpu.VMEM((CHUNK, LANES), BF16), pltpu.VMEM((24, LANES), F32), pltpu.VMEM((8, LANES), F32),
                            pltpu.VMEM((total, 32, LANES), F32), pltpu.VMEM((total, 32, LANES), F32),
                            pltpu.SemaphoreType.DMA((total,)), pltpu.SemaphoreType.DMA((total,)),
                            pltpu.SemaphoreType.DMA((2, steps))],
            compiler_params=pltpu.CompilerParams(has_side_effects=True, vmem_limit_bytes=VMEM_LIMIT),
            cost_estimate=pl.CostEstimate(flops=2 * rows * model * 3 * total * LANES * 2, bytes_accessed=70_000_000, transcendentals=0),
            name="temporal",
        )(x_full, pos, w_in, w_in, gates_all, w_back, w_back, vch_all, vd_all)

        tile = 2 * LANES
        per = piece // tile
        rows_up = 512
        acc = res
        for c in range(CALLS):
            final = c == CALLS - 1
            up_rows = 2 * piece // LANES * width
            acc = pl.pallas_call(
                functools.partial(mlp, final),
                grid=(nch * per,),
                out_shape=jax.ShapeDtypeStruct((rows, model), BF16 if final else F32),
                in_specs=[ANY, ANY,
                          pl.BlockSpec((1, nwd, 2 * width, LANES), lambda f: (f // per, 0, f % per, 0)),
                          pl.BlockSpec((1, nwd, 2 * width, LANES), lambda f: (f // per, 0, per + f % per, 0)),
                          pl.BlockSpec((1, nwd, tile, LANES), lambda f: (f // per, 0, up_rows // tile + f % per, 0)),
                          pl.BlockSpec((1, nwd, tile, LANES), lambda f: (f // per, 0, up_rows // tile + per + f % per, 0)),
                          pl.BlockSpec((1, 8, tile), lambda f, c=c: (f // per, 0, c * per + f % per))],
                out_specs=ANY,
                scratch_shapes=[pltpu.VMEM((rows, model), BF16), pltpu.VMEM((rows, model), F32),
                                pltpu.VMEM((2, rows_up, tile), BF16),
                                pltpu.SemaphoreType.DMA((2, rows // rows_up)), pltpu.SemaphoreType.DMA((rows // rows_up,))],
                compiler_params=pltpu.CompilerParams(vmem_limit_bytes=VMEM_LIMIT),
                cost_estimate=pl.CostEstimate(flops=6 * rows * model * nch * piece, bytes_accessed=60_000_000, transcendentals=0),
                name=f"mlp_{c}",
            )(m, acc, w_mlp[c], w_mlp[c], w_mlp[c], w_mlp[c], vmlp_all)

        pieces = 4
        return pl.pallas_call(
            functools.partial(exchange_out, nwd, pieces),
            out_shape=jax.ShapeDtypeStruct((tokens, width), BF16),
            in_specs=[ANY], out_specs=ANY,
            scratch_shapes=[pltpu.VMEM((rows, width), BF16),
                            pltpu.SemaphoreType.DMA((3, pieces)), pltpu.SemaphoreType.DMA((3, pieces)),
                            pltpu.SemaphoreType.DMA((4, pieces)), pltpu.SemaphoreType.DMA((4, pieces)),
                            pltpu.SemaphoreType.DMA((2,))],
            compiler_params=pltpu.CompilerParams(has_side_effects=True),
            name="exchange_out",
        )(acc)

    return jax.shard_map(local_layer, mesh=mesh, in_specs=specs, out_specs=row_spec, check_vma=False)
```

```python
import jax
import jax.numpy as jnp
from jax import lax
from jax.experimental import pallas as pl
from jax.experimental.pallas import tpu as pltpu
from jax.sharding import PartitionSpec as P

MESH = pl.DeviceIdType.MESH
F32, BF16 = jnp.float32, jnp.bfloat16
EPS = 1e-6
LANES = 256
CHUNK = 256
UP = 512
NX = 4
NWD, NCH = 4, 2
NDEV = NWD * NCH
ANY = pl.BlockSpec(memory_space=pl.ANY)
VMEM_LIMIT = 62 * 1024 * 1024
OWN_X, OWN_Y, OWN_P, X_P, X_Y, Y_P, Y_X, D_P = range(8)


def gelu(v):
    return 0.5 * v * (1.0 + jnp.tanh(0.7978845608028654 * (v + 0.044715 * (v * v * v))))


def sigmoid(v):
    return 1.0 / (1.0 + jnp.exp(-v))


def shuffle_matrix(transposed):
    rows = lax.broadcasted_iota(jnp.int32, (CHUNK, CHUNK), 0)
    cols = lax.broadcasted_iota(jnp.int32, (CHUNK, CHUNK), 1)
    out, src = (cols, rows) if transposed else (rows, cols)
    return jnp.where((out % 8) * (CHUNK // 8) + out // 8 == src, 1.0, 0.0).astype(BF16)


def layer(resid, pos_ref, w_y, w_x, w_o, w_g, w_u, w_d, rgate, igate, vch, vmlp, vwd,
          out, g_y, g_x, g_o, g_g, g_u, g_d, x_far,
          n_s, acc_s, t_a, t_b, t_c, rg_s, ig_s, par_s, mlp_s, vwd_s, x_s, raw_s, u_s, h_s, prod_s, y_s, tail_s, h0_s, act_s,
          msg_out, msg_in, ssem, rsem, tsem, xssem, xrsem, pssem, prsem, lsem, mssem, mrsem, xlsem, ossem, orsem, fssem, frsem, olsem):
    ch, wd = lax.axis_index("ch"), lax.axis_index("wd")
    core = lax.rem(wd, 2)
    me = ch * NWD + wd
    wx, wp = lax.rem(wd + 2, NWD), wd + 1 - 2 * core
    dev_x, dev_y, dev_p = (0, ch, wx), (0, 1 - ch, wd), (0, ch, wp)
    id_x, id_y, id_d = ch * NWD + wx, (1 - ch) * NWD + wd, (1 - ch) * NWD + wx
    tokens, model = n_s.shape
    width = resid.shape[1]
    blocks = w_y.shape[1] // LANES
    halves = blocks * NCH
    groups = w_g.shape[1] // LANES
    steps = tokens // CHUNK
    ups = tokens // UP
    every = slice(None)

    def remote(src, dst, device, send, recv):
        return pltpu.make_async_remote_copy(src_ref=src, dst_ref=dst, send_sem=send, recv_sem=recv, device_id=device,
                                            device_id_type=MESH)

    def cols_of(i):
        return pl.ds(pl.multiple_of(i * LANES, LANES), LANES)

    def first(i):
        return [(w_y, g_y, every, cols_of(i)), (w_x, g_x, every, cols_of(i)), (w_o, g_o, i, every)]

    def second(i):
        return [(w_g, g_g, every, cols_of(i)), (w_u, g_u, every, cols_of(i)), (w_d, g_d, i, every)]

    def cut(unit, owner, part):
        own, far, rows, cols = unit
        if rows == every:
            size, base = own.shape[0], 0
        else:
            size, base = LANES, rows * LANES
        if part is not None:
            size = size // 2
            base = base + part * size
        rows = pl.ds(pl.multiple_of(base, size) if not isinstance(base, int) else base, size)
        return own.at[rows, cols] if owner is None else far.at[owner, rows, cols]

    def transfer(kind, g, u, unit, split):
        owner, part, device = {OWN_X: (None, None, dev_x), OWN_Y: (None, None, dev_y), OWN_P: (None, None, dev_p),
                               X_P: (id_x, None, dev_p), X_Y: (id_x, 0 if split else None, dev_y),
                               Y_P: (id_y, None, dev_p), Y_X: (id_y, 1, dev_x), D_P: (id_d, None, dev_p)}[kind]
        src = cut(unit, owner, part)
        dst = cut(unit, me if owner is None else owner, part)
        return remote(src, dst, device, ssem.at[kind, g, u], rsem.at[kind, g, u])

    def send(g, units, kinds, split):
        for kind in kinds:
            for u, unit in enumerate(units):
                transfer(kind, g, u, unit, split).start()

    def forward(g, units, split):
        for u, unit in enumerate(units):
            transfer(OWN_X, g, u, unit, split).wait_recv()
            transfer(X_Y, g, u, unit, split).start()
            transfer(X_P, g, u, unit, split).start()
        for u, unit in enumerate(units):
            transfer(OWN_Y, g, u, unit, split).wait_recv()
            if split:
                transfer(Y_X, g, u, unit, split).start()
            transfer(Y_P, g, u, unit, split).start()

    def relay(g, units, split):
        for u, unit in enumerate(units):
            transfer(X_Y, g, u, unit, split).wait_recv()
            if split:
                transfer(Y_X, g, u, unit, split).wait_recv()
            transfer(D_P, g, u, unit, split).start()

    def ready(g, units, split):
        for u, unit in enumerate(units):
            for kind in (OWN_P, X_P, Y_P, D_P):
                transfer(kind, g, u, unit, split).wait_recv()

    def drain(g, units, split):
        for u, unit in enumerate(units):
            for kind in range(8):
                if split or kind != Y_X:
                    transfer(kind, g, u, unit, split).wait_send()

    both = (OWN_X, OWN_Y, OWN_P)

    def tile(units, owner, slot, place, own, start):
        for u, (unit, buf) in enumerate(zip(units, (t_a, t_b, t_c))):
            d = pltpu.make_async_copy(cut(unit, None if own else owner, None), buf.at[slot, place], tsem.at[slot, u, place])
            if start:
                d.start()
            else:
                d.wait()

    def load_tiles(units, slot, count, base):
        @pl.loop(0, count)
        def _(k):
            owner = base + k

            @pl.when(owner == me)
            def _():
                tile(units, owner, slot, k, True, True)

            @pl.when(owner != me)
            def _():
                tile(units, owner, slot, k, False, True)

    def wait_tiles(units, slot, count):
        @pl.loop(0, count)
        def _(k):
            tile(units, 0, slot, k, False, False)

    send(0, first(0), both, False)
    small = [(vch, par_s.at[pl.ds(ch * blocks, blocks)]), (rgate, rg_s.at[pl.ds(ch * blocks, blocks)]),
             (igate, ig_s.at[pl.ds(ch * blocks, blocks)]), (vmlp, mlp_s.at[ch])]
    small_sends = [remote(s, d, dev_y, pssem.at[i], prsem.at[i]) for i, (s, d) in enumerate(small)]
    for p in (1, 2, 3):
        i = len(small) + p - 1
        small_sends.append(remote(vwd, vwd_s.at[wd], (0, ch, lax.rem(wd + p, NWD)), pssem.at[i], prsem.at[i]))
    small_own = [pltpu.make_async_copy(s, d, lsem.at[i]) for i, (s, d) in enumerate(small + [(vwd, vwd_s.at[wd])])]
    for d in small_sends + small_own:
        d.start()

    rows_x = tokens // NX

    def x_copy(p, q):
        peer = lax.rem(wd + p, NWD)
        return remote(resid.at[pl.ds((ch * NWD + peer) * tokens + q * rows_x, rows_x)],
                      x_far.at[pl.ds(q * rows_x, rows_x), pl.ds(pl.multiple_of(wd * width, width), width)],
                      (0, ch, peer), xssem.at[p - 1, q], xrsem.at[p - 1, q])

    for q in range(NX):
        for p in (2, 1, 3):
            x_copy(p, q).start()
    for g in range(1, blocks):
        send(g, first(g), (OWN_X,), False)
    forward(0, first(0), False)
    for g in range(1, blocks):
        send(g, first(g), (OWN_Y, OWN_P), False)
    for d in small_own:
        d.wait()
    for d in small_sends:
        d.wait()
    relay(0, first(0), False)
    ready(0, first(0), False)
    load_tiles(first(0), 0, NWD, 0)

    def wide(i):
        return jnp.concatenate([vwd_s[k, i:i + 1, :] for k in range(NWD)], axis=1)

    def x_load(c):
        rows = pl.ds(c * CHUNK, CHUNK)
        for k in range(NWD):
            cols = pl.ds(k * width, width)

            @pl.when(wd == k)
            def _():
                pltpu.make_async_copy(resid.at[pl.ds(me * tokens + c * CHUNK, CHUNK)], x_s.at[:, cols], xlsem.at[k]).start()

            @pl.when(wd != k)
            def _():
                pltpu.make_async_copy(x_far.at[rows, cols], x_s.at[:, cols], xlsem.at[k]).start()

        for k in range(NWD):
            cols = pl.ds(k * width, width)
            pltpu.make_async_copy(x_far.at[rows, cols], x_s.at[:, cols], xlsem.at[k]).wait()

    mix = shuffle_matrix(False)

    @pl.loop(0, steps)
    def _(c):
        @pl.when(lax.rem(c, steps // NX) == 0)
        def _():
            for p in (1, 2, 3):
                x_copy(p, c // (steps // NX)).wait_recv()

        x_load(c)
        rows = pl.ds(c * CHUNK, CHUNK)
        vals = jnp.dot(mix, x_s[...], preferred_element_type=F32)
        scale = lax.rsqrt(jnp.mean(vals * vals, axis=1, keepdims=True) + EPS)
        n_s[rows, :] = (vals * scale * (1.0 + wide(0))).astype(BF16)
        acc_s[rows, :] = vals + wide(1)

    def message(i):
        return remote(msg_out.at[i], msg_in.at[i], dev_p, mssem.at[i], mrsem.at[i])

    def project(q, slot, tiles):
        vals = n_s[pl.ds(q * CHUNK, CHUNK), :]
        raw_s[slot, 0] = jnp.dot(vals, t_a[tiles, 0:NWD].reshape(model, LANES), preferred_element_type=F32)
        raw_s[slot, 1] = jnp.dot(vals, t_b[tiles, 0:NWD].reshape(model, LANES), preferred_element_type=F32)

    def recur(q, slot, tiles, block):
        def row(i):
            return par_s[block, i:i + 1, :]

        rows = pl.ds(q * CHUNK, CHUNK)
        time = CHUNK // 8
        pos = pos_ref[rows, :]
        pos = jnp.concatenate([pos] * (LANES // pos.shape[1]), axis=1)
        y_s[...] = gelu(raw_s[slot, 0] + row(1)).astype(BF16)
        u = (raw_s[slot, 1] + row(0)).astype(BF16).astype(F32)
        u_s[24:, :] = u
        sub = lax.broadcasted_iota(jnp.int32, (8, LANES), 0)
        last = u[CHUNK - 24:, :]
        for k in range(3):
            edge = jnp.where(sub == 7, tail_s[k * 8:(k + 1) * 8, :], last[k * 8:(k + 1) * 8, :])
            u_s[k * 8:(k + 1) * 8, :] = pltpu.roll(edge, 1, 0)
        tail_s[...] = last
        c = row(2) + u * row(3)
        for k in range(1, 4):
            c = c + jnp.where(pos >= k, u_s[pl.ds(24 - 8 * k, CHUNK), :], 0.0) * row(3 + k)
        c16 = c.astype(BF16)
        rate = sigmoid(jnp.dot(c16, rg_s[block], preferred_element_type=F32) + row(8))
        inflow = sigmoid(jnp.dot(c16, ig_s[block], preferred_element_type=F32) + row(9))
        log_a = rate * row(7)
        a = jnp.exp(log_a)
        scale = jnp.sqrt(jnp.tanh(-log_a) * (1.0 + a * a))
        reset = pos == 0
        a = jnp.where(reset, 0.0, a)
        scale = jnp.where(reset, 1.0, scale)
        b = scale * inflow * c16.astype(F32)
        h, prod = b[0:8, :], a[0:8, :]
        h_s[0:8, :] = h
        prod_s[0:8, :] = prod
        for t in range(1, time):
            at = a[t * 8:(t + 1) * 8, :]
            h = at * h + b[t * 8:(t + 1) * 8, :]
            prod = at * prod
            h_s[t * 8:(t + 1) * 8, :] = h
            prod_s[t * 8:(t + 1) * 8, :] = prod
        for k in (1, 2, 4):
            far = sub >= k
            h = jnp.where(far, h + prod * pltpu.roll(h, k, 0), h)
            prod = jnp.where(far, prod * pltpu.roll(prod, k, 0), prod)
        before = h0_s[...]
        ends = h + prod * before
        carry = jnp.where(sub == 0, before, pltpu.roll(ends, 1, 0))
        h0_s[...] = jnp.broadcast_to(ends[7:8, :], (8, LANES))
        hid = h_s[...].reshape(time, 8, LANES) + prod_s[...].reshape(time, 8, LANES) * carry[None]
        mixed = (hid.reshape(CHUNK, LANES) * y_s[...].astype(F32)).astype(BF16)
        for k in range(NWD):
            cols = pl.ds(k * width, width)
            acc_s[rows, cols] += jnp.dot(mixed, t_c[tiles, k], preferred_element_type=F32)

    @pl.loop(0, halves)
    def _(i):
        jj, side = i // 2, lax.rem(i, 2)
        tiles = side
        block = side * blocks + jj

        for g in range(1, blocks):
            @pl.when(i == g)
            def _(g=g):
                forward(g, first(g), False)

        for at, b in ((3, 0), (4, 1), (5, 2), (7, 3)):
            @pl.when(i == at)
            def _(b=b):
                send(blocks + b, second(b), both, True)

        for at, b in ((6, 0), (8, 1)):
            @pl.when(i == at)
            def _(b=b):
                forward(blocks + b, second(b), True)

        def relay_next(of):
            for g in range(1, blocks):
                @pl.when((core == of) & (i == 2 * g - 1))
                def _(g=g):
                    relay(g, first(g), False)

            @pl.when((core == of) & (i == halves - 1))
            def _():
                relay(blocks, second(0), True)

        relay_next(1)
        wait_tiles(first(0), tiles, NWD)
        project(0, 0, tiles)

        @pl.when(core == 0)
        def _():
            h0_s[...] = jnp.zeros_like(h0_s)
            tail_s[...] = jnp.zeros_like(tail_s)

        @pl.when(core == 1)
        def _():
            message(i).wait_recv()
            tail_s[...] = msg_in[i, 0:24, :]
            h0_s[...] = msg_in[i, 24:32, :]

        @pl.loop(0, steps - 1)
        def _(q):
            @pl.when((q == 3) & (side == 0))
            def _():
                load_tiles(first(jj), 1, NWD, NWD)

            slot = lax.rem(q, 2)
            project(q + 1, 1 - slot, tiles)
            recur(q, slot, tiles, block)

        recur(steps - 1, (steps - 1) % 2, tiles, block)

        @pl.when(core == 0)
        def _():
            msg_out[i, 0:24, :] = tail_s[...]
            msg_out[i, 24:32, :] = h0_s[...]
            message(i).start()

        relay_next(0)

        @pl.when((side == 1) & (i < halves - 1))
        def _():
            for g in range(1, blocks):
                @pl.when(jj == g - 1)
                def _(g=g):
                    ready(g, first(g), False)
            load_tiles(first(jj + 1), 0, NWD, 0)

    ready(blocks, second(0), True)
    load_tiles(second(0), 0, NDEV, 0)

    @pl.loop(0, steps)
    def _(c):
        rows = pl.ds(c * CHUNK, CHUNK)
        vals = acc_s[rows, :]
        scale = lax.rsqrt(jnp.mean(vals * vals, axis=1, keepdims=True) + EPS)
        n_s[rows, :] = (vals * scale * (1.0 + wide(2))).astype(BF16)
        acc_s[rows, :] = vals + wide(3)

    def rows_of(i):
        return pl.ds(i * UP, UP)

    def up(i, slot, tiles, b):
        vals = n_s[rows_of(i), :]
        for c in range(NCH):
            part = slice(c * NWD, (c + 1) * NWD)
            gate = jnp.dot(vals, t_a[tiles, part].reshape(model, LANES), preferred_element_type=F32) + mlp_s[c, 0:1, cols_of(b)]
            upper = jnp.dot(vals, t_b[tiles, part].reshape(model, LANES), preferred_element_type=F32) + mlp_s[c, 1:2, cols_of(b)]
            act_s[slot, :, c * LANES:(c + 1) * LANES] = (gelu(gate) * upper).astype(BF16)

    def down(i, slot, tiles):
        for k in range(NWD):
            cols = pl.ds(k * width, width)
            more = [jnp.dot(act_s[slot, :, c * LANES:(c + 1) * LANES], t_c[tiles, c * NWD + k], preferred_element_type=F32) for c in range(NCH)]
            acc_s[rows_of(i), cols] += more[0] + more[1]

    base = me * tokens
    own_cols = pl.ds(pl.multiple_of(wd * width, width), width)

    def direct(p, i):
        peer = lax.rem(wd + p, NWD)
        return remote(n_s.at[rows_of(i), pl.ds(pl.multiple_of(peer * width, width), width)], out.at[pl.ds(base + i * UP, UP)],
                      (0, ch, peer), ossem.at[p - 1, i], orsem.at[p - 1, i])

    def across(i):
        return remote(n_s.at[rows_of(i), own_cols], out.at[pl.ds(base + i * UP, UP)], dev_y, fssem.at[0, i], frsem.at[0, i])

    def onward(p, i):
        came = lax.rem(wd + NWD - p, NWD)
        here = pl.ds((ch * NWD + came) * tokens + i * UP, UP)
        return remote(out.at[here], out.at[here], dev_y, fssem.at[p, i], frsem.at[p, i])

    def keep(i):
        return pltpu.make_async_copy(n_s.at[rows_of(i), own_cols], out.at[pl.ds(base + i * UP, UP)], olsem.at[i])

    def hand_out(i):
        back = shuffle_matrix(True)
        for c in range(UP // CHUNK):
            rows = pl.ds(i * UP + c * CHUNK, CHUNK)
            n_s[rows, :] = jnp.dot(back, acc_s[rows, :].astype(BF16), preferred_element_type=F32).astype(BF16)
        across(i).start()
        for p in (2, 1, 3):
            direct(p, i).start()
        keep(i).start()

    def ahead(s):
        return s + 2 - (s + 7) // 12

    @pl.loop(0, groups)
    def _(s):
        tiles = lax.rem(s, 2)

        @pl.when(s + 4 < groups)
        def _():
            send(blocks + s + 4, second(s + 4), both, True)

        @pl.when((ahead(s + 1) > ahead(s)) & (ahead(s) < groups))
        def _():
            forward(blocks + ahead(s), second(ahead(s)), True)

        wait_tiles(second(0), tiles, NDEV)
        up(0, 0, tiles, s)

        @pl.loop(1, ups)
        def _(i):
            @pl.when((i == 2) & (s + 1 < groups))
            def _():
                relay(blocks + s + 1, second(s + 1), True)
                ready(blocks + s + 1, second(s + 1), True)
                load_tiles(second(s + 1), 1 - tiles, NDEV, 0)

            slot = lax.rem(i, 2)
            up(i, slot, tiles, s)
            down(i - 1, 1 - slot, tiles)

            @pl.when(s == groups - 1)
            def _():
                hand_out(i - 1)

        down(ups - 1, (ups - 1) % 2, tiles)

    hand_out(ups - 1)

    for i in range(ups):
        for p in (1, 2, 3):
            direct(p, i).wait_recv()
            onward(p, i).start()
    for g in range(blocks):
        drain(g, first(g), False)

    @pl.loop(0, groups)
    def _(b):
        drain(blocks + b, second(b), True)

    for q in range(NX):
        for p in (1, 2, 3):
            x_copy(p, q).wait_send()

    @pl.when(core == 0)
    def _():
        @pl.loop(0, halves)
        def _(i):
            message(i).wait_send()

    for i in range(ups):
        keep(i).wait()
        across(i).wait()
        for p in (1, 2, 3):
            direct(p, i).wait_send()
            onward(p, i).wait()


def solution(mesh):
    row_spec = P("dp", "wd")
    specs = (row_spec, P("dp", None), P("wd"), P("wd", "ch"), P("ch"), P("wd", "ch"), P("ch"), P(None, "ch"), P("ch"), P("ch"), P("ch", None, None), P("ch"), P("ch", None, None), P("ch"), P("ch", "wd"), P("wd"), P("wd"), P("wd", "ch"), P("ch"), P("wd", "ch"), P("ch"), P("ch", "wd"), P("wd"))

    def local_layer(resid_in, seg_pos, gain_temporal, w_x, bias_x, w_y, bias_y, conv_w, conv_bias, lam_param, rgate_w, rgate_b, igate_w, igate_b, w_o, bias_o, gain_mlp, w_g, bias_g, w_u, bias_u, w_d, bias_d):
        tokens, width = resid_in.shape
        model = width * NWD
        rows = tokens // NDEV
        blocks = w_x.shape[1] // LANES
        groups = w_g.shape[1] // LANES
        total = NCH * blocks
        ch, wd = lax.axis_index("ch"), lax.axis_index("wd")
        per_chan = jnp.stack([bias_x, bias_y, conv_bias, *conv_w, -8.0 * jax.nn.softplus(-lam_param), rgate_b, igate_b]).astype(F32)
        per_chan = jnp.pad(per_chan, ((0, 16 - per_chan.shape[0]), (0, 0)))
        vch = per_chan.reshape(16, blocks, LANES).transpose(1, 0, 2)
        vmlp = jnp.pad(jnp.stack([bias_g, bias_u]).astype(F32), ((0, 6), (0, 0)))
        vwd = jnp.pad(jnp.stack([gain_temporal, bias_o, gain_mlp, bias_d]).astype(F32), ((0, 4), (0, 0)))
        pos = lax.dynamic_index_in_dim(seg_pos.reshape(NDEV, rows), ch * NWD + wd, 0, keepdims=False)
        pos = pos.reshape(rows // CHUNK, 8, CHUNK // 8).transpose(0, 2, 1).reshape(rows, 1)
        pos = jnp.broadcast_to(pos, (rows, 128))

        def like(w):
            return jax.ShapeDtypeStruct((NDEV, *w.shape), BF16)

        dma = pltpu.SemaphoreType.DMA
        ups = rows // UP
        kinds = (8, blocks + groups, 3)
        outs = pl.pallas_call(
            layer,
            out_shape=[jax.ShapeDtypeStruct((tokens, width), BF16), like(w_y), like(w_x), like(w_o), like(w_g), like(w_u), like(w_d),
                       jax.ShapeDtypeStruct((rows, model), BF16)],
            in_specs=[ANY, pl.BlockSpec(memory_space=pltpu.VMEM)] + [ANY] * 11,
            out_specs=[ANY] * 8,
            scratch_shapes=[pltpu.VMEM((rows, model), BF16), pltpu.VMEM((rows, model), F32),
                            pltpu.VMEM((2, NDEV, width, LANES), BF16), pltpu.VMEM((2, NDEV, width, LANES), BF16),
                            pltpu.VMEM((2, NDEV, LANES, width), BF16),
                            pltpu.VMEM((total, LANES, LANES), BF16), pltpu.VMEM((total, LANES, LANES), BF16),
                            pltpu.VMEM((total, 16, LANES), F32), pltpu.VMEM((NCH, *vmlp.shape), F32), pltpu.VMEM((NWD, *vwd.shape), F32),
                            pltpu.VMEM((CHUNK, model), BF16), pltpu.VMEM((2, 2, CHUNK, LANES), F32), pltpu.VMEM((CHUNK + 24, LANES), F32),
                            pltpu.VMEM((CHUNK, LANES), F32), pltpu.VMEM((CHUNK, LANES), F32), pltpu.VMEM((CHUNK, LANES), BF16),
                            pltpu.VMEM((24, LANES), F32), pltpu.VMEM((8, LANES), F32), pltpu.VMEM((2, UP, NCH * LANES), BF16),
                            pltpu.VMEM((total, 32, LANES), F32), pltpu.VMEM((total, 32, LANES), F32),
                            dma(kinds), dma(kinds), dma((2, 3, NDEV)), dma((3, NX)), dma((3, NX)), dma((7,)), dma((7,)), dma((5,)),
                            dma((total,)), dma((total,)), dma((NWD,)), dma((3, ups)), dma((3, ups)), dma((4, ups)), dma((4, ups)), dma((ups,))],
            compiler_params=pltpu.CompilerParams(has_side_effects=True, vmem_limit_bytes=VMEM_LIMIT),
            name="layer",
        )(resid_in, pos, w_y, w_x, w_o, w_g, w_u, w_d, rgate_w, igate_w, vch, vmlp, vwd)
        return outs[0]

    return jax.shard_map(local_layer, mesh=mesh, in_specs=specs, out_specs=row_spec, check_vma=False)
```

```python
import jax
import jax.numpy as jnp
from jax import lax
from jax.experimental import pallas as pl
from jax.experimental.pallas import tpu as pltpu
from jax.sharding import PartitionSpec as P

MESH = pl.DeviceIdType.MESH
F32, BF16 = jnp.float32, jnp.bfloat16
EPS = 1e-6
LANES = 256
CHUNK = 256
UP = 512
DOWN = 2
NX = 4
NWD, NCH = 4, 2
NDEV = NWD * NCH
ANY = pl.BlockSpec(memory_space=pl.ANY)
VMEM_LIMIT = 65_800_000
OWN_X, OWN_Y, OWN_P, X_P, X_Y, Y_P, Y_X, D_P = range(8)


def gelu(v):
    return 0.5 * v * (1.0 + jnp.tanh(0.7978845608028654 * (v + 0.044715 * (v * v * v))))


def sigmoid(v):
    return 1.0 / (1.0 + jnp.exp(-v))


def shuffle_matrix(transposed):
    rows = lax.broadcasted_iota(jnp.int32, (CHUNK, CHUNK), 0)
    cols = lax.broadcasted_iota(jnp.int32, (CHUNK, CHUNK), 1)
    out, src = (cols, rows) if transposed else (rows, cols)
    return jnp.where((out % 8) * (CHUNK // 8) + out // 8 == src, 1.0, 0.0).astype(BF16)


def layer(resid, pos_ref, w_y, w_x, w_o, w_g, w_u, w_d, rgate, igate, vch, vmlp, vwd,
          out, g_y, g_x, g_o, g_g, g_u, g_d, x_far,
          n_s, acc_s, act_s, t_w, par_s, mlp_s, vwd_s, raw_s, u_s, h_s, prod_s, y_s, tail_s, h0_s,
          msg_out, msg_in, ssem, rsem, dssem, drsem, tsem, xssem, xrsem, pssem, prsem, lsem, mssem, mrsem, xlsem, ossem, orsem, fssem, frsem, olsem):
    ch, wd = lax.axis_index("ch"), lax.axis_index("wd")
    core = lax.rem(wd, 2)
    me = ch * NWD + wd
    wx, wp = lax.rem(wd + 2, NWD), wd + 1 - 2 * core
    dev_x, dev_y, dev_p = (0, ch, wx), (0, 1 - ch, wd), (0, ch, wp)
    id_x, id_y, id_d = ch * NWD + wx, (1 - ch) * NWD + wd, (1 - ch) * NWD + wx
    tokens, model = n_s.shape
    width = resid.shape[1]
    blocks = w_y.shape[1] // LANES
    halves = blocks * NCH
    groups = w_g.shape[1] // LANES
    steps = tokens // CHUNK
    ups = tokens // UP
    every = slice(None)
    deep = w_d.shape[0] // DOWN

    x_s = act_s.at[1, pl.ds(2 * LANES, CHUNK), pl.ds(0, model)]
    gate_rows = 3 * LANES

    def gate_area(which, side):
        cols = pl.ds(pl.multiple_of((2 * which + side) * LANES, LANES), LANES)
        return act_s.at[1, pl.ds(gate_rows, blocks * LANES), cols]

    def back_tile(slot, k):
        return act_s.at[1, pl.ds(pl.multiple_of(slot * LANES, LANES), LANES), pl.ds(pl.multiple_of(k * width, width), width)]

    def remote(src, dst, device, send, recv):
        return pltpu.make_async_remote_copy(src_ref=src, dst_ref=dst, send_sem=send, recv_sem=recv, device_id=device,
                                            device_id_type=MESH)

    def cols_of(i):
        return pl.ds(pl.multiple_of(i * LANES, LANES), LANES)

    def first(i):
        return [(w_y, g_y, every, cols_of(i)), (w_x, g_x, every, cols_of(i)), (w_o, g_o, i, every)]

    def second(i):
        return [(w_g, g_g, every, cols_of(i)), (w_u, g_u, every, cols_of(i))]

    def cut(unit, owner, part):
        own, far, rows, cols = unit
        if rows == every:
            size, base = own.shape[0], 0
        else:
            size, base = LANES, rows * LANES
        if part is not None:
            size = size // 2
            base = base + part * size
        rows = pl.ds(pl.multiple_of(base, size) if not isinstance(base, int) else base, size)
        return own.at[rows, cols] if owner is None else far.at[owner, rows, cols]

    def transfer(kind, g, u, unit, split):
        owner, part, device = {OWN_X: (None, None, dev_x), OWN_Y: (None, None, dev_y), OWN_P: (None, None, dev_p),
                               X_P: (id_x, None, dev_p), X_Y: (id_x, 0 if split else None, dev_y),
                               Y_P: (id_y, None, dev_p), Y_X: (id_y, 1, dev_x), D_P: (id_d, None, dev_p)}[kind]
        src = cut(unit, owner, part)
        dst = cut(unit, me if owner is None else owner, part)
        return remote(src, dst, device, ssem.at[kind, g, u], rsem.at[kind, g, u])

    def send(g, units, kinds, split):
        for kind in kinds:
            for u, unit in enumerate(units):
                transfer(kind, g, u, unit, split).start()

    def forward(g, units, split):
        for u, unit in enumerate(units):
            transfer(OWN_X, g, u, unit, split).wait_recv()
            transfer(X_Y, g, u, unit, split).start()
            transfer(X_P, g, u, unit, split).start()
        for u, unit in enumerate(units):
            transfer(OWN_Y, g, u, unit, split).wait_recv()
            if split:
                transfer(Y_X, g, u, unit, split).start()
            transfer(Y_P, g, u, unit, split).start()

    def relay(g, units, split):
        for u, unit in enumerate(units):
            transfer(X_Y, g, u, unit, split).wait_recv()
            if split:
                transfer(Y_X, g, u, unit, split).wait_recv()
            transfer(D_P, g, u, unit, split).start()

    def ready(g, units, split):
        for u, unit in enumerate(units):
            for kind in (OWN_P, X_P, Y_P, D_P):
                transfer(kind, g, u, unit, split).wait_recv()

    def drain(g, units, split):
        for u, unit in enumerate(units):
            for kind in range(8):
                if split or kind != Y_X:
                    transfer(kind, g, u, unit, split).wait_send()

    both = (OWN_X, OWN_Y, OWN_P)

    def down_piece(kind, d):
        owner, device = {OWN_X: (None, dev_x), OWN_Y: (None, dev_y), OWN_P: (None, dev_p), X_P: (id_x, dev_p),
                         Y_P: (id_y, dev_p), Y_X: (id_y, dev_x), D_P: (id_d, dev_p)}[kind]
        rows = pl.ds(d * deep, deep)
        src = w_d.at[rows] if owner is None else g_d.at[owner, rows]
        return remote(src, g_d.at[me if owner is None else owner, rows], device, dssem.at[kind, d], drsem.at[kind, d])

    def forward_down(d):
        down_piece(OWN_Y, d).wait_recv()
        down_piece(Y_X, d).start()
        down_piece(Y_P, d).start()
        down_piece(OWN_X, d).wait_recv()
        down_piece(X_P, d).start()

    def tile(units, owner, slot, place, own, start):
        for u, unit in enumerate(units):
            buf = back_tile(slot, place) if u == 2 else t_w.at[2 * u + slot, place]
            d = pltpu.make_async_copy(cut(unit, None if own else owner, None), buf, tsem.at[slot, u, place])
            if start:
                d.start()
            else:
                d.wait()

    def load_tiles(units, slot, count, base):
        @pl.loop(0, count)
        def _(k):
            owner = base + k

            @pl.when(owner == me)
            def _():
                tile(units, owner, slot, k, True, True)

            @pl.when(owner != me)
            def _():
                tile(units, owner, slot, k, False, True)

    def wait_tiles(units, slot, count):
        @pl.loop(0, count)
        def _(k):
            tile(units, 0, slot, k, False, False)

    send(0, first(0), both, False)
    small = [(vch, par_s.at[pl.ds(ch * blocks, blocks)]), (rgate, gate_area(0, ch)), (igate, gate_area(1, ch)), (vmlp, mlp_s.at[ch])]
    small_sends = [remote(s, d, dev_y, pssem.at[i], prsem.at[i]) for i, (s, d) in enumerate(small)]
    for p in (1, 2, 3):
        i = len(small) + p - 1
        small_sends.append(remote(vwd, vwd_s.at[wd], (0, ch, lax.rem(wd + p, NWD)), pssem.at[i], prsem.at[i]))
    small_own = [pltpu.make_async_copy(s, d, lsem.at[i]) for i, (s, d) in enumerate(small + [(vwd, vwd_s.at[wd])])]
    for d in small_sends[:1] + small_sends[3:] + small_own:
        d.start()

    rows_x = tokens // NX

    def x_copy(p, q):
        peer = lax.rem(wd + p, NWD)
        return remote(resid.at[pl.ds((ch * NWD + peer) * tokens + q * rows_x, rows_x)],
                      x_far.at[pl.ds(q * rows_x, rows_x), pl.ds(pl.multiple_of(wd * width, width), width)],
                      (0, ch, peer), xssem.at[p - 1, q], xrsem.at[p - 1, q])

    for q in range(NX):
        for p in (2, 1, 3):
            x_copy(p, q).start()
    for g in range(1, blocks):
        send(g, first(g), (OWN_X,), False)
    forward(0, first(0), False)
    for g in range(1, blocks):
        send(g, first(g), (OWN_Y, OWN_P), False)
        if g == 1:
            for d in small_sends[1:3]:
                d.start()
    for d in small_own + small_sends[4:]:
        d.wait()
    relay(0, first(0), False)
    ready(0, first(0), False)
    load_tiles(first(0), 0, NWD, 0)

    def wide(i):
        return jnp.concatenate([vwd_s[k, i:i + 1, :] for k in range(NWD)], axis=1)

    def x_load(c):
        rows = pl.ds(c * CHUNK, CHUNK)
        for k in range(NWD):
            cols = pl.ds(k * width, width)

            @pl.when(wd == k)
            def _():
                pltpu.make_async_copy(resid.at[pl.ds(me * tokens + c * CHUNK, CHUNK)], x_s.at[:, cols], xlsem.at[k]).start()

            @pl.when(wd != k)
            def _():
                pltpu.make_async_copy(x_far.at[rows, cols], x_s.at[:, cols], xlsem.at[k]).start()

        for k in range(NWD):
            cols = pl.ds(k * width, width)
            pltpu.make_async_copy(x_far.at[rows, cols], x_s.at[:, cols], xlsem.at[k]).wait()

    mix = shuffle_matrix(False)

    @pl.loop(0, steps)
    def _(c):
        @pl.when(lax.rem(c, steps // NX) == 0)
        def _():
            for p in (1, 2, 3):
                x_copy(p, c // (steps // NX)).wait_recv()

        x_load(c)
        rows = pl.ds(c * CHUNK, CHUNK)
        vals = jnp.dot(mix, x_s[...], preferred_element_type=F32)
        scale = lax.rsqrt(jnp.mean(vals * vals, axis=1, keepdims=True) + EPS)
        n_s[rows, :] = (vals * scale * (1.0 + wide(0))).astype(BF16)
        acc_s[rows, :] = vals + wide(1)

    for d in small_sends[:4]:
        d.wait()

    def message(i):
        return remote(msg_out.at[i], msg_in.at[i], dev_p, mssem.at[i], mrsem.at[i])

    def project(q, slot, tiles):
        vals = n_s[pl.ds(q * CHUNK, CHUNK), :]
        raw_s[slot, 0] = jnp.dot(vals, t_w[tiles, 0:NWD].reshape(model, LANES), preferred_element_type=F32)
        raw_s[slot, 1] = jnp.dot(vals, t_w[2 + tiles, 0:NWD].reshape(model, LANES), preferred_element_type=F32)

    def recur(q, slot, tiles, block):
        def row(i):
            return par_s[block, i:i + 1, :]

        rows = pl.ds(q * CHUNK, CHUNK)
        time = CHUNK // 8
        pos = pos_ref[rows, :]
        pos = jnp.concatenate([pos] * (LANES // pos.shape[1]), axis=1)
        y_s[...] = gelu(raw_s[slot, 0] + row(1)).astype(BF16)
        u = (raw_s[slot, 1] + row(0)).astype(BF16).astype(F32)
        u_s[24:, :] = u
        sub = lax.broadcasted_iota(jnp.int32, (8, LANES), 0)
        last = u[CHUNK - 24:, :]
        for k in range(3):
            edge = jnp.where(sub == 7, tail_s[k * 8:(k + 1) * 8, :], last[k * 8:(k + 1) * 8, :])
            u_s[k * 8:(k + 1) * 8, :] = pltpu.roll(edge, 1, 0)
        tail_s[...] = last
        c = row(2) + u * row(3)
        for k in range(1, 4):
            c = c + jnp.where(pos >= k, u_s[pl.ds(24 - 8 * k, CHUNK), :], 0.0) * row(3 + k)
        c16 = c.astype(BF16)
        gates = [gate_area(which, block // blocks)[pl.ds(pl.multiple_of(lax.rem(block, blocks) * LANES, LANES), LANES), :] for which in range(2)]
        rate = sigmoid(jnp.dot(c16, gates[0], preferred_element_type=F32) + row(8))
        inflow = sigmoid(jnp.dot(c16, gates[1], preferred_element_type=F32) + row(9))
        log_a = rate * row(7)
        a = jnp.exp(log_a)
        scale = jnp.sqrt(jnp.tanh(-log_a) * (1.0 + a * a))
        reset = pos == 0
        a = jnp.where(reset, 0.0, a)
        scale = jnp.where(reset, 1.0, scale)
        b = scale * inflow * c16.astype(F32)
        h, prod = b[0:8, :], a[0:8, :]
        h_s[0:8, :] = h
        prod_s[0:8, :] = prod
        for t in range(1, time):
            at = a[t * 8:(t + 1) * 8, :]
            h = at * h + b[t * 8:(t + 1) * 8, :]
            prod = at * prod
            h_s[t * 8:(t + 1) * 8, :] = h
            prod_s[t * 8:(t + 1) * 8, :] = prod
        for k in (1, 2, 4):
            far = sub >= k
            h = jnp.where(far, h + prod * pltpu.roll(h, k, 0), h)
            prod = jnp.where(far, prod * pltpu.roll(prod, k, 0), prod)
        before = h0_s[...]
        ends = h + prod * before
        carry = jnp.where(sub == 0, before, pltpu.roll(ends, 1, 0))
        h0_s[...] = jnp.broadcast_to(ends[7:8, :], (8, LANES))
        hid = h_s[...].reshape(time, 8, LANES) + prod_s[...].reshape(time, 8, LANES) * carry[None]
        mixed = (hid.reshape(CHUNK, LANES) * y_s[...].astype(F32)).astype(BF16)
        for k in range(NWD):
            cols = pl.ds(k * width, width)
            acc_s[rows, cols] += jnp.dot(mixed, back_tile(tiles, k)[...], preferred_element_type=F32)

    def came(i):
        return jnp.maximum(i - 4, 0)

    def pass_on(low, high):
        @pl.loop(low, high)
        def _(b):
            forward(blocks + b, second(b), True)

            @pl.when(b + 3 < groups)
            def _():
                send(blocks + b + 3, second(b + 3), both, True)

    @pl.loop(0, halves)
    def _(i):
        jj, side = i // 2, lax.rem(i, 2)
        tiles = side
        block = side * blocks + jj

        for g in range(1, blocks):
            @pl.when(i == g)
            def _(g=g):
                forward(g, first(g), False)

        @pl.when((i >= 2) & (i < 5))
        def _():
            send(blocks + i - 2, second(i - 2), both, True)

        pass_on(came(i), came(i + 1))

        def relay_next(of):
            for g in range(1, blocks):
                @pl.when((core == of) & (i == 2 * g - 1))
                def _(g=g):
                    relay(g, first(g), False)

            @pl.when((core == of) & (i == halves - 1))
            def _():
                relay(blocks, second(0), True)

        relay_next(1)
        wait_tiles(first(0), tiles, NWD)
        project(0, 0, tiles)

        @pl.when(core == 0)
        def _():
            h0_s[...] = jnp.zeros_like(h0_s)
            tail_s[...] = jnp.zeros_like(tail_s)

        @pl.when(core == 1)
        def _():
            message(i).wait_recv()
            tail_s[...] = msg_in[i, 0:24, :]
            h0_s[...] = msg_in[i, 24:32, :]

        @pl.loop(0, steps - 1)
        def _(q):
            @pl.when((q == 3) & (side == 0))
            def _():
                load_tiles(first(jj), 1, NWD, NWD)

            slot = lax.rem(q, 2)
            project(q + 1, 1 - slot, tiles)
            recur(q, slot, tiles, block)

        recur(steps - 1, (steps - 1) % 2, tiles, block)

        @pl.when(core == 0)
        def _():
            msg_out[i, 0:24, :] = tail_s[...]
            msg_out[i, 24:32, :] = h0_s[...]
            message(i).start()

        relay_next(0)

        @pl.when((side == 1) & (i < halves - 1))
        def _():
            for g in range(1, blocks):
                @pl.when(jj == g - 1)
                def _(g=g):
                    ready(g, first(g), False)
            load_tiles(first(jj + 1), 0, NWD, 0)

    pass_on(6, 7)
    ready(blocks, second(0), True)
    load_tiles(second(0), 0, NDEV, 0)

    @pl.loop(0, steps)
    def _(c):
        rows = pl.ds(c * CHUNK, CHUNK)
        vals = acc_s[rows, :]
        scale = lax.rsqrt(jnp.mean(vals * vals, axis=1, keepdims=True) + EPS)
        n_s[rows, :] = (vals * scale * (1.0 + wide(2))).astype(BF16)
        acc_s[rows, :] = vals + wide(3)

    def rows_of(i):
        return pl.ds(i * UP, UP)

    def up(i, tiles, b):
        vals = n_s[rows_of(i), :]
        for c in range(NCH):
            part = slice(c * NWD, (c + 1) * NWD)
            gate = jnp.dot(vals, t_w[tiles, part].reshape(model, LANES), preferred_element_type=F32) + mlp_s[c, 0:1, cols_of(b)]
            upper = jnp.dot(vals, t_w[2 + tiles, part].reshape(model, LANES), preferred_element_type=F32) + mlp_s[c, 1:2, cols_of(b)]
            act_s[c, rows_of(i), cols_of(b)] = (gelu(gate) * upper).astype(BF16)

    def ahead(s):
        return jnp.minimum(s + 7 - s // 5, groups)

    @pl.loop(0, groups)
    def _(s):
        tiles = lax.rem(s, 2)
        pass_on(ahead(s), ahead(s + 1))

        @pl.when(s == 2)
        def _():
            for d in range(DOWN):
                for kind in both:
                    down_piece(kind, d).start()

        @pl.when(s == 9)
        def _():
            forward_down(0)

        wait_tiles(second(0), tiles, NDEV)

        @pl.loop(0, ups)
        def _(i):
            @pl.when((i == 2) & (s + 1 < groups))
            def _():
                relay(blocks + s + 1, second(s + 1), True)
                ready(blocks + s + 1, second(s + 1), True)
                load_tiles(second(s + 1), 1 - tiles, NDEV, 0)

            up(i, tiles, s)

    forward_down(1)

    base = me * tokens

    def col_block(b):
        return lax.rem(wd + lax.rem(b, 2) * (1 - 2 * core) + 2 * (b // 2) + NWD, NWD)

    def wide_cols(b):
        return pl.ds(pl.multiple_of(col_block(b) * width, width), width)

    def across(i):
        return remote(n_s.at[rows_of(i), wide_cols(0)], out.at[pl.ds(base + i * UP, UP)], dev_y, fssem.at[0, i], frsem.at[0, i])

    def keep(i):
        return pltpu.make_async_copy(n_s.at[rows_of(i), wide_cols(0)], out.at[pl.ds(base + i * UP, UP)], olsem.at[i])

    def direct(b, i):
        return remote(n_s.at[rows_of(i), wide_cols(b)], out.at[pl.ds(base + i * UP, UP)], (0, ch, col_block(b)),
                      ossem.at[b - 1, i], orsem.at[b - 1, i])

    def onward(b, i):
        here = pl.ds((ch * NWD + col_block(b)) * tokens + i * UP, UP)
        return remote(out.at[here], out.at[here], dev_y, fssem.at[b, i], frsem.at[b, i])

    def load_down(b, p):
        side = lax.rem(ch + p // DOWN, NCH)
        owner = side * NWD + col_block(b)
        third = deep // width

        @pl.loop(0, 2 * third)
        def _(e):
            rows = pl.ds(pl.multiple_of(lax.rem(p, DOWN) * deep + lax.rem(e, third) * width, width), width)
            cols = cols_of(e // third)

            @pl.when(owner == me)
            def _():
                pltpu.make_async_copy(w_d.at[rows, cols], t_w.at[p, e], tsem.at[p, 2, e]).start()

            @pl.when(owner != me)
            def _():
                pltpu.make_async_copy(g_d.at[owner, rows, cols], t_w.at[p, e], tsem.at[p, 2, e]).start()

    def wait_down(p):
        @pl.loop(0, 2 * (deep // width))
        def _(e):
            pltpu.make_async_copy(w_d.at[pl.ds(0, width), cols_of(0)], t_w.at[p, e], tsem.at[p, 2, e]).wait()

    def down(b, p, i):
        third = deep // width
        side = lax.rem(ch + p // DOWN, NCH)
        vals = act_s[side, rows_of(i), pl.ds(pl.multiple_of(lax.rem(p, DOWN) * deep, deep), deep)]
        for half in range(2):
            cols = pl.ds(pl.multiple_of(col_block(b) * width + half * LANES, LANES), LANES)
            acc_s[rows_of(i), cols] += jnp.dot(vals, t_w[p, half * third:(half + 1) * third].reshape(deep, LANES), preferred_element_type=F32)

    def hand_out(b, i):
        back = shuffle_matrix(True)
        for c in range(UP // CHUNK):
            rows = pl.ds(i * UP + c * CHUNK, CHUNK)
            n_s[rows, wide_cols(b)] = jnp.dot(back, acc_s[rows, wide_cols(b)].astype(BF16), preferred_element_type=F32).astype(BF16)

        @pl.when(b == 0)
        def _():
            across(i).start()
            keep(i).start()

        @pl.when(b > 0)
        def _():
            direct(b, i).start()

    @pl.loop(0, NWD)
    def _(b):
        @pl.when(b == 1)
        def _():
            for d in range(DOWN):
                down_piece(OWN_P, d).wait_recv()
                down_piece(Y_P, d).wait_recv()

        @pl.when(b == 2)
        def _():
            for i in range(ups):
                direct(1, i).wait_recv()
                onward(1, i).start()
            for d in range(DOWN):
                down_piece(Y_X, d).wait_recv()
                down_piece(D_P, d).start()

        @pl.when(b == 3)
        def _():
            for d in range(DOWN):
                down_piece(X_P, d).wait_recv()
                down_piece(D_P, d).wait_recv()

        @pl.loop(0, 2 * DOWN)
        def _(p):
            load_down(b, p)

        @pl.loop(0, 2 * DOWN)
        def _(p):
            wait_down(p)

            @pl.loop(0, ups)
            def _(i):
                down(b, p, i)

                @pl.when(p == 2 * DOWN - 1)
                def _():
                    hand_out(b, i)

    for b in (2, 3):
        for i in range(ups):
            direct(b, i).wait_recv()
            onward(b, i).start()
    for g in range(blocks):
        drain(g, first(g), False)

    @pl.loop(0, groups)
    def _(b):
        drain(blocks + b, second(b), True)

    for d in range(DOWN):
        for kind in (OWN_X, OWN_Y, OWN_P, X_P, Y_P, Y_X, D_P):
            down_piece(kind, d).wait_send()

    for q in range(NX):
        for p in (1, 2, 3):
            x_copy(p, q).wait_send()

    @pl.when(core == 0)
    def _():
        @pl.loop(0, halves)
        def _(i):
            message(i).wait_send()

    for i in range(ups):
        keep(i).wait()
        across(i).wait()
        for p in (1, 2, 3):
            direct(p, i).wait_send()
            onward(p, i).wait()


def solution(mesh):
    row_spec = P("dp", "wd")
    specs = (row_spec, P("dp", None), P("wd"), P("wd", "ch"), P("ch"), P("wd", "ch"), P("ch"), P(None, "ch"), P("ch"), P("ch"), P("ch", None, None), P("ch"), P("ch", None, None), P("ch"), P("ch", "wd"), P("wd"), P("wd"), P("wd", "ch"), P("ch"), P("wd", "ch"), P("ch"), P("ch", "wd"), P("wd"))

    def local_layer(resid_in, seg_pos, gain_temporal, w_x, bias_x, w_y, bias_y, conv_w, conv_bias, lam_param, rgate_w, rgate_b, igate_w, igate_b, w_o, bias_o, gain_mlp, w_g, bias_g, w_u, bias_u, w_d, bias_d):
        tokens, width = resid_in.shape
        model = width * NWD
        rows = tokens // NDEV
        blocks = w_x.shape[1] // LANES
        groups = w_g.shape[1] // LANES
        total = NCH * blocks
        ch, wd = lax.axis_index("ch"), lax.axis_index("wd")
        per_chan = jnp.stack([bias_x, bias_y, conv_bias, *conv_w, -8.0 * jax.nn.softplus(-lam_param), rgate_b, igate_b]).astype(F32)
        per_chan = jnp.pad(per_chan, ((0, 16 - per_chan.shape[0]), (0, 0)))
        vch = per_chan.reshape(16, blocks, LANES).transpose(1, 0, 2)
        vmlp = jnp.pad(jnp.stack([bias_g, bias_u]).astype(F32), ((0, 6), (0, 0)))
        vwd = jnp.pad(jnp.stack([gain_temporal, bias_o, gain_mlp, bias_d]).astype(F32), ((0, 4), (0, 0)))
        pos = lax.dynamic_index_in_dim(seg_pos.reshape(NDEV, rows), ch * NWD + wd, 0, keepdims=False)
        pos = pos.reshape(rows // CHUNK, 8, CHUNK // 8).transpose(0, 2, 1).reshape(rows, 1)
        pos = jnp.broadcast_to(pos, (rows, 128))

        def like(w):
            return jax.ShapeDtypeStruct((NDEV, *w.shape), BF16)

        dma = pltpu.SemaphoreType.DMA
        ups = rows // UP
        kinds = (8, blocks + groups, 3)
        outs = pl.pallas_call(
            layer,
            out_shape=[jax.ShapeDtypeStruct((tokens, width), BF16), like(w_y), like(w_x), like(w_o), like(w_g), like(w_u), like(w_d),
                       jax.ShapeDtypeStruct((rows, model), BF16)],
            in_specs=[ANY, pl.BlockSpec(memory_space=pltpu.VMEM)] + [ANY] * 11,
            out_specs=[ANY] * 8,
            scratch_shapes=[pltpu.VMEM((rows, model), BF16), pltpu.VMEM((rows, model), F32),
                            pltpu.VMEM((NCH, rows, w_g.shape[1]), BF16), pltpu.VMEM((4, NDEV, width, LANES), BF16),
                            pltpu.VMEM((total, 16, LANES), F32), pltpu.VMEM((NCH, *vmlp.shape), F32), pltpu.VMEM((NWD, *vwd.shape), F32),
                            pltpu.VMEM((2, 2, CHUNK, LANES), F32), pltpu.VMEM((CHUNK + 24, LANES), F32),
                            pltpu.VMEM((CHUNK, LANES), F32), pltpu.VMEM((CHUNK, LANES), F32), pltpu.VMEM((CHUNK, LANES), BF16),
                            pltpu.VMEM((24, LANES), F32), pltpu.VMEM((8, LANES), F32),
                            pltpu.VMEM((total, 32, LANES), F32), pltpu.VMEM((total, 32, LANES), F32),
                            dma(kinds), dma(kinds), dma((8, DOWN)), dma((8, DOWN)), dma((4, 3, NDEV)), dma((3, NX)), dma((3, NX)), dma((7,)), dma((7,)), dma((5,)),
                            dma((total,)), dma((total,)), dma((NWD,)), dma((3, ups)), dma((3, ups)), dma((4, ups)), dma((4, ups)), dma((ups,))],
            compiler_params=pltpu.CompilerParams(has_side_effects=True, vmem_limit_bytes=VMEM_LIMIT),
            name="layer",
        )(resid_in, pos, w_y, w_x, w_o, w_g, w_u, w_d, rgate_w.reshape(-1, LANES), igate_w.reshape(-1, LANES), vch, vmlp, vwd)
        return outs[0]

    return jax.shard_map(local_layer, mesh=mesh, in_specs=specs, out_specs=row_spec, check_vma=False)
```

```python
import jax
import jax.numpy as jnp
from jax import lax
from jax.experimental import pallas as pl
from jax.experimental.pallas import tpu as pltpu
from jax.sharding import PartitionSpec as P

MESH = pl.DeviceIdType.MESH
F32, BF16 = jnp.float32, jnp.bfloat16
EPS = 1e-6
LANES = 256
CHUNK = 256
SUB = 8
EDGE = 24
ROW = 128
UP = 512
DOWN = 2
NEAR = 224
NX = 4
NWD, NCH = 4, 2
NDEV = NWD * NCH
ANY = pl.BlockSpec(memory_space=pl.ANY)
VMEM_LIMIT = 65_800_000
OWN_X, OWN_Y, OWN_P, X_P, X_Y, Y_P, Y_X, D_P = range(8)


def gelu(v):
    return 0.5 * v * (1.0 + jnp.tanh(0.7978845608028654 * (v + 0.044715 * (v * v * v))))


def sigmoid(v):
    return 1.0 / (1.0 + jnp.exp(-v))


def eight(k):
    return slice(k * SUB, (k + 1) * SUB)


def shuffle_matrix(transposed):
    rows = lax.broadcasted_iota(jnp.int32, (CHUNK, CHUNK), 0)
    cols = lax.broadcasted_iota(jnp.int32, (CHUNK, CHUNK), 1)
    out, src = (cols, rows) if transposed else (rows, cols)
    return jnp.where((out % SUB) * (CHUNK // SUB) + out // SUB == src, 1.0, 0.0).astype(BF16)


def layer(resid, seg_ref, w_y, w_x, w_o, w_g, w_u, w_d, rgate, igate, small,
          out, g_y, g_x, g_o, g_g, g_u, g_d, x_far,
          n_s, acc_s, act_s, t_w, par_s, vwd_s, pos_s, u_s, h_s, prod_s, tail_s, h0_s,
          msg_out, msg_in, ssem, rsem, dssem, drsem, tsem, osem, xssem, xrsem, pssem, prsem, lsem, mssem, mrsem, xlsem, ossem, orsem, fssem, frsem, olsem):
    ch, wd = lax.axis_index("ch"), lax.axis_index("wd")
    core = lax.rem(wd, 2)
    me = ch * NWD + wd
    wx, wp = lax.rem(wd + 2, NWD), wd + 1 - 2 * core
    dev_x, dev_y, dev_p = (0, ch, wx), (0, 1 - ch, wd), (0, ch, wp)
    own, far_x, far_y, far_d = (ch, wd), (ch, wx), (1 - ch, wd), (1 - ch, wx)
    tokens, model = n_s.shape
    width = resid.shape[1]
    blocks = w_y.shape[1] // LANES
    halves = blocks * NCH
    groups = w_g.shape[1] // LANES
    steps = tokens // CHUNK
    ups = tokens // UP
    deep = w_d.shape[0] // DOWN

    def part_of(i, size):
        return pl.ds(i * size if isinstance(i, int) else pl.multiple_of(i * size, size), size)

    def cols_of(i):
        return part_of(i, LANES)

    def wide_of(k):
        return part_of(k, width)

    x_s = act_s.at[1, pl.ds(2 * LANES, CHUNK), pl.ds(0, model)]

    def gate_area(which, side):
        return act_s.at[1, pl.ds(3 * LANES, blocks * LANES), cols_of(2 * which + side)]

    def back_tile(slot):
        return act_s.at[1, cols_of(slot), pl.ds(0, model)]

    def kept(which, slot, q):
        return act_s.at[0, part_of(q, CHUNK), cols_of(2 * which + slot)]

    def remote(src, dst, device, send, recv):
        return pltpu.make_async_remote_copy(src_ref=src, dst_ref=dst, send_sem=send, recv_sem=recv, device_id=device,
                                            device_id_type=MESH)

    def first(i):
        return [(w_y, g_y, i, False), (w_x, g_x, i, False), (w_o, g_o, i, True)]

    def second(i):
        return [(w_g, g_g, i, False), (w_u, g_u, i, False)]

    def cut(unit, owner, part):
        mine, far, i, by_rows = unit
        if by_rows:
            return mine.at[cols_of(i)] if owner is None else far.at[owner[0], cols_of(i), wide_of(owner[1])]
        base, size = (0, width) if part is None else ((0, NEAR), (NEAR, width - NEAR))[part]
        if owner is None:
            return mine.at[pl.ds(base, size), cols_of(i)]
        return far.at[owner[0], pl.ds(pl.multiple_of(owner[1] * width + base, 32), size), cols_of(i)]

    def transfer(kind, g, u, unit):
        split = not unit[-1] and unit[0] is not w_y and unit[0] is not w_x
        owner, part, device = {OWN_X: (None, None, dev_x), OWN_Y: (None, None, dev_y), OWN_P: (None, None, dev_p),
                               X_P: (far_x, None, dev_p), X_Y: (far_x, 0 if split else None, dev_y),
                               Y_P: (far_y, None, dev_p), Y_X: (far_y, 1, dev_x), D_P: (far_d, None, dev_p)}[kind]
        return remote(cut(unit, owner, part), cut(unit, owner or own, part), device, ssem.at[kind, g, u], rsem.at[kind, g, u])

    def send(g, units, kinds):
        for kind in kinds:
            for u, unit in enumerate(units):
                transfer(kind, g, u, unit).start()

    def forward(g, units):
        for u, unit in enumerate(units):
            transfer(OWN_X, g, u, unit).wait_recv()
            transfer(X_Y, g, u, unit).start()
            transfer(X_P, g, u, unit).start()
        for u, unit in enumerate(units):
            transfer(OWN_Y, g, u, unit).wait_recv()
            if len(units) == NCH:
                transfer(Y_X, g, u, unit).start()
            transfer(Y_P, g, u, unit).start()

    def relay(g, units):
        for u, unit in enumerate(units):
            transfer(X_Y, g, u, unit).wait_recv()
            if len(units) == NCH:
                transfer(Y_X, g, u, unit).wait_recv()
            transfer(D_P, g, u, unit).start()

    def ready(g, units):
        for u, unit in enumerate(units):
            for kind in (OWN_P, X_P, Y_P, D_P):
                transfer(kind, g, u, unit).wait_recv()

    def drain(g, units):
        for u, unit in enumerate(units):
            for kind in range(8):
                if len(units) == NCH or kind != Y_X:
                    transfer(kind, g, u, unit).wait_send()

    both = (OWN_X, OWN_Y, OWN_P)

    def down_piece(kind, d):
        owner, device = {OWN_X: (None, dev_x), OWN_Y: (None, dev_y), OWN_P: (None, dev_p), X_P: (far_x, dev_p),
                         Y_P: (far_y, dev_p), Y_X: (far_y, dev_x), D_P: (far_d, dev_p)}[kind]
        rows = part_of(d, deep)
        at = owner or own
        far = g_d.at[at[0], rows, wide_of(at[1])]
        return remote(w_d.at[rows] if owner is None else far, far, device, dssem.at[kind, d], drsem.at[kind, d])

    def forward_down(d):
        down_piece(OWN_Y, d).wait_recv()
        down_piece(Y_X, d).start()
        down_piece(Y_P, d).start()
        down_piece(OWN_X, d).wait_recv()
        down_piece(X_P, d).start()

    def in_tiles(j, slot):
        jj, side = j // NCH, lax.rem(j, NCH)
        return [pltpu.make_async_copy(g.at[side, :, cols_of(jj)], t_w.at[2 * u + slot, pl.ds(0, model)], tsem.at[u, slot, 0])
                for u, g in enumerate((g_y, g_x))]

    def back_tiles(j, slot):
        jj, side = j // NCH, lax.rem(j, NCH)
        return [pltpu.make_async_copy(g_o.at[side, cols_of(jj)], back_tile(slot), tsem.at[2, slot, 0])]

    def up_tiles(b, slot):
        return [pltpu.make_async_copy(g.at[c, :, cols_of(b)], t_w.at[2 * u + slot, pl.ds(c * model, model)], tsem.at[u, slot, c])
                for u, g in enumerate((g_g, g_u)) for c in range(NCH)]

    def start(copies):
        for d in copies:
            d.start()

    def wait(copies):
        for d in copies:
            d.wait()

    send(0, first(0), both)
    shared = par_s.shape[1]
    tail_rows = pl.ds(small.shape[0] - vwd_s.shape[1], vwd_s.shape[1])
    small_sends = [remote(small.at[pl.ds(0, shared)], par_s.at[ch], dev_y, pssem.at[0], prsem.at[0])]
    for p in (1, 2, 3):
        small_sends.append(remote(small.at[tail_rows], vwd_s.at[wd], (0, ch, lax.rem(wd + p, NWD)), pssem.at[p], prsem.at[p]))
    small_own = [pltpu.make_async_copy(s, d, lsem.at[i]) for i, (s, d) in enumerate(
        [(small.at[pl.ds(0, shared)], par_s.at[ch]), (small.at[tail_rows], vwd_s.at[wd]), (rgate, gate_area(0, ch)), (igate, gate_area(1, ch))])]
    start(small_sends)
    start(small_own)

    tall = w_y.shape[1]
    stay = [(w_y, act_s.at[0, pl.ds(0, width), pl.ds(0, tall)], g_y.at[ch, wide_of(wd)]),
            (w_x, act_s.at[0, pl.ds(0, width), pl.ds(tall, tall)], g_x.at[ch, wide_of(wd)]),
            (w_o, n_s.at[pl.ds(0, tall), pl.ds(0, width)], g_o.at[ch, :, wide_of(wd)]),
            (w_g, act_s.at[0, pl.ds(width, width)], g_g.at[ch, wide_of(wd)]),
            (w_u, act_s.at[0, pl.ds(2 * width, width)], g_u.at[ch, wide_of(wd)])]
    stay_in = [pltpu.make_async_copy(s, v, lsem.at[5 + i]) for i, (s, v, _) in enumerate(stay)]
    stay_out = [pltpu.make_async_copy(v, d, lsem.at[10 + i]) for i, (_, v, d) in enumerate(stay)]
    start(stay_in)

    rows_x = tokens // NX

    def x_copy(p, q):
        peer = lax.rem(wd + p, NWD)
        return remote(resid.at[pl.ds((ch * NWD + peer) * tokens + q * rows_x, rows_x)], x_far.at[pl.ds(q * rows_x, rows_x), wide_of(wd)],
                      (0, ch, peer), xssem.at[p - 1, q], xrsem.at[p - 1, q])

    for q in range(NX):
        for p in (2, 1, 3):
            x_copy(p, q).start()
    for g in range(1, blocks):
        send(g, first(g), (OWN_X,))
    forward(0, first(0))
    for c, d in zip(stay_in, stay_out):
        c.wait()
        d.start()

    def gate_over(which):
        return remote((rgate, igate)[which], gate_area(which, ch), dev_y, pssem.at[4], prsem.at[4])

    def gate_on(which):
        return remote(gate_area(which, 1 - ch), gate_area(which, 1 - ch), dev_p, pssem.at[5], prsem.at[5])

    def by_core(do):
        for which in range(2):
            @pl.when(core == which)
            def _(which=which):
                do(which)

    for g in range(1, blocks):
        send(g, first(g), (OWN_Y, OWN_P))
        if g == 1:
            by_core(lambda which: gate_over(which).start())
    send(blocks, second(0), both)
    send(blocks + 1, second(1), (OWN_X,))
    send(blocks + 2, second(2), (OWN_X,))
    wait(small_own + small_sends + stay_out)
    relay(0, first(0))
    ready(0, first(0))
    start(in_tiles(0, 0))
    start(in_tiles(1, 1))

    def wide(i):
        per = width // ROW
        first_row = vwd_s.shape[1] - 4 * per + i * per
        return jnp.concatenate([vwd_s[k, first_row + r:first_row + r + 1, :] for k in range(NWD) for r in range(per)], axis=1)

    def narrow(side, base, i):
        return jnp.concatenate([par_s[side, pl.ds(base + 2 * i + r, 1), :] for r in range(2)], axis=1)

    def channel_row(j, k):
        return narrow(lax.rem(j, NCH), 2 * blocks * k, j // NCH)

    def inner_row(side, k, b):
        return narrow(side, 2 * blocks * 10 + 2 * groups * k, b)

    def x_load(c):
        for k in range(NWD):
            @pl.when(wd == k)
            def _(k=k):
                pltpu.make_async_copy(resid.at[pl.ds(me * tokens + c * CHUNK, CHUNK)], x_s.at[:, wide_of(k)], xlsem.at[k]).start()

            @pl.when(wd != k)
            def _(k=k):
                pltpu.make_async_copy(x_far.at[part_of(c, CHUNK), wide_of(k)], x_s.at[:, wide_of(k)], xlsem.at[k]).start()

        for k in range(NWD):
            pltpu.make_async_copy(x_far.at[part_of(c, CHUNK), wide_of(k)], x_s.at[:, wide_of(k)], xlsem.at[k]).wait()

    def message(i):
        return remote(msg_out.at[i], msg_in.at[i], dev_p, mssem.at[i], mrsem.at[i])

    def project(j, q, slot):
        vals = n_s[part_of(q, CHUNK), :]
        y = jnp.dot(vals, t_w[slot, 0:model], preferred_element_type=F32) + channel_row(j, 1)
        u = jnp.dot(vals, t_w[2 + slot, 0:model], preferred_element_type=F32) + channel_row(j, 0)
        return gelu(y).astype(BF16), u.astype(BF16)

    def gate_sums(j, q, u):
        def row(i):
            return channel_row(j, i)

        pos = pos_s[part_of(q, CHUNK), :]
        pos = jnp.concatenate([pos] * (LANES // pos.shape[1]), axis=1)
        u = u.astype(F32)
        u_s[EDGE:, :] = u
        sub = lax.broadcasted_iota(jnp.int32, (SUB, LANES), 0)
        last = u[CHUNK - EDGE:, :]
        for k in range(3):
            edge = jnp.where(sub == SUB - 1, tail_s[eight(k), :], last[eight(k), :])
            u_s[eight(k), :] = pltpu.roll(edge, 1, 0)
        tail_s[:] = last
        c = row(2) + u * row(3)
        for k in range(1, 4):
            c = c + jnp.where(pos >= k, u_s[pl.ds(EDGE - SUB * k, CHUNK), :], 0.0) * row(3 + k)
        c16 = c.astype(BF16)
        gates = [gate_area(which, lax.rem(j, NCH))[cols_of(j // NCH), :] for which in range(2)]
        return c16, [jnp.dot(c16, gate, preferred_element_type=F32) for gate in gates]

    def recur(j, q, y, c16, sums):
        def row(i):
            return channel_row(j, i)

        time = CHUNK // SUB
        sub = lax.broadcasted_iota(jnp.int32, (SUB, LANES), 0)
        pos = pos_s[part_of(q, CHUNK), :]
        pos = jnp.concatenate([pos] * (LANES // pos.shape[1]), axis=1)
        rate = sigmoid(sums[0] + row(8))
        inflow = 0.5 + 0.5 * jnp.tanh(0.5 * (sums[1] + row(9)))
        log_a = rate * row(7)
        a = jnp.exp(log_a)
        scale = jnp.tanh(-log_a) * (1.0 + a * a)
        scale = scale * lax.rsqrt(jnp.maximum(scale, 1e-37))
        reset = pos == 0
        a = jnp.where(reset, 0.0, a)
        b = jnp.where(reset, 1.0, scale) * inflow * c16.astype(F32)
        h, prod = b[eight(0), :], a[eight(0), :]
        for t in range(time):
            if t:
                h = a[eight(t), :] * h + b[eight(t), :]
                prod = a[eight(t), :] * prod
            h_s[eight(t), :] = h
            prod_s[eight(t), :] = prod
        for k in (1, 2, 4):
            far = sub >= k
            h = jnp.where(far, h + prod * pltpu.roll(h, k, 0), h)
            prod = jnp.where(far, prod * pltpu.roll(prod, k, 0), prod)
        before = h0_s[:]
        ends = h + prod * before
        carry = jnp.where(sub == 0, before, pltpu.roll(ends, 1, 0))
        h0_s[:] = jnp.broadcast_to(ends[SUB - 1:, :], (SUB, LANES))
        hid = h_s[:].reshape(time, SUB, LANES) + prod_s[:].reshape(time, SUB, LANES) * carry[None]
        return (hid.reshape(CHUNK, LANES) * y.astype(F32)).astype(BF16)

    def project_back(mixed, q, slot):
        acc_s[part_of(q, CHUNK), :] += jnp.dot(mixed, back_tile(slot)[:], preferred_element_type=F32)

    wait(in_tiles(0, 0))
    mix = shuffle_matrix(False)

    @pl.loop(0, steps)
    def _(c):
        @pl.when(lax.rem(c, steps // NX) == 0)
        def _():
            for p in (1, 2, 3):
                x_copy(p, c // (steps // NX)).wait_recv()

        x_load(c)
        rows = part_of(c, CHUNK)
        vals = jnp.dot(mix, x_s[:], preferred_element_type=F32)
        scale = lax.rsqrt(jnp.mean(vals * vals, axis=1, keepdims=True) + EPS)
        n_s[rows, :] = (vals * scale * (1.0 + wide(0))).astype(BF16)
        acc_s[rows, :] = vals + wide(1)
        seq = pl.ds(me // (seg_ref.shape[1] // tokens), 1)
        here = seg_ref[seq, pl.ds(pl.multiple_of(lax.rem(me, seg_ref.shape[1] // tokens) * tokens + c * CHUNK, CHUNK), CHUNK)]
        here = jnp.broadcast_to(here, (ROW, CHUNK))
        high, low = [jnp.einsum('rc,kc->rk', mix, v.astype(F32).astype(BF16), preferred_element_type=F32) for v in (here // 64, here % 64)]
        pos_s[rows, :] = (high * 64.0 + low).astype(jnp.int32)

        @pl.when(c == steps // 2)
        def _():
            by_core(lambda which: gate_over(which).wait_recv())
            by_core(lambda which: gate_on(which).start())

        kept(0, 0, c)[:], kept(1, 0, c)[:] = project(0, c, 0)

    by_core(lambda which: gate_on(which).wait())
    back_tile(1)[:] = jnp.zeros((LANES, model), BF16)

    @pl.loop(0, steps)
    def _(q):
        kept(2, 1, q)[:] = jnp.zeros((CHUNK, LANES), BF16)

    def came(i):
        return jnp.minimum(jnp.maximum(i - 5 - i // 8, 0), 4)

    def pass_on(low, high):
        @pl.loop(low, high)
        def _(b):
            forward(blocks + b, second(b))

            @pl.when(b < 6)
            def _():
                send(blocks + b + 3, second(b + 3), both)

            @pl.when((b > 6) & (b + 2 < groups))
            def _():
                send(blocks + b + 2, second(b + 2), both)

    @pl.loop(0, halves)
    def _(i):
        slot, other = lax.rem(i, 2), lax.rem(i + 1, 2)

        pass_on(came(i + core), came(i + core + 1))

        def onward_first(of):
            for at, g in ((1, 2), (2, 3), (3, 4)):
                @pl.when((core == of) & (i == at))
                def _(at=at, g=g):
                    forward(g, first(g))
                    if at > 1:
                        send(blocks + at - 1, second(at - 1), (OWN_Y, OWN_P))

        onward_first(1)
        for g, at in ((1, 0), (2, 2), (3, 4), (4, 6)):
            @pl.when((core == 1) & (i == at))
            def _(g=g):
                if g == 1:
                    forward(g, first(g))
                relay(g, first(g))

        @pl.when((core == 1) & (i == 8))
        def _():
            relay(blocks, second(0))

        @pl.when(i < halves - 1)
        def _():
            wait(in_tiles(i + 1, other))

        @pl.when((lax.rem(i, 2) == 1) & (i < halves - 2))
        def _():
            start(in_tiles(i + 2, slot))

        start(back_tiles(i, slot))

        def middle():
            onward_first(0)

            @pl.when((core == 0) & (i == 8))
            def _():
                relay(blocks, second(0))

        @pl.when(core == 0)
        def _():
            h0_s[:] = jnp.zeros_like(h0_s)
            tail_s[:] = jnp.zeros_like(tail_s)

        @pl.when(core == 1)
        def _():
            message(i).wait_recv()
            tail_s[:] = msg_in[i, :EDGE, :]
            h0_s[:] = msg_in[i, EDGE:, :]

        @pl.loop(0, steps)
        def _(q):
            @pl.when(q == steps // 2)
            def _():
                middle()

            mixed, y, u = kept(2, other, q)[:], kept(0, slot, q)[:], kept(1, slot, q)[:]
            project_back(mixed, q, other)
            c16, sums = gate_sums(i, q, u)
            y_next, u_next = project(i + 1, q, other)
            mixed_next = recur(i, q, y, c16, sums)
            kept(2, slot, q)[:] = mixed_next
            kept(0, other, q)[:] = y_next
            kept(1, other, q)[:] = u_next

        @pl.when(core == 0)
        def _():
            msg_out[i, :EDGE, :] = tail_s[:]
            msg_out[i, EDGE:, :] = h0_s[:]
            message(i).start()

        wait(back_tiles(i, slot))

        for g in range(1, blocks):
            @pl.when(i == 2 * g - 2)
            def _(g=g):
                @pl.when(core == 0)
                def _():
                    if g == 1:
                        forward(g, first(g))
                    relay(g, first(g))

                ready(g, first(g))
                start(in_tiles(i + 2, slot))

    ready(blocks, second(0))
    start(up_tiles(0, 0))

    @pl.loop(0, steps)
    def _(c):
        project_back(kept(2, (halves - 1) % 2, c)[:], c, (halves - 1) % 2)
        rows = part_of(c, CHUNK)
        vals = acc_s[rows, :]
        scale = lax.rsqrt(jnp.mean(vals * vals, axis=1, keepdims=True) + EPS)
        n_s[rows, :] = (vals * scale * (1.0 + wide(2))).astype(BF16)
        acc_s[rows, :] = vals + wide(3)

    def rows_of(i):
        return part_of(i, UP)

    def up(i, slot, b):
        vals = n_s[rows_of(i), :]
        for c in range(NCH):
            part = slice(c * model, (c + 1) * model)
            gate = jnp.dot(vals, t_w[slot, part], preferred_element_type=F32) + inner_row(c, 0, b)
            upper = jnp.dot(vals, t_w[2 + slot, part], preferred_element_type=F32) + inner_row(c, 1, b)
            act_s[c, rows_of(i), cols_of(b)] = (gelu(gate) * upper).astype(BF16)

    def ahead(s):
        return jnp.minimum(4 + s - (s > 4).astype(jnp.int32) - (s > 7).astype(jnp.int32), groups)

    @pl.loop(0, groups)
    def _(s):
        slot = lax.rem(s, 2)
        pass_on(ahead(s), ahead(s + 1))

        @pl.when(s == 9)
        def _():
            for d in range(DOWN):
                for kind in both:
                    down_piece(kind, d).start()

        wait(up_tiles(s, slot))

        @pl.loop(0, ups)
        def _(i):
            @pl.when((i == 1) & (s + 1 < groups))
            def _():
                relay(blocks + s + 1, second(s + 1))

            @pl.when((i == 3) & (s + 1 < groups))
            def _():
                ready(blocks + s + 1, second(s + 1))
                start(up_tiles(s + 1, 1 - slot))

            up(i, slot, s)

    base = me * tokens

    def col_block(b):
        return lax.rem(wd + lax.rem(b, 2) * (1 - 2 * core) + 2 * (b // 2) + NWD, NWD)

    def wide_cols(b):
        return wide_of(col_block(b))

    def across(i):
        return remote(n_s.at[rows_of(i), wide_cols(0)], out.at[pl.ds(base + i * UP, UP)], dev_y, fssem.at[0, i], frsem.at[0, i])

    def keep(i):
        return pltpu.make_async_copy(n_s.at[rows_of(i), wide_cols(0)], out.at[pl.ds(base + i * UP, UP)], olsem.at[i])

    def direct(b, i):
        return remote(n_s.at[rows_of(i), wide_cols(b)], out.at[pl.ds(base + i * UP, UP)], (0, ch, col_block(b)),
                      ossem.at[b - 1, i], orsem.at[b - 1, i])

    def onward(b, i):
        here = pl.ds((ch * NWD + col_block(b)) * tokens + i * UP, UP)
        return remote(out.at[here], out.at[here], dev_y, fssem.at[b, i], frsem.at[b, i])

    def load_down(b, p):
        side = lax.rem(ch + p // DOWN, NCH)
        rows = part_of(lax.rem(p, DOWN), deep)
        for half in range(2):
            cols = pl.ds(pl.multiple_of(col_block(b) * width + half * LANES, LANES), LANES)
            buf = t_w.at[p, pl.ds(half * deep, deep)]
            mine = (b == 0) & (p < DOWN)

            @pl.when(mine)
            def _():
                pltpu.make_async_copy(w_d.at[rows, cols_of(half)], buf, osem.at[p, half]).start()

            @pl.when(jnp.logical_not(mine))
            def _():
                pltpu.make_async_copy(g_d.at[side, rows, cols], buf, osem.at[p, half]).start()

    def wait_down(p):
        for half in range(2):
            pltpu.make_async_copy(w_d.at[pl.ds(0, deep), cols_of(half)], t_w.at[p, pl.ds(half * deep, deep)], osem.at[p, half]).wait()

    def down(b, p, i):
        side = lax.rem(ch + p // DOWN, NCH)
        vals = act_s[side, rows_of(i), part_of(lax.rem(p, DOWN), deep)]
        both = [jnp.dot(vals, t_w[p, half * deep:(half + 1) * deep], preferred_element_type=F32) for half in range(2)]
        acc_s[rows_of(i), wide_cols(b)] += jnp.concatenate(both, axis=1)

    def next_piece(b, p):
        d = lax.rem(p, DOWN)
        near = p < DOWN
        for at, kind_near, kind_far in ((0, OWN_P, Y_P), (1, None, Y_X), (2, X_P, D_P)):
            if kind_near is not None:
                @pl.when((b == at) & near)
                def _(kind=kind_near):
                    down_piece(kind, d).wait_recv()

            @pl.when((b == at) & jnp.logical_not(near))
            def _(kind=kind_far):
                down_piece(kind, d).wait_recv()
                if kind == Y_X:
                    down_piece(D_P, d).start()

        @pl.when(b < NWD - 1)
        def _():
            load_down(b + 1, p)

    def hand_out(b, i):
        back = shuffle_matrix(True)
        for c in range(UP // CHUNK):
            rows = pl.ds(i * UP + c * CHUNK, CHUNK)
            n_s[rows, wide_cols(b)] = jnp.dot(back, acc_s[rows, wide_cols(b)].astype(BF16), preferred_element_type=F32).astype(BF16)

        @pl.when(b == 0)
        def _():
            across(i).start()
            keep(i).start()

        @pl.when(b > 0)
        def _():
            direct(b, i).start()

    load_down(0, 0)
    load_down(0, 1)

    @pl.loop(0, NWD)
    def _(b):
        @pl.loop(0, 2 * DOWN)
        def _(p):
            @pl.when((b == 0) & (p >= DOWN))
            def _():
                forward_down(p - DOWN)
                load_down(0, p)

            wait_down(p)

            @pl.loop(0, ups)
            def _(i):
                down(b, p, i)

                @pl.when(p == 2 * DOWN - 1)
                def _():
                    hand_out(b, i)

            @pl.when((b == 1) & (p == 2 * DOWN - 1))
            def _():
                for i in range(ups):
                    direct(1, i).wait_recv()
                    onward(1, i).start()

            next_piece(b, p)

    for b in (2, 3):
        for i in range(ups):
            direct(b, i).wait_recv()
            onward(b, i).start()
    for g in range(blocks):
        drain(g, first(g))

    @pl.loop(0, groups)
    def _(b):
        drain(blocks + b, second(b))

    for d in range(DOWN):
        for kind in (OWN_X, OWN_Y, OWN_P, X_P, Y_P, Y_X, D_P):
            down_piece(kind, d).wait_send()
    by_core(lambda which: gate_over(which).wait_send())
    for q in range(NX):
        for p in (1, 2, 3):
            x_copy(p, q).wait_send()

    @pl.when(core == 0)
    def _():
        @pl.loop(0, halves)
        def _(i):
            message(i).wait_send()

    for i in range(ups):
        keep(i).wait()
        across(i).wait()
        for b in (1, 2, 3):
            direct(b, i).wait_send()
            onward(b, i).wait()


def solution(mesh):
    row_spec = P("dp", "wd")
    specs = (row_spec, P("dp"), P("wd"), P("wd", "ch"), P("ch"), P("wd", "ch"), P("ch"), P(None, "ch"), P("ch"), P("ch"), P("ch"), P("ch"), P("ch"), P("ch"), P("ch", "wd"), P("wd"), P("wd"), P("wd", "ch"), P("ch"), P("wd", "ch"), P("ch"), P("ch", "wd"), P("wd"))

    def local_layer(resid_in, seg_pos, gain_temporal, w_x, bias_x, w_y, bias_y, conv_w, conv_bias, lam_param, rgate_w, rgate_b, igate_w, igate_b, w_o, bias_o, gain_mlp, w_g, bias_g, w_u, bias_u, w_d, bias_d):
        tokens, width = resid_in.shape
        model = width * NWD
        rows = tokens // NDEV
        blocks = w_x.shape[1] // LANES
        groups = w_g.shape[1] // LANES
        total = NCH * blocks
        vectors = [bias_x, bias_y, conv_bias, conv_w.reshape(-1), -8.0 * jax.nn.softplus(-lam_param), rgate_b, igate_b, bias_g, bias_u,
                   gain_temporal, bias_o, gain_mlp, bias_d]
        flat = jnp.concatenate([v.astype(F32) for v in vectors])
        shared = (10 * blocks + 2 * groups) * LANES
        tail = flat.shape[0] - shared
        lead = -(-shared // 1024) * 1024
        small = jnp.concatenate([flat[:shared], jnp.zeros((lead - shared,), F32), jnp.zeros((-(-tail // 1024) * 1024 - tail,), F32), flat[shared:]]).reshape(-1, ROW)

        def like(w, by_rows):
            return jax.ShapeDtypeStruct((NCH, w.shape[0] * (1 if by_rows else NWD), w.shape[1] * (NWD if by_rows else 1)), BF16)

        dma = pltpu.SemaphoreType.DMA
        ups = rows // UP
        kinds = (8, blocks + groups, 3)
        outs = pl.pallas_call(
            layer,
            out_shape=[jax.ShapeDtypeStruct((tokens, width), BF16), like(w_y, False), like(w_x, False), like(w_o, True), like(w_g, False), like(w_u, False), like(w_d, True),
                       jax.ShapeDtypeStruct((rows, model), BF16)],
            in_specs=[ANY, pl.BlockSpec(memory_space=pltpu.VMEM)] + [ANY] * 9,
            out_specs=[ANY] * 8,
            scratch_shapes=[pltpu.VMEM((rows, model), BF16), pltpu.VMEM((rows, model), F32),
                            pltpu.VMEM((NCH, rows, w_g.shape[1]), BF16), pltpu.VMEM((4, NCH * model, LANES), BF16),
                            pltpu.VMEM((NCH, lead // ROW, ROW), F32), pltpu.VMEM((NWD, small.shape[0] - lead // ROW, ROW), F32), pltpu.VMEM((rows, ROW), jnp.int32),
                            pltpu.VMEM((CHUNK + EDGE, LANES), F32), pltpu.VMEM((CHUNK, LANES), F32), pltpu.VMEM((CHUNK, LANES), F32),
                            pltpu.VMEM((EDGE, LANES), F32), pltpu.VMEM((SUB, LANES), F32),
                            pltpu.VMEM((total, EDGE + SUB, LANES), F32), pltpu.VMEM((total, EDGE + SUB, LANES), F32),
                            dma(kinds), dma(kinds), dma((8, DOWN)), dma((8, DOWN)), dma((3, 2, NCH)), dma((2 * DOWN, 2)), dma((3, NX)), dma((3, NX)), dma((7,)), dma((7,)), dma((15,)),
                            dma((total,)), dma((total,)), dma((NWD,)), dma((3, ups)), dma((3, ups)), dma((4, ups)), dma((4, ups)), dma((ups,))],
            compiler_params=pltpu.CompilerParams(has_side_effects=True, vmem_limit_bytes=VMEM_LIMIT),
            name="layer",
        )(resid_in, seg_pos, w_y, w_x, w_o, w_g, w_u, w_d, rgate_w.reshape(-1, LANES), igate_w.reshape(-1, LANES), small)
        return outs[0]

    return jax.shard_map(local_layer, mesh=mesh, in_specs=specs, out_specs=row_spec, check_vma=False)
```

```python
import jax
import jax.numpy as jnp
from jax import lax
from jax.experimental import pallas as pl
from jax.experimental.pallas import tpu as pltpu
from jax.sharding import PartitionSpec as P

MESH = pl.DeviceIdType.MESH
F32, BF16 = jnp.float32, jnp.bfloat16
EPS = 1e-6
LANES = 256
CHUNK = 256
SUB = 8
EDGE = 24
ROW = 128
UP = 512
DOWN = 2
NEAR = 224
NX = 4
NWD, NCH = 4, 2
NDEV = NWD * NCH
ANY = pl.BlockSpec(memory_space=pl.ANY)
VMEM_LIMIT = 65_800_000
OWN_X, OWN_Y, OWN_P, X_P, X_Y, Y_P, Y_X, D_P = range(8)


def gelu(v):
    return 0.5 * v * (1.0 + jnp.tanh(0.7978845608028654 * (v + 0.044715 * (v * v * v))))


def sigmoid(v):
    return 1.0 / (1.0 + jnp.exp(-v))


def eight(k):
    return slice(k * SUB, (k + 1) * SUB)


def shuffle_matrix(transposed):
    rows = lax.broadcasted_iota(jnp.int32, (CHUNK, CHUNK), 0)
    cols = lax.broadcasted_iota(jnp.int32, (CHUNK, CHUNK), 1)
    out, src = (cols, rows) if transposed else (rows, cols)
    return jnp.where((out % SUB) * (CHUNK // SUB) + out // SUB == src, 1.0, 0.0).astype(BF16)


def layer(resid, seg_ref, w_y, w_x, w_o, w_g, w_u, w_d, rgate, igate, small,
          out, g_y, g_x, g_o, g_g, g_u, g_d, x_far,
          n_s, acc_s, act_s, t_w, par_s, vwd_s, pos_s, u_s, h_s, prod_s, tail_s, h0_s,
          msg_out, msg_in, ssem, rsem, dssem, drsem, tsem, osem, xssem, xrsem, pssem, prsem, lsem, mssem, mrsem, xlsem, ossem, orsem, fssem, frsem, olsem):
    ch, wd = lax.axis_index("ch"), lax.axis_index("wd")
    core = lax.rem(wd, 2)
    me = ch * NWD + wd
    wx, wp = lax.rem(wd + 2, NWD), wd + 1 - 2 * core
    dev_x, dev_y, dev_p = (0, ch, wx), (0, 1 - ch, wd), (0, ch, wp)
    own, far_x, far_y, far_d = (ch, wd), (ch, wx), (1 - ch, wd), (1 - ch, wx)
    tokens, model = n_s.shape
    width = resid.shape[1]
    blocks = w_y.shape[1] // LANES
    halves = blocks * NCH
    groups = w_g.shape[1] // LANES
    steps = tokens // CHUNK
    ups = tokens // UP
    deep = w_d.shape[0] // DOWN

    def part_of(i, size):
        return pl.ds(i * size if isinstance(i, int) else pl.multiple_of(i * size, size), size)

    def cols_of(i):
        return part_of(i, LANES)

    def wide_of(k):
        return part_of(k, width)

    x_s = act_s.at[1, pl.ds(2 * LANES, CHUNK), pl.ds(0, model)]

    def gate_area(which, side):
        return act_s.at[1, pl.ds(3 * LANES, blocks * LANES), cols_of(2 * which + side)]

    def back_tile(slot):
        return act_s.at[1, cols_of(slot), pl.ds(0, model)]

    def kept(which, slot, q):
        return act_s.at[0, part_of(q, CHUNK), cols_of(2 * which + slot)]

    def remote(src, dst, device, send, recv):
        return pltpu.make_async_remote_copy(src_ref=src, dst_ref=dst, send_sem=send, recv_sem=recv, device_id=device,
                                            device_id_type=MESH)

    def first(i):
        return [(w_y, g_y, i, False), (w_x, g_x, i, False), (w_o, g_o, i, True)]

    def second(i):
        return [(w_g, g_g, i, False), (w_u, g_u, i, False)]

    def cut(unit, owner, part):
        mine, far, i, by_rows = unit
        if by_rows:
            return mine.at[cols_of(i)] if owner is None else far.at[owner[0], cols_of(i), wide_of(owner[1])]
        base, size = (0, width) if part is None else ((0, NEAR), (NEAR, width - NEAR))[part]
        if owner is None:
            return mine.at[pl.ds(base, size), cols_of(i)]
        return far.at[owner[0], pl.ds(pl.multiple_of(owner[1] * width + base, 32), size), cols_of(i)]

    def transfer(kind, g, u, unit):
        split = not unit[-1] and unit[0] is not w_y and unit[0] is not w_x
        owner, part, device = {OWN_X: (None, None, dev_x), OWN_Y: (None, None, dev_y), OWN_P: (None, None, dev_p),
                               X_P: (far_x, None, dev_p), X_Y: (far_x, 0 if split else None, dev_y),
                               Y_P: (far_y, None, dev_p), Y_X: (far_y, 1, dev_x), D_P: (far_d, None, dev_p)}[kind]
        return remote(cut(unit, owner, part), cut(unit, owner or own, part), device, ssem.at[kind, g, u], rsem.at[kind, g, u])

    def send(g, units, kinds):
        for kind in kinds:
            for u, unit in enumerate(units):
                transfer(kind, g, u, unit).start()

    def forward(g, units):
        for u, unit in enumerate(units):
            transfer(OWN_X, g, u, unit).wait_recv()
            transfer(X_Y, g, u, unit).start()
            transfer(X_P, g, u, unit).start()
        for u, unit in enumerate(units):
            transfer(OWN_Y, g, u, unit).wait_recv()
            if len(units) == NCH:
                transfer(Y_X, g, u, unit).start()
            transfer(Y_P, g, u, unit).start()

    def relay(g, units):
        for u, unit in enumerate(units):
            transfer(X_Y, g, u, unit).wait_recv()
            if len(units) == NCH:
                transfer(Y_X, g, u, unit).wait_recv()
            transfer(D_P, g, u, unit).start()

    def ready(g, units):
        for u, unit in enumerate(units):
            for kind in (OWN_P, X_P, Y_P, D_P):
                transfer(kind, g, u, unit).wait_recv()

    def drain(g, units):
        for u, unit in enumerate(units):
            for kind in range(8):
                if len(units) == NCH or kind != Y_X:
                    transfer(kind, g, u, unit).wait_send()

    both = (OWN_X, OWN_Y, OWN_P)

    def down_piece(kind, d):
        owner, device = {OWN_X: (None, dev_x), OWN_Y: (None, dev_y), OWN_P: (None, dev_p), X_P: (far_x, dev_p),
                         Y_P: (far_y, dev_p), Y_X: (far_y, dev_x), D_P: (far_d, dev_p)}[kind]
        rows = part_of(d, deep)
        at = owner or own
        far = g_d.at[at[0], rows, wide_of(at[1])]
        return remote(w_d.at[rows] if owner is None else far, far, device, dssem.at[kind, d], drsem.at[kind, d])

    def forward_down(d):
        down_piece(OWN_Y, d).wait_recv()
        down_piece(Y_X, d).start()
        down_piece(Y_P, d).start()

    def in_tiles(j, slot):
        jj, side = j // NCH, lax.rem(j, NCH)
        return [pltpu.make_async_copy(g.at[side, :, cols_of(jj)], t_w.at[2 * u + slot, pl.ds(0, model)], tsem.at[u, slot, 0])
                for u, g in enumerate((g_y, g_x))]

    def back_tiles(j, slot):
        jj, side = j // NCH, lax.rem(j, NCH)
        return [pltpu.make_async_copy(g_o.at[side, cols_of(jj)], back_tile(slot), tsem.at[2, slot, 0])]

    def up_tiles(b, slot):
        return [pltpu.make_async_copy(g.at[c, :, cols_of(b)], t_w.at[2 * u + slot, pl.ds(c * model, model)], tsem.at[u, slot, c])
                for u, g in enumerate((g_g, g_u)) for c in range(NCH)]

    def start(copies):
        for d in copies:
            d.start()

    def wait(copies):
        for d in copies:
            d.wait()

    send(0, first(0), both)
    shared = par_s.shape[1]
    tail_rows = pl.ds(small.shape[0] - vwd_s.shape[1], vwd_s.shape[1])
    send(1, first(1), (OWN_Y, OWN_P))
    small_sends = [remote(small.at[pl.ds(0, shared)], par_s.at[ch], dev_y, pssem.at[0], prsem.at[0])]
    for p in (1, 2, 3):
        small_sends.append(remote(small.at[tail_rows], vwd_s.at[wd], (0, ch, lax.rem(wd + p, NWD)), pssem.at[p], prsem.at[p]))
    small_own = [pltpu.make_async_copy(s, d, lsem.at[i]) for i, (s, d) in enumerate(
        [(small.at[pl.ds(0, shared)], par_s.at[ch]), (small.at[tail_rows], vwd_s.at[wd]), (rgate, gate_area(0, ch)), (igate, gate_area(1, ch))])]
    start(small_sends)
    start(small_own)

    tall = w_y.shape[1]
    stay = [(w_y, act_s.at[0, pl.ds(0, width), pl.ds(0, tall)], g_y.at[ch, wide_of(wd)]),
            (w_x, act_s.at[0, pl.ds(0, width), pl.ds(tall, tall)], g_x.at[ch, wide_of(wd)]),
            (w_o, n_s.at[pl.ds(0, tall), pl.ds(0, width)], g_o.at[ch, :, wide_of(wd)]),
            (w_g, act_s.at[0, pl.ds(width, width)], g_g.at[ch, wide_of(wd)]),
            (w_u, act_s.at[0, pl.ds(2 * width, width)], g_u.at[ch, wide_of(wd)])]
    stay_in = [pltpu.make_async_copy(s, v, lsem.at[5 + i]) for i, (s, v, _) in enumerate(stay)]
    stay_out = [pltpu.make_async_copy(v, d, lsem.at[10 + i]) for i, (_, v, d) in enumerate(stay)]
    start(stay_in)

    rows_x = tokens // NX

    def x_copy(p, q):
        peer = lax.rem(wd + p, NWD)
        return remote(resid.at[pl.ds((ch * NWD + peer) * tokens + q * rows_x, rows_x)], x_far.at[pl.ds(q * rows_x, rows_x), wide_of(wd)],
                      (0, ch, peer), xssem.at[p - 1, q], xrsem.at[p - 1, q])

    for q in range(NX):
        for p in (2, 1, 3):
            x_copy(p, q).start()
    for g in range(1, blocks):
        send(g, first(g), (OWN_X,))
    forward(0, first(0))
    for c, d in zip(stay_in, stay_out):
        c.wait()
        d.start()

    def gate_over(which):
        return remote((rgate, igate)[which], gate_area(which, ch), dev_y, pssem.at[4], prsem.at[4])

    def gate_on(which):
        return remote(gate_area(which, 1 - ch), gate_area(which, 1 - ch), dev_p, pssem.at[5], prsem.at[5])

    def by_core(do):
        for which in range(2):
            @pl.when(core == which)
            def _(which=which):
                do(which)

    by_core(lambda which: gate_over(which).start())
    for g in range(2, blocks):
        send(g, first(g), (OWN_Y, OWN_P))
    send(blocks, second(0), both)
    send(blocks + 1, second(1), (OWN_X,))
    send(blocks + 2, second(2), (OWN_X,))
    wait(small_own + small_sends + stay_out)
    relay(0, first(0))
    ready(0, first(0))
    start(in_tiles(0, 0))
    start(in_tiles(1, 1))

    def wide(i):
        per = width // ROW
        first_row = vwd_s.shape[1] - 4 * per + i * per
        return jnp.concatenate([vwd_s[k, first_row + r:first_row + r + 1, :] for k in range(NWD) for r in range(per)], axis=1)

    def narrow(side, base, i):
        return jnp.concatenate([par_s[side, pl.ds(base + 2 * i + r, 1), :] for r in range(2)], axis=1)

    def channel_row(j, k):
        return narrow(lax.rem(j, NCH), 2 * blocks * k, j // NCH)

    def inner_row(side, k, b):
        return narrow(side, 2 * blocks * 10 + 2 * groups * k, b)

    def x_load(c):
        for k in range(NWD):
            @pl.when(wd == k)
            def _(k=k):
                pltpu.make_async_copy(resid.at[pl.ds(me * tokens + c * CHUNK, CHUNK)], x_s.at[:, wide_of(k)], xlsem.at[k]).start()

            @pl.when(wd != k)
            def _(k=k):
                pltpu.make_async_copy(x_far.at[part_of(c, CHUNK), wide_of(k)], x_s.at[:, wide_of(k)], xlsem.at[k]).start()

        for k in range(NWD):
            pltpu.make_async_copy(x_far.at[part_of(c, CHUNK), wide_of(k)], x_s.at[:, wide_of(k)], xlsem.at[k]).wait()

    def message(i):
        return remote(msg_out.at[i], msg_in.at[i], dev_p, mssem.at[i], mrsem.at[i])

    def project(j, q, slot):
        vals = n_s[part_of(q, CHUNK), :]
        y = jnp.dot(vals, t_w[slot, 0:model], preferred_element_type=F32) + channel_row(j, 1)
        u = jnp.dot(vals, t_w[2 + slot, 0:model], preferred_element_type=F32) + channel_row(j, 0)
        return gelu(y).astype(BF16), u.astype(BF16)

    def gate_sums(j, q, u):
        def row(i):
            return channel_row(j, i)

        pos = pos_s[part_of(q, CHUNK), :]
        pos = jnp.concatenate([pos] * (LANES // pos.shape[1]), axis=1)
        u = u.astype(F32)
        u_s[EDGE:, :] = u
        sub = lax.broadcasted_iota(jnp.int32, (SUB, LANES), 0)
        last = u[CHUNK - EDGE:, :]
        for k in range(3):
            edge = jnp.where(sub == SUB - 1, tail_s[eight(k), :], last[eight(k), :])
            u_s[eight(k), :] = pltpu.roll(edge, 1, 0)
        tail_s[:] = last
        c = row(2) + u * row(3)
        for k in range(1, 4):
            c = c + jnp.where(pos >= k, u_s[pl.ds(EDGE - SUB * k, CHUNK), :], 0.0) * row(3 + k)
        c16 = c.astype(BF16)
        gates = [gate_area(which, lax.rem(j, NCH))[cols_of(j // NCH), :] for which in range(2)]
        return c16, [jnp.dot(c16, gate, preferred_element_type=F32) for gate in gates]

    def recur(j, q, y, c16, sums):
        def row(i):
            return channel_row(j, i)

        time = CHUNK // SUB
        sub = lax.broadcasted_iota(jnp.int32, (SUB, LANES), 0)
        pos = pos_s[part_of(q, CHUNK), :]
        pos = jnp.concatenate([pos] * (LANES // pos.shape[1]), axis=1)
        rate = sigmoid(sums[0] + row(8))
        inflow = 0.5 + 0.5 * jnp.tanh(0.5 * (sums[1] + row(9)))
        log_a = rate * row(7)
        a = jnp.exp(log_a)
        scale = jnp.tanh(-log_a) * (1.0 + a * a)
        scale = scale * lax.rsqrt(jnp.maximum(scale, 1e-37))
        reset = pos == 0
        a = jnp.where(reset, 0.0, a)
        b = jnp.where(reset, 1.0, scale) * inflow * c16.astype(F32)
        h, prod = b[eight(0), :], a[eight(0), :]
        for t in range(time):
            if t:
                h = a[eight(t), :] * h + b[eight(t), :]
                prod = a[eight(t), :] * prod
            h_s[eight(t), :] = h
            prod_s[eight(t), :] = prod
        for k in (1, 2, 4):
            far = sub >= k
            h = jnp.where(far, h + prod * pltpu.roll(h, k, 0), h)
            prod = jnp.where(far, prod * pltpu.roll(prod, k, 0), prod)
        before = h0_s[:]
        ends = h + prod * before
        carry = jnp.where(sub == 0, before, pltpu.roll(ends, 1, 0))
        h0_s[:] = jnp.broadcast_to(ends[SUB - 1:, :], (SUB, LANES))
        hid = h_s[:].reshape(time, SUB, LANES) + prod_s[:].reshape(time, SUB, LANES) * carry[None]
        return (hid.reshape(CHUNK, LANES) * y.astype(F32)).astype(BF16)

    def project_back(mixed, q, slot):
        acc_s[part_of(q, CHUNK), :] += jnp.dot(mixed, back_tile(slot)[:], preferred_element_type=F32)

    wait(in_tiles(0, 0))
    mix = shuffle_matrix(False)

    @pl.loop(0, steps)
    def _(c):
        @pl.when(lax.rem(c, steps // NX) == 0)
        def _():
            for p in (1, 2, 3):
                x_copy(p, c // (steps // NX)).wait_recv()

        x_load(c)
        rows = part_of(c, CHUNK)
        vals = jnp.dot(mix, x_s[:], preferred_element_type=F32)
        scale = lax.rsqrt(jnp.mean(vals * vals, axis=1, keepdims=True) + EPS)
        n_s[rows, :] = (vals * scale * (1.0 + wide(0))).astype(BF16)
        acc_s[rows, :] = vals + wide(1)
        seq = pl.ds(me // (seg_ref.shape[1] // tokens), 1)
        here = seg_ref[seq, pl.ds(pl.multiple_of(lax.rem(me, seg_ref.shape[1] // tokens) * tokens + c * CHUNK, CHUNK), CHUNK)]
        here = jnp.broadcast_to(here, (ROW, CHUNK))
        high, low = [jnp.einsum('rc,kc->rk', mix, v.astype(F32).astype(BF16), preferred_element_type=F32) for v in (here // 64, here % 64)]
        pos_s[rows, :] = (high * 64.0 + low).astype(jnp.int32)

        @pl.when(c == steps // 2)
        def _():
            by_core(lambda which: gate_over(which).wait_recv())
            by_core(lambda which: gate_on(which).start())

        kept(0, 0, c)[:], kept(1, 0, c)[:] = project(0, c, 0)

    by_core(lambda which: gate_on(which).wait())
    back_tile(1)[:] = jnp.zeros((LANES, model), BF16)

    @pl.loop(0, steps)
    def _(q):
        kept(2, 1, q)[:] = jnp.zeros((CHUNK, LANES), BF16)

    def came(i):
        return jnp.minimum(jnp.maximum(i - 5 - i // 8, 0), 4)

    def pass_on(low, high):
        @pl.loop(low, high)
        def _(b):
            forward(blocks + b, second(b))

            @pl.when(b < 6)
            def _():
                send(blocks + b + 3, second(b + 3), both)

            @pl.when((b > 6) & (b + 2 < groups))
            def _():
                send(blocks + b + 2, second(b + 2), both)

    @pl.loop(0, halves)
    def _(i):
        slot, other = lax.rem(i, 2), lax.rem(i + 1, 2)

        pass_on(came(i + core), came(i + core + 1))

        for g, at in ((1, 0), (2, 2), (3, 4), (4, 6)):
            @pl.when((core == 1) & (i == at))
            def _(g=g):
                if g == 1:
                    forward(g, first(g))
                relay(g, first(g))

        @pl.when((core == 1) & (i == 8))
        def _():
            relay(blocks, second(0))

        for g in range(2, blocks):
            @pl.when(i + core == g - 1)
            def _(g=g):
                forward(g, first(g))
                if g > 2:
                    send(blocks + g - 2, second(g - 2), (OWN_Y, OWN_P))

        @pl.when(i < halves - 1)
        def _():
            wait(in_tiles(i + 1, other))

        @pl.when((lax.rem(i, 2) == 1) & (i < halves - 2))
        def _():
            start(in_tiles(i + 2, slot))

        start(back_tiles(i, slot))

        def middle():
            @pl.when((core == 0) & (i == 8))
            def _():
                relay(blocks, second(0))

        @pl.when(core == 0)
        def _():
            h0_s[:] = jnp.zeros_like(h0_s)
            tail_s[:] = jnp.zeros_like(tail_s)

        @pl.when(core == 1)
        def _():
            message(i).wait_recv()
            tail_s[:] = msg_in[i, :EDGE, :]
            h0_s[:] = msg_in[i, EDGE:, :]

        @pl.loop(0, steps)
        def _(q):
            @pl.when(q == steps // 2)
            def _():
                middle()

            mixed, y, u = kept(2, other, q)[:], kept(0, slot, q)[:], kept(1, slot, q)[:]
            project_back(mixed, q, other)
            c16, sums = gate_sums(i, q, u)
            y_next, u_next = project(i + 1, q, other)
            mixed_next = recur(i, q, y, c16, sums)
            kept(2, slot, q)[:] = mixed_next
            kept(0, other, q)[:] = y_next
            kept(1, other, q)[:] = u_next

        @pl.when(core == 0)
        def _():
            msg_out[i, :EDGE, :] = tail_s[:]
            msg_out[i, EDGE:, :] = h0_s[:]
            message(i).start()

        wait(back_tiles(i, slot))

        for g in range(1, blocks):
            @pl.when(i == 2 * g - 2)
            def _(g=g):
                @pl.when(core == 0)
                def _():
                    if g == 1:
                        forward(g, first(g))
                    relay(g, first(g))

                ready(g, first(g))
                start(in_tiles(i + 2, slot))

    pass_on(4, 5)
    ready(blocks, second(0))
    start(up_tiles(0, 0))

    @pl.loop(0, steps)
    def _(c):
        project_back(kept(2, (halves - 1) % 2, c)[:], c, (halves - 1) % 2)
        rows = part_of(c, CHUNK)
        vals = acc_s[rows, :]
        scale = lax.rsqrt(jnp.mean(vals * vals, axis=1, keepdims=True) + EPS)
        n_s[rows, :] = (vals * scale * (1.0 + wide(2))).astype(BF16)
        acc_s[rows, :] = vals + wide(3)

    def rows_of(i):
        return part_of(i, UP)

    def up(i, slot, b):
        vals = n_s[rows_of(i), :]
        for c in range(NCH):
            part = slice(c * model, (c + 1) * model)
            gate = jnp.dot(vals, t_w[slot, part], preferred_element_type=F32) + inner_row(c, 0, b)
            upper = jnp.dot(vals, t_w[2 + slot, part], preferred_element_type=F32) + inner_row(c, 1, b)
            act_s[c, rows_of(i), cols_of(b)] = (gelu(gate) * upper).astype(BF16)

    def ahead(s):
        return jnp.minimum(5 + s - (s > 5).astype(jnp.int32) - (s > 7).astype(jnp.int32), groups)

    @pl.loop(0, groups)
    def _(s):
        slot = lax.rem(s, 2)
        pass_on(ahead(s), ahead(s + 1))

        for at, kinds, low, high in ((6, (OWN_Y, OWN_P), 0, 1), (8, (OWN_Y, OWN_P), 1, DOWN), (8, (OWN_X,), 0, DOWN)):
            @pl.when(s == at)
            def _(kinds=kinds, low=low, high=high):
                for d in range(low, high):
                    for kind in kinds:
                        down_piece(kind, d).start()

        wait(up_tiles(s, slot))

        @pl.loop(0, ups)
        def _(i):
            @pl.when((i == 1) & (s + 1 < groups))
            def _():
                relay(blocks + s + 1, second(s + 1))

            @pl.when((i == 3) & (s + 1 < groups))
            def _():
                ready(blocks + s + 1, second(s + 1))
                start(up_tiles(s + 1, 1 - slot))

            up(i, slot, s)

    base = me * tokens

    def col_block(b):
        return lax.rem(wd + lax.rem(b, 2) * (1 - 2 * core) + 2 * (b // 2) + NWD, NWD)

    def wide_cols(b):
        return wide_of(col_block(b))

    def there(q):
        return part_of(q, CHUNK), out.at[pl.ds(base + q * CHUNK, CHUNK)]

    def across(q):
        rows, place = there(q)
        return remote(n_s.at[rows, wide_cols(0)], place, dev_y, fssem.at[0, q], frsem.at[0, q])

    def keep(q):
        rows, place = there(q)
        return pltpu.make_async_copy(n_s.at[rows, wide_cols(0)], place, olsem.at[q])

    def direct(b, q):
        rows, place = there(q)
        return remote(n_s.at[rows, wide_cols(b)], place, (0, ch, col_block(b)), ossem.at[b - 1, q], orsem.at[b - 1, q])

    def onward(b, q):
        here = out.at[pl.ds((ch * NWD + col_block(b)) * tokens + q * CHUNK, CHUNK)]
        return remote(here, here, dev_y, fssem.at[b, q], frsem.at[b, q])

    def load_down(b, p):
        side = lax.rem(ch + p // DOWN, NCH)
        rows = part_of(lax.rem(p, DOWN), deep)
        for half in range(2):
            cols = pl.ds(pl.multiple_of(col_block(b) * width + half * LANES, LANES), LANES)
            buf = t_w.at[p, pl.ds(half * deep, deep)]
            mine = (b == 0) & (p < DOWN)

            @pl.when(mine)
            def _():
                pltpu.make_async_copy(w_d.at[rows, cols_of(half)], buf, osem.at[p, half]).start()

            @pl.when(jnp.logical_not(mine))
            def _():
                pltpu.make_async_copy(g_d.at[side, rows, cols], buf, osem.at[p, half]).start()

    def wait_down(p):
        for half in range(2):
            pltpu.make_async_copy(w_d.at[pl.ds(0, deep), cols_of(half)], t_w.at[p, pl.ds(half * deep, deep)], osem.at[p, half]).wait()

    def down(b, p, i):
        side = lax.rem(ch + p // DOWN, NCH)
        vals = act_s[side, rows_of(i), part_of(lax.rem(p, DOWN), deep)]
        both = [jnp.dot(vals, t_w[p, half * deep:(half + 1) * deep], preferred_element_type=F32) for half in range(2)]
        acc_s[rows_of(i), wide_cols(b)] += jnp.concatenate(both, axis=1)

    def next_piece(b, p):
        d = lax.rem(p, DOWN)
        near = p < DOWN
        for at, kind_near, kind_far in ((0, OWN_P, Y_P), (1, OWN_X, Y_X), (2, X_P, D_P)):
            for kind, here in ((kind_near, near), (kind_far, jnp.logical_not(near))):
                @pl.when((b == at) & here)
                def _(kind=kind):
                    down_piece(kind, d).wait_recv()
                    if kind in (OWN_X, Y_X):
                        down_piece(X_P if kind == OWN_X else D_P, d).start()

        @pl.when(b < NWD - 1)
        def _():
            load_down(b + 1, p)

    def hand_out(b, i):
        back = shuffle_matrix(True)
        for c in range(UP // CHUNK):
            q = i * (UP // CHUNK) + c
            rows = part_of(q, CHUNK)
            n_s[rows, wide_cols(b)] = jnp.dot(back, acc_s[rows, wide_cols(b)].astype(BF16), preferred_element_type=F32).astype(BF16)

            @pl.when(b == 0)
            def _():
                across(q).start()
                keep(q).start()

            @pl.when(b > 0)
            def _():
                direct(b, q).start()

    def pass_results(b, low, high):
        @pl.loop(low, high)
        def _(q):
            direct(b, q).wait_recv()
            onward(b, q).start()

    load_down(0, 0)
    load_down(0, 1)

    @pl.loop(0, NWD)
    def _(b):
        @pl.loop(0, 2 * DOWN)
        def _(p):
            @pl.when((b == 0) & (p >= DOWN))
            def _():
                forward_down(p - DOWN)
                load_down(0, p)

            wait_down(p)

            @pl.loop(0, ups)
            def _(i):
                down(b, p, i)

                @pl.when(p == 2 * DOWN - 1)
                def _():
                    hand_out(b, i)

            @pl.when(b != 1)
            def _():
                next_piece(b, p)

            @pl.when((b == 1) & (p == 2 * DOWN - 1))
            def _():
                pass_results(b, 0, steps)

                @pl.loop(0, p)
                def _(k):
                    next_piece(b, k)

            @pl.when((b == NWD - 1) & (p < DOWN))
            def _():
                pass_results(2, p * 2, p * 2 + 2)

            @pl.when((b == 2) & (p == 2 * DOWN - 2))
            def _():
                next_piece(b - 1, p + 1)

    pass_results(2, 2 * DOWN, steps)
    pass_results(3, 0, steps)
    for g in range(blocks):
        drain(g, first(g))

    @pl.loop(0, groups)
    def _(b):
        drain(blocks + b, second(b))

    for d in range(DOWN):
        for kind in (OWN_X, OWN_Y, OWN_P, X_P, Y_P, Y_X, D_P):
            down_piece(kind, d).wait_send()
    by_core(lambda which: gate_over(which).wait_send())
    for q in range(NX):
        for p in (1, 2, 3):
            x_copy(p, q).wait_send()

    @pl.when(core == 0)
    def _():
        @pl.loop(0, halves)
        def _(i):
            message(i).wait_send()

    @pl.loop(0, steps)
    def _(q):
        keep(q).wait()
        across(q).wait()
        for b in range(1, NWD):
            direct(b, q).wait_send()
            onward(b, q).wait()


def solution(mesh):
    row_spec = P("dp", "wd")
    specs = (row_spec, P("dp"), P("wd"), P("wd", "ch"), P("ch"), P("wd", "ch"), P("ch"), P(None, "ch"), P("ch"), P("ch"), P("ch"), P("ch"), P("ch"), P("ch"), P("ch", "wd"), P("wd"), P("wd"), P("wd", "ch"), P("ch"), P("wd", "ch"), P("ch"), P("ch", "wd"), P("wd"))

    def local_layer(resid_in, seg_pos, gain_temporal, w_x, bias_x, w_y, bias_y, conv_w, conv_bias, lam_param, rgate_w, rgate_b, igate_w, igate_b, w_o, bias_o, gain_mlp, w_g, bias_g, w_u, bias_u, w_d, bias_d):
        tokens, width = resid_in.shape
        model = width * NWD
        rows = tokens // NDEV
        blocks = w_x.shape[1] // LANES
        groups = w_g.shape[1] // LANES
        total = NCH * blocks
        vectors = [bias_x, bias_y, conv_bias, *conv_w, -8.0 * jax.nn.softplus(-lam_param), rgate_b, igate_b, bias_g, bias_u,
                   gain_temporal, bias_o, gain_mlp, bias_d]
        shared = (10 * blocks + 2 * groups) * LANES
        lead = -(-shared // 1024) * 1024
        whole = lead + 4 * width
        at, packed = 0, jnp.zeros((whole,), F32)
        for v in vectors:
            at = lead if at == shared else at
            packed = packed + lax.pad(v.astype(F32), jnp.zeros((), F32), [(at, whole - at - v.shape[0], 0)])
            at += v.shape[0]
        small = packed.reshape(-1, ROW)

        def like(w, by_rows):
            return jax.ShapeDtypeStruct((NCH, w.shape[0] * (1 if by_rows else NWD), w.shape[1] * (NWD if by_rows else 1)), BF16)

        dma = pltpu.SemaphoreType.DMA
        steps = rows // CHUNK
        kinds = (8, blocks + groups, 3)
        outs = pl.pallas_call(
            layer,
            out_shape=[jax.ShapeDtypeStruct((tokens, width), BF16), like(w_y, False), like(w_x, False), like(w_o, True), like(w_g, False), like(w_u, False), like(w_d, True),
                       jax.ShapeDtypeStruct((rows, model), BF16)],
            in_specs=[ANY, pl.BlockSpec(memory_space=pltpu.VMEM)] + [ANY] * 9,
            out_specs=[ANY] * 8,
            scratch_shapes=[pltpu.VMEM((rows, model), BF16), pltpu.VMEM((rows, model), F32),
                            pltpu.VMEM((NCH, rows, w_g.shape[1]), BF16), pltpu.VMEM((4, NCH * model, LANES), BF16),
                            pltpu.VMEM((NCH, lead // ROW, ROW), F32), pltpu.VMEM((NWD, small.shape[0] - lead // ROW, ROW), F32), pltpu.VMEM((rows, ROW), jnp.int32),
                            pltpu.VMEM((CHUNK + EDGE, LANES), F32), pltpu.VMEM((CHUNK, LANES), F32), pltpu.VMEM((CHUNK, LANES), F32),
                            pltpu.VMEM((EDGE, LANES), F32), pltpu.VMEM((SUB, LANES), F32),
                            pltpu.VMEM((total, EDGE + SUB, LANES), F32), pltpu.VMEM((total, EDGE + SUB, LANES), F32),
                            dma(kinds), dma(kinds), dma((8, DOWN)), dma((8, DOWN)), dma((3, 2, NCH)), dma((2 * DOWN, 2)), dma((3, NX)), dma((3, NX)), dma((7,)), dma((7,)), dma((15,)),
                            dma((total,)), dma((total,)), dma((NWD,)), dma((3, steps)), dma((3, steps)), dma((4, steps)), dma((4, steps)), dma((steps,))],
            compiler_params=pltpu.CompilerParams(has_side_effects=True, vmem_limit_bytes=VMEM_LIMIT),
            name="layer",
        )(resid_in, seg_pos, w_y, w_x, w_o, w_g, w_u, w_d, rgate_w.reshape(-1, LANES), igate_w.reshape(-1, LANES), small)
        return outs[0]

    return jax.shard_map(local_layer, mesh=mesh, in_specs=specs, out_specs=row_spec, check_vma=False)
```

```python
import jax
import jax.numpy as jnp
from jax import lax
from jax.experimental import pallas as pl
from jax.experimental.pallas import tpu as pltpu
from jax.sharding import PartitionSpec as P

MESH = pl.DeviceIdType.MESH
F32, BF16 = jnp.float32, jnp.bfloat16
EPS = 1e-6
LANES = 256
CHUNK = 256
SUB = 8
EDGE = 24
ROW = 128
UP = 512
DOWN = 2
NEAR = 224
NX = 4
NWD, NCH = 4, 2
NDEV = NWD * NCH
ANY = pl.BlockSpec(memory_space=pl.ANY)
VMEM_LIMIT = 65_800_000
OWN_X, OWN_Y, OWN_P, X_P, X_Y, Y_P, Y_X, D_P = range(8)


def gelu(v):
    return 0.5 * v * (1.0 + jnp.tanh(0.7978845608028654 * (v + 0.044715 * (v * v * v))))


def sigmoid(v):
    return 1.0 / (1.0 + jnp.exp(-v))


def eight(k):
    return slice(k * SUB, (k + 1) * SUB)


def shuffle_matrix(transposed):
    rows = lax.broadcasted_iota(jnp.int32, (CHUNK, CHUNK), 0)
    cols = lax.broadcasted_iota(jnp.int32, (CHUNK, CHUNK), 1)
    out, src = (cols, rows) if transposed else (rows, cols)
    return jnp.where((out % SUB) * (CHUNK // SUB) + out // SUB == src, 1.0, 0.0).astype(BF16)


def layer(resid, seg_ref, w_y, w_x, w_o, w_g, w_u, w_d, rgate, igate, bias_x, bias_y, conv_bias, conv_w, lam_param, rgate_b, igate_b, bias_g, bias_u,
          gain_temporal, bias_o, gain_mlp, bias_d,
          out, g_y, g_x, g_o, g_g, g_u, g_d, x_far,
          v_conv, v_lam, v_chan, v_inner, v_model, n_s, acc_s, act_s, t_w, par_s, vwd_s, pos_s, u_s, h_s, prod_s, tail_s, h0_s,
          msg_out, msg_in, ssem, rsem, dssem, drsem, tsem, osem, vsem, xssem, xrsem, pssem, prsem, lsem, mssem, mrsem, xlsem, ossem, orsem, fssem, frsem, olsem):
    ch, wd = lax.axis_index("ch"), lax.axis_index("wd")
    core = lax.rem(wd, 2)
    me = ch * NWD + wd
    wx, wp = lax.rem(wd + 2, NWD), wd + 1 - 2 * core
    dev_x, dev_y, dev_p = (0, ch, wx), (0, 1 - ch, wd), (0, ch, wp)
    own, far_x, far_y, far_d = (ch, wd), (ch, wx), (1 - ch, wd), (1 - ch, wx)
    tokens, model = n_s.shape
    width = resid.shape[1]
    blocks = w_y.shape[1] // LANES
    halves = blocks * NCH
    groups = w_g.shape[1] // LANES
    steps = tokens // CHUNK
    ups = tokens // UP
    deep = w_d.shape[0] // DOWN

    def part_of(i, size):
        return pl.ds(i * size if isinstance(i, int) else pl.multiple_of(i * size, size), size)

    def cols_of(i):
        return part_of(i, LANES)

    def wide_of(k):
        return part_of(k, width)

    x_s = act_s.at[1, pl.ds(2 * LANES, CHUNK), pl.ds(0, model)]

    def gate_area(which, side):
        return act_s.at[1, pl.ds(3 * LANES, blocks * LANES), cols_of(2 * which + side)]

    def back_tile(slot):
        return act_s.at[1, cols_of(slot), pl.ds(0, model)]

    def kept(which, slot, q):
        return act_s.at[0, part_of(q, CHUNK), cols_of(2 * which + slot)]

    def remote(src, dst, device, send, recv):
        return pltpu.make_async_remote_copy(src_ref=src, dst_ref=dst, send_sem=send, recv_sem=recv, device_id=device,
                                            device_id_type=MESH)

    def first(i):
        return [(w_y, g_y, i, False), (w_x, g_x, i, False), (w_o, g_o, i, True)]

    def second(i):
        return [(w_g, g_g, i, False), (w_u, g_u, i, False)]

    def cut(unit, owner, part):
        mine, far, i, by_rows = unit
        if by_rows:
            return mine.at[cols_of(i)] if owner is None else far.at[owner[0], cols_of(i), wide_of(owner[1])]
        base, size = (0, width) if part is None else ((0, NEAR), (NEAR, width - NEAR))[part]
        if owner is None:
            return mine.at[pl.ds(base, size), cols_of(i)]
        return far.at[owner[0], pl.ds(pl.multiple_of(owner[1] * width + base, 32), size), cols_of(i)]

    def transfer(kind, g, u, unit):
        split = not unit[-1] and unit[0] is not w_y and unit[0] is not w_x
        owner, part, device = {OWN_X: (None, None, dev_x), OWN_Y: (None, None, dev_y), OWN_P: (None, None, dev_p),
                               X_P: (far_x, None, dev_p), X_Y: (far_x, 0 if split else None, dev_y),
                               Y_P: (far_y, None, dev_p), Y_X: (far_y, 1, dev_x), D_P: (far_d, None, dev_p)}[kind]
        return remote(cut(unit, owner, part), cut(unit, owner or own, part), device, ssem.at[kind, g, u], rsem.at[kind, g, u])

    def send(g, units, kinds):
        for kind in kinds:
            for u, unit in enumerate(units):
                transfer(kind, g, u, unit).start()

    def forward(g, units):
        for u, unit in enumerate(units):
            transfer(OWN_X, g, u, unit).wait_recv()
            transfer(X_Y, g, u, unit).start()
            transfer(X_P, g, u, unit).start()
        for u, unit in enumerate(units):
            transfer(OWN_Y, g, u, unit).wait_recv()
            if len(units) == NCH:
                transfer(Y_X, g, u, unit).start()
            transfer(Y_P, g, u, unit).start()

    def relay(g, units):
        for u, unit in enumerate(units):
            transfer(X_Y, g, u, unit).wait_recv()
            if len(units) == NCH:
                transfer(Y_X, g, u, unit).wait_recv()
            transfer(D_P, g, u, unit).start()

    def ready(g, units):
        for u, unit in enumerate(units):
            for kind in (OWN_P, X_P, Y_P, D_P):
                transfer(kind, g, u, unit).wait_recv()

    def drain(g, units):
        for u, unit in enumerate(units):
            for kind in range(8):
                if len(units) == NCH or kind != Y_X:
                    transfer(kind, g, u, unit).wait_send()

    both = (OWN_X, OWN_Y, OWN_P)

    def down_piece(kind, d):
        owner, device = {OWN_X: (None, dev_x), OWN_Y: (None, dev_y), OWN_P: (None, dev_p), X_P: (far_x, dev_p),
                         Y_P: (far_y, dev_p), Y_X: (far_y, dev_x), D_P: (far_d, dev_p)}[kind]
        rows = part_of(d, deep)
        at = owner or own
        far = g_d.at[at[0], rows, wide_of(at[1])]
        return remote(w_d.at[rows] if owner is None else far, far, device, dssem.at[kind, d], drsem.at[kind, d])

    def forward_down(d):
        down_piece(OWN_Y, d).wait_recv()
        down_piece(Y_X, d).start()
        down_piece(Y_P, d).start()

    def in_tiles(j, slot):
        jj, side = j // NCH, lax.rem(j, NCH)
        return [pltpu.make_async_copy(g.at[side, :, cols_of(jj)], t_w.at[2 * u + slot, pl.ds(0, model)], tsem.at[u, slot, 0])
                for u, g in enumerate((g_y, g_x))]

    def back_tiles(j, slot):
        jj, side = j // NCH, lax.rem(j, NCH)
        return [pltpu.make_async_copy(g_o.at[side, cols_of(jj)], back_tile(slot), tsem.at[2, slot, 0])]

    def up_tiles(b, slot):
        return [pltpu.make_async_copy(g.at[c, :, cols_of(b)], t_w.at[2 * u + slot, pl.ds(c * model, model)], tsem.at[u, slot, c])
                for u, g in enumerate((g_g, g_u)) for c in range(NCH)]

    def start(copies):
        for d in copies:
            d.start()

    def wait(copies):
        for d in copies:
            d.wait()

    barrier = pltpu.get_barrier_semaphore()
    peers = (dev_x, dev_y, dev_p, (0, ch, lax.rem(wp + 2, NWD)))
    for device in peers:
        pl.semaphore_signal(barrier, device_id=device, device_id_type=MESH)
    pl.semaphore_wait(barrier, len(peers))

    send(0, first(0), both)
    send(1, first(1), (OWN_Y, OWN_P))
    chan_vectors = (bias_x, bias_y, conv_bias, rgate_b, igate_b)
    loads = [*zip(chan_vectors, v_chan), (conv_w, v_conv), (lam_param, v_lam), *zip((bias_g, bias_u), v_inner),
             *zip((gain_temporal, bias_o, gain_mlp, bias_d), v_model)]
    small_loads = [pltpu.make_async_copy(v, d, vsem.at[i]) for i, (v, d) in enumerate(loads)]
    small_own = [pltpu.make_async_copy(s, d, lsem.at[i]) for i, (s, d) in enumerate([(rgate, gate_area(0, ch)), (igate, gate_area(1, ch))])]
    start(small_loads)
    start(small_own)

    wait(small_loads)
    at = 0
    chan = [v[:] for v in v_chan]
    decay = -8.0 * jax.nn.softplus(-v_lam[:])
    for v in chan[:3] + [v_conv[k] for k in range(conv_w.shape[0])] + [decay] + chan[3:] + [v[:] for v in v_inner]:
        count = v.shape[0] // ROW
        par_s[ch, at:at + count, :] = v.astype(F32).reshape(count, ROW)
        at += count
    per = width // ROW
    for i, v in enumerate(v_model):
        vwd_s[wd, i * per:(i + 1) * per, :] = v[:].astype(F32).reshape(per, ROW)
    small_sends = [remote(par_s.at[ch], par_s.at[ch], dev_y, pssem.at[0], prsem.at[0])]
    for p in (1, 2, 3):
        small_sends.append(remote(vwd_s.at[wd], vwd_s.at[wd], (0, ch, lax.rem(wd + p, NWD)), pssem.at[p], prsem.at[p]))
    start(small_sends)

    tall = w_y.shape[1]
    stay = [(w_y, act_s.at[0, pl.ds(0, width), pl.ds(0, tall)], g_y.at[ch, wide_of(wd)]),
            (w_x, act_s.at[0, pl.ds(0, width), pl.ds(tall, tall)], g_x.at[ch, wide_of(wd)]),
            (w_o, n_s.at[pl.ds(0, tall), pl.ds(0, width)], g_o.at[ch, :, wide_of(wd)]),
            (w_g, act_s.at[0, pl.ds(width, width)], g_g.at[ch, wide_of(wd)]),
            (w_u, act_s.at[0, pl.ds(2 * width, width)], g_u.at[ch, wide_of(wd)])]
    stay_in = [pltpu.make_async_copy(s, v, lsem.at[5 + i]) for i, (s, v, _) in enumerate(stay)]
    stay_out = [pltpu.make_async_copy(v, d, lsem.at[10 + i]) for i, (_, v, d) in enumerate(stay)]
    start(stay_in)

    rows_x = tokens // NX

    def x_copy(p, q):
        peer = lax.rem(wd + p, NWD)
        return remote(resid.at[pl.ds((ch * NWD + peer) * tokens + q * rows_x, rows_x)], x_far.at[pl.ds(q * rows_x, rows_x), wide_of(wd)],
                      (0, ch, peer), xssem.at[p - 1, q], xrsem.at[p - 1, q])

    for q in range(NX):
        for p in (2, 1, 3):
            x_copy(p, q).start()
    for g in range(1, blocks):
        send(g, first(g), (OWN_X,))
    forward(0, first(0))
    for c, d in zip(stay_in, stay_out):
        c.wait()
        d.start()

    def gate_over(which):
        return remote((rgate, igate)[which], gate_area(which, ch), dev_y, pssem.at[4], prsem.at[4])

    def gate_on(which):
        return remote(gate_area(which, 1 - ch), gate_area(which, 1 - ch), dev_p, pssem.at[5], prsem.at[5])

    def by_core(do):
        for which in range(2):
            @pl.when(core == which)
            def _(which=which):
                do(which)

    by_core(lambda which: gate_over(which).start())
    for g in range(2, blocks):
        send(g, first(g), (OWN_Y, OWN_P))
    send(blocks, second(0), both)
    send(blocks + 1, second(1), (OWN_X,))
    send(blocks + 2, second(2), (OWN_X,))
    wait(small_own + small_sends + stay_out)
    relay(0, first(0))
    ready(0, first(0))
    start(in_tiles(0, 0))
    start(in_tiles(1, 1))

    def wide(i):
        return jnp.concatenate([vwd_s[k, i * per + r:i * per + r + 1, :] for k in range(NWD) for r in range(per)], axis=1)

    def narrow(side, base, i):
        return jnp.concatenate([par_s[side, pl.ds(base + 2 * i + r, 1), :] for r in range(2)], axis=1)

    def channel_row(j, k):
        return narrow(lax.rem(j, NCH), 2 * blocks * k, j // NCH)

    def inner_row(side, k, b):
        return narrow(side, 2 * blocks * 10 + 2 * groups * k, b)

    def x_load(c):
        for k in range(NWD):
            @pl.when(wd == k)
            def _(k=k):
                pltpu.make_async_copy(resid.at[pl.ds(me * tokens + c * CHUNK, CHUNK)], x_s.at[:, wide_of(k)], xlsem.at[k]).start()

            @pl.when(wd != k)
            def _(k=k):
                pltpu.make_async_copy(x_far.at[part_of(c, CHUNK), wide_of(k)], x_s.at[:, wide_of(k)], xlsem.at[k]).start()

        for k in range(NWD):
            pltpu.make_async_copy(x_far.at[part_of(c, CHUNK), wide_of(k)], x_s.at[:, wide_of(k)], xlsem.at[k]).wait()

    def message(i):
        return remote(msg_out.at[i], msg_in.at[i], dev_p, mssem.at[i], mrsem.at[i])

    def project(j, q, slot):
        vals = n_s[part_of(q, CHUNK), :]
        y = jnp.dot(vals, t_w[slot, 0:model], preferred_element_type=F32) + channel_row(j, 1)
        u = jnp.dot(vals, t_w[2 + slot, 0:model], preferred_element_type=F32) + channel_row(j, 0)
        return gelu(y).astype(BF16), u.astype(BF16)

    def gate_sums(j, q, u):
        def row(i):
            return channel_row(j, i)

        pos = pos_s[part_of(q, CHUNK), :]
        pos = jnp.concatenate([pos] * (LANES // pos.shape[1]), axis=1)
        u = u.astype(F32)
        u_s[EDGE:, :] = u
        sub = lax.broadcasted_iota(jnp.int32, (SUB, LANES), 0)
        last = u[CHUNK - EDGE:, :]
        for k in range(3):
            edge = jnp.where(sub == SUB - 1, tail_s[eight(k), :], last[eight(k), :])
            u_s[eight(k), :] = pltpu.roll(edge, 1, 0)
        tail_s[:] = last
        c = row(2) + u * row(3)
        for k in range(1, 4):
            c = c + jnp.where(pos >= k, u_s[pl.ds(EDGE - SUB * k, CHUNK), :], 0.0) * row(3 + k)
        c16 = c.astype(BF16)
        gates = [gate_area(which, lax.rem(j, NCH))[cols_of(j // NCH), :] for which in range(2)]
        return c16, [jnp.dot(c16, gate, preferred_element_type=F32) for gate in gates]

    def recur(j, q, y, c16, sums):
        def row(i):
            return channel_row(j, i)

        time = CHUNK // SUB
        sub = lax.broadcasted_iota(jnp.int32, (SUB, LANES), 0)
        pos = pos_s[part_of(q, CHUNK), :]
        pos = jnp.concatenate([pos] * (LANES // pos.shape[1]), axis=1)
        rate = sigmoid(sums[0] + row(8))
        inflow = 0.5 + 0.5 * jnp.tanh(0.5 * (sums[1] + row(9)))
        log_a = rate * row(7)
        a = jnp.exp(log_a)
        scale = jnp.tanh(-log_a) * (1.0 + a * a)
        scale = scale * lax.rsqrt(jnp.maximum(scale, 1e-37))
        reset = pos == 0
        a = jnp.where(reset, 0.0, a)
        b = jnp.where(reset, 1.0, scale) * inflow * c16.astype(F32)
        h, prod = b[eight(0), :], a[eight(0), :]
        for t in range(time):
            if t:
                h = a[eight(t), :] * h + b[eight(t), :]
                prod = a[eight(t), :] * prod
            h_s[eight(t), :] = h
            prod_s[eight(t), :] = prod
        for k in (1, 2, 4):
            far = sub >= k
            h = jnp.where(far, h + prod * pltpu.roll(h, k, 0), h)
            prod = jnp.where(far, prod * pltpu.roll(prod, k, 0), prod)
        before = h0_s[:]
        ends = h + prod * before
        carry = jnp.where(sub == 0, before, pltpu.roll(ends, 1, 0))
        h0_s[:] = jnp.broadcast_to(ends[SUB - 1:, :], (SUB, LANES))
        hid = h_s[:].reshape(time, SUB, LANES) + prod_s[:].reshape(time, SUB, LANES) * carry[None]
        return (hid.reshape(CHUNK, LANES) * y.astype(F32)).astype(BF16)

    def project_back(mixed, q, slot):
        acc_s[part_of(q, CHUNK), :] += jnp.dot(mixed, back_tile(slot)[:], preferred_element_type=F32)

    wait(in_tiles(0, 0))
    mix = shuffle_matrix(False)

    @pl.loop(0, steps)
    def _(c):
        @pl.when(lax.rem(c, steps // NX) == 0)
        def _():
            for p in (1, 2, 3):
                x_copy(p, c // (steps // NX)).wait_recv()

        x_load(c)
        rows = part_of(c, CHUNK)
        vals = jnp.dot(mix, x_s[:], preferred_element_type=F32)
        scale = lax.rsqrt(jnp.mean(vals * vals, axis=1, keepdims=True) + EPS)
        n_s[rows, :] = (vals * scale * (1.0 + wide(0))).astype(BF16)
        acc_s[rows, :] = vals + wide(1)
        seq = pl.ds(me // (seg_ref.shape[1] // tokens), 1)
        here = seg_ref[seq, pl.ds(pl.multiple_of(lax.rem(me, seg_ref.shape[1] // tokens) * tokens + c * CHUNK, CHUNK), CHUNK)]
        here = jnp.broadcast_to(here, (ROW, CHUNK))
        high, low = [jnp.einsum('rc,kc->rk', mix, v.astype(F32).astype(BF16), preferred_element_type=F32) for v in (here // 64, here % 64)]
        pos_s[rows, :] = (high * 64.0 + low).astype(jnp.int32)

        @pl.when(c == steps // 2)
        def _():
            by_core(lambda which: gate_over(which).wait_recv())
            by_core(lambda which: gate_on(which).start())

        kept(0, 0, c)[:], kept(1, 0, c)[:] = project(0, c, 0)

    by_core(lambda which: gate_on(which).wait())
    back_tile(1)[:] = jnp.zeros((LANES, model), BF16)

    @pl.loop(0, steps)
    def _(q):
        kept(2, 1, q)[:] = jnp.zeros((CHUNK, LANES), BF16)

    def came(i):
        return jnp.minimum(jnp.maximum(i - 5 - i // 8, 0), 4)

    def pass_on(low, high):
        @pl.loop(low, high)
        def _(b):
            forward(blocks + b, second(b))

            @pl.when(b < 6)
            def _():
                send(blocks + b + 3, second(b + 3), both)

            @pl.when((b > 6) & (b + 2 < groups))
            def _():
                send(blocks + b + 2, second(b + 2), both)

    @pl.loop(0, halves)
    def _(i):
        slot, other = lax.rem(i, 2), lax.rem(i + 1, 2)

        pass_on(came(i + core), came(i + core + 1))

        for g, at in ((1, 0), (2, 2), (3, 4), (4, 6)):
            @pl.when((core == 1) & (i == at))
            def _(g=g):
                if g == 1:
                    forward(g, first(g))
                relay(g, first(g))

        @pl.when((core == 1) & (i == 8))
        def _():
            relay(blocks, second(0))

        for g in range(2, blocks):
            @pl.when(i + core == g - 1)
            def _(g=g):
                forward(g, first(g))
                if g > 2:
                    send(blocks + g - 2, second(g - 2), (OWN_Y, OWN_P))

        @pl.when(i < halves - 1)
        def _():
            wait(in_tiles(i + 1, other))

        @pl.when((lax.rem(i, 2) == 1) & (i < halves - 2))
        def _():
            start(in_tiles(i + 2, slot))

        start(back_tiles(i, slot))

        def middle():
            @pl.when((core == 0) & (i == 8))
            def _():
                relay(blocks, second(0))

        @pl.when(core == 0)
        def _():
            h0_s[:] = jnp.zeros_like(h0_s)
            tail_s[:] = jnp.zeros_like(tail_s)

        @pl.when(core == 1)
        def _():
            message(i).wait_recv()
            tail_s[:] = msg_in[i, :EDGE, :]
            h0_s[:] = msg_in[i, EDGE:, :]

        @pl.loop(0, steps)
        def _(q):
            @pl.when(q == steps // 2)
            def _():
                middle()

            mixed, y, u = kept(2, other, q)[:], kept(0, slot, q)[:], kept(1, slot, q)[:]
            project_back(mixed, q, other)
            c16, sums = gate_sums(i, q, u)
            y_next, u_next = project(i + 1, q, other)
            mixed_next = recur(i, q, y, c16, sums)
            kept(2, slot, q)[:] = mixed_next
            kept(0, other, q)[:] = y_next
            kept(1, other, q)[:] = u_next

        @pl.when(core == 0)
        def _():
            msg_out[i, :EDGE, :] = tail_s[:]
            msg_out[i, EDGE:, :] = h0_s[:]
            message(i).start()

        wait(back_tiles(i, slot))

        for g in range(1, blocks):
            @pl.when(i == 2 * g - 2)
            def _(g=g):
                @pl.when(core == 0)
                def _():
                    if g == 1:
                        forward(g, first(g))
                    relay(g, first(g))

                ready(g, first(g))
                start(in_tiles(i + 2, slot))

    pass_on(4, 5)
    ready(blocks, second(0))
    start(up_tiles(0, 0))

    @pl.loop(0, steps)
    def _(c):
        project_back(kept(2, (halves - 1) % 2, c)[:], c, (halves - 1) % 2)
        rows = part_of(c, CHUNK)
        vals = acc_s[rows, :]
        scale = lax.rsqrt(jnp.mean(vals * vals, axis=1, keepdims=True) + EPS)
        n_s[rows, :] = (vals * scale * (1.0 + wide(2))).astype(BF16)
        acc_s[rows, :] = vals + wide(3)

    def rows_of(i):
        return part_of(i, UP)

    def up(i, slot, b):
        vals = n_s[rows_of(i), :]
        for c in range(NCH):
            part = slice(c * model, (c + 1) * model)
            gate = jnp.dot(vals, t_w[slot, part], preferred_element_type=F32) + inner_row(c, 0, b)
            upper = jnp.dot(vals, t_w[2 + slot, part], preferred_element_type=F32) + inner_row(c, 1, b)
            act_s[c, rows_of(i), cols_of(b)] = (gelu(gate) * upper).astype(BF16)

    def ahead(s):
        return jnp.minimum(5 + s - (s > 5).astype(jnp.int32) - (s > 7).astype(jnp.int32), groups)

    @pl.loop(0, groups)
    def _(s):
        slot = lax.rem(s, 2)
        pass_on(ahead(s), ahead(s + 1))

        for at, kinds, low, high in ((6, (OWN_Y, OWN_P), 0, 1), (8, (OWN_Y, OWN_P), 1, DOWN), (8, (OWN_X,), 0, DOWN)):
            @pl.when(s == at)
            def _(kinds=kinds, low=low, high=high):
                for d in range(low, high):
                    for kind in kinds:
                        down_piece(kind, d).start()

        wait(up_tiles(s, slot))

        @pl.loop(0, ups)
        def _(i):
            @pl.when((i == 1) & (s + 1 < groups))
            def _():
                relay(blocks + s + 1, second(s + 1))

            @pl.when((i == 3) & (s + 1 < groups))
            def _():
                ready(blocks + s + 1, second(s + 1))
                start(up_tiles(s + 1, 1 - slot))

            up(i, slot, s)

    base = me * tokens

    def col_block(b):
        return lax.rem(wd + lax.rem(b, 2) * (1 - 2 * core) + 2 * (b // 2) + NWD, NWD)

    def wide_cols(b):
        return wide_of(col_block(b))

    def there(q):
        return part_of(q, CHUNK), out.at[pl.ds(base + q * CHUNK, CHUNK)]

    def across(q):
        rows, place = there(q)
        return remote(n_s.at[rows, wide_cols(0)], place, dev_y, fssem.at[0, q], frsem.at[0, q])

    def keep(q):
        rows, place = there(q)
        return pltpu.make_async_copy(n_s.at[rows, wide_cols(0)], place, olsem.at[q])

    def direct(b, q):
        rows, place = there(q)
        return remote(n_s.at[rows, wide_cols(b)], place, (0, ch, col_block(b)), ossem.at[b - 1, q], orsem.at[b - 1, q])

    def onward(b, q):
        here = out.at[pl.ds((ch * NWD + col_block(b)) * tokens + q * CHUNK, CHUNK)]
        return remote(here, here, dev_y, fssem.at[b, q], frsem.at[b, q])

    def load_down(b, p):
        side = lax.rem(ch + p // DOWN, NCH)
        rows = part_of(lax.rem(p, DOWN), deep)
        for half in range(2):
            cols = pl.ds(pl.multiple_of(col_block(b) * width + half * LANES, LANES), LANES)
            buf = t_w.at[p, pl.ds(half * deep, deep)]
            mine = (b == 0) & (p < DOWN)

            @pl.when(mine)
            def _():
                pltpu.make_async_copy(w_d.at[rows, cols_of(half)], buf, osem.at[p, half]).start()

            @pl.when(jnp.logical_not(mine))
            def _():
                pltpu.make_async_copy(g_d.at[side, rows, cols], buf, osem.at[p, half]).start()

    def wait_down(p):
        for half in range(2):
            pltpu.make_async_copy(w_d.at[pl.ds(0, deep), cols_of(half)], t_w.at[p, pl.ds(half * deep, deep)], osem.at[p, half]).wait()

    def down(b, p, i):
        side = lax.rem(ch + p // DOWN, NCH)
        vals = act_s[side, rows_of(i), part_of(lax.rem(p, DOWN), deep)]
        both = [jnp.dot(vals, t_w[p, half * deep:(half + 1) * deep], preferred_element_type=F32) for half in range(2)]
        acc_s[rows_of(i), wide_cols(b)] += jnp.concatenate(both, axis=1)

    def next_piece(b, p):
        d = lax.rem(p, DOWN)
        near = p < DOWN
        for at, kind_near, kind_far in ((0, OWN_P, Y_P), (1, OWN_X, Y_X), (2, X_P, D_P)):
            for kind, here in ((kind_near, near), (kind_far, jnp.logical_not(near))):
                @pl.when((b == at) & here)
                def _(kind=kind):
                    down_piece(kind, d).wait_recv()
                    if kind in (OWN_X, Y_X):
                        down_piece(X_P if kind == OWN_X else D_P, d).start()

        @pl.when(b < NWD - 1)
        def _():
            load_down(b + 1, p)

    def hand_out(b, i):
        back = shuffle_matrix(True)
        for c in range(UP // CHUNK):
            q = i * (UP // CHUNK) + c
            rows = part_of(q, CHUNK)
            n_s[rows, wide_cols(b)] = jnp.dot(back, acc_s[rows, wide_cols(b)].astype(BF16), preferred_element_type=F32).astype(BF16)

            @pl.when(b == 0)
            def _():
                across(q).start()
                keep(q).start()

            @pl.when(b > 0)
            def _():
                direct(b, q).start()

    def pass_results(b, low, high):
        @pl.loop(low, high)
        def _(q):
            direct(b, q).wait_recv()
            onward(b, q).start()

    load_down(0, 0)
    load_down(0, 1)

    @pl.loop(0, NWD)
    def _(b):
        @pl.loop(0, 2 * DOWN)
        def _(p):
            @pl.when((b == 0) & (p >= DOWN))
            def _():
                forward_down(p - DOWN)
                load_down(0, p)

            wait_down(p)

            @pl.loop(0, ups)
            def _(i):
                down(b, p, i)

                @pl.when(p == 2 * DOWN - 1)
                def _():
                    hand_out(b, i)

            @pl.when(b != 1)
            def _():
                next_piece(b, p)

            @pl.when((b == 1) & (p == 2 * DOWN - 1))
            def _():
                pass_results(b, 0, steps)

                @pl.loop(0, p)
                def _(k):
                    next_piece(b, k)

            @pl.when((b == NWD - 1) & (p < DOWN))
            def _():
                pass_results(2, p * 2, p * 2 + 2)

            @pl.when((b == 2) & (p == 2 * DOWN - 2))
            def _():
                next_piece(b - 1, p + 1)

    pass_results(2, 2 * DOWN, steps)
    pass_results(3, 0, steps)
    for g in range(blocks):
        drain(g, first(g))

    @pl.loop(0, groups)
    def _(b):
        drain(blocks + b, second(b))

    for d in range(DOWN):
        for kind in (OWN_X, OWN_Y, OWN_P, X_P, Y_P, Y_X, D_P):
            down_piece(kind, d).wait_send()
    by_core(lambda which: gate_over(which).wait_send())
    for q in range(NX):
        for p in (1, 2, 3):
            x_copy(p, q).wait_send()

    @pl.when(core == 0)
    def _():
        @pl.loop(0, halves)
        def _(i):
            message(i).wait_send()

    @pl.loop(0, steps)
    def _(q):
        keep(q).wait()
        across(q).wait()
        for b in range(1, NWD):
            direct(b, q).wait_send()
            onward(b, q).wait()


def put_out(src, dst, buf, isem, osem):
    part = src.shape[0] // SUB
    ins = [pltpu.make_async_copy(src.at[pl.ds(k * part, part)], buf.at[pl.ds(k * part, part)], isem.at[k]) for k in range(SUB)]
    outs = [pltpu.make_async_copy(buf.at[pl.ds(k * part, part)], dst.at[pl.ds(k * part, part)], osem.at[k]) for k in range(SUB)]
    for c in ins:
        c.start()
    for c, d in zip(ins, outs):
        c.wait()
        d.start()
    for d in outs:
        d.wait()


def solution(mesh):
    row_spec = P("dp", "wd")
    specs = (row_spec, P("dp"), P("wd"), P("wd", "ch"), P("ch"), P("wd", "ch"), P("ch"), P(None, "ch"), P("ch"), P("ch"), P("ch"), P("ch"), P("ch"), P("ch"), P("ch", "wd"), P("wd"), P("wd"), P("wd", "ch"), P("ch"), P("wd", "ch"), P("ch"), P("ch", "wd"), P("wd"))

    def local_layer(resid_in, seg_pos, gain_temporal, w_x, bias_x, w_y, bias_y, conv_w, conv_bias, lam_param, rgate_w, rgate_b, igate_w, igate_b, w_o, bias_o, gain_mlp, w_g, bias_g, w_u, bias_u, w_d, bias_d):
        tokens, width = resid_in.shape
        model = width * NWD
        rows = tokens // NDEV
        blocks = w_x.shape[1] // LANES
        groups = w_g.shape[1] // LANES
        total = NCH * blocks
        vectors = (bias_x, bias_y, conv_bias, conv_w, lam_param, rgate_b, igate_b, bias_g, bias_u, gain_temporal, bias_o, gain_mlp, bias_d)
        chan, inner = w_x.shape[1], w_g.shape[1]
        shared = (10 * chan + 2 * inner) // ROW
        lead = -(-shared // SUB) * SUB

        def like(w, by_rows):
            return jax.ShapeDtypeStruct((NCH, w.shape[0] * (1 if by_rows else NWD), w.shape[1] * (NWD if by_rows else 1)), BF16)

        dma = pltpu.SemaphoreType.DMA
        steps = rows // CHUNK
        kinds = (8, blocks + groups, 3)
        outs = pl.pallas_call(
            layer,
            out_shape=[jax.ShapeDtypeStruct((tokens, width), BF16), like(w_y, False), like(w_x, False), like(w_o, True), like(w_g, False), like(w_u, False), like(w_d, True),
                       jax.ShapeDtypeStruct((rows, model), BF16)],
            in_specs=[ANY, pl.BlockSpec(memory_space=pltpu.VMEM)] + [ANY] * (8 + len(vectors)),
            out_specs=[ANY] * 8,
            scratch_shapes=[pltpu.VMEM(conv_w.shape, BF16), pltpu.VMEM((chan,), F32), [pltpu.VMEM((chan,), BF16)] * 5, [pltpu.VMEM((inner,), BF16)] * 2, [pltpu.VMEM((width,), BF16)] * 4,
                            pltpu.VMEM((rows, model), BF16), pltpu.VMEM((rows, model), F32),
                            pltpu.VMEM((NCH, rows, w_g.shape[1]), BF16), pltpu.VMEM((4, NCH * model, LANES), BF16),
                            pltpu.VMEM((NCH, lead, ROW), F32), pltpu.VMEM((NWD, 4 * width // ROW, ROW), F32), pltpu.VMEM((rows, ROW), jnp.int32),
                            pltpu.VMEM((CHUNK + EDGE, LANES), F32), pltpu.VMEM((CHUNK, LANES), F32), pltpu.VMEM((CHUNK, LANES), F32),
                            pltpu.VMEM((EDGE, LANES), F32), pltpu.VMEM((SUB, LANES), F32),
                            pltpu.VMEM((total, EDGE + SUB, LANES), F32), pltpu.VMEM((total, EDGE + SUB, LANES), F32),
                            dma(kinds), dma(kinds), dma((8, DOWN)), dma((8, DOWN)), dma((3, 2, NCH)), dma((2 * DOWN, 2)), dma((len(vectors),)), dma((3, NX)), dma((3, NX)), dma((7,)), dma((7,)), dma((15,)),
                            dma((total,)), dma((total,)), dma((NWD,)), dma((3, steps)), dma((3, steps)), dma((4, steps)), dma((4, steps)), dma((steps,))],
            compiler_params=pltpu.CompilerParams(collective_id=0, has_side_effects=True, vmem_limit_bytes=VMEM_LIMIT),
            name="layer",
        )(resid_in, seg_pos, w_y, w_x, w_o, w_g, w_u, w_d, rgate_w.reshape(-1, LANES), igate_w.reshape(-1, LANES), *vectors)
        return pl.pallas_call(
            put_out, out_shape=jax.ShapeDtypeStruct((tokens, width), BF16), in_specs=[ANY], out_specs=ANY,
            scratch_shapes=[pltpu.VMEM((tokens, width), BF16), dma((SUB,)), dma((SUB,))],
            compiler_params=pltpu.CompilerParams(vmem_limit_bytes=VMEM_LIMIT), name="put_out",
        )(outs[0])

    return jax.shard_map(local_layer, mesh=mesh, in_specs=specs, out_specs=row_spec, check_vma=False)
```

```python
import jax
import jax.numpy as jnp
from jax import lax
from jax.experimental import pallas as pl
from jax.experimental.pallas import tpu as pltpu
from jax.sharding import PartitionSpec as P

MESH = pl.DeviceIdType.MESH
F32, BF16 = jnp.float32, jnp.bfloat16
EPS = 1e-6
LANES = 256
CHUNK = 256
SUB = 8
EDGE = 24
ROW = 128
UP = 512
DOWN = 2
NEAR = 216
NX = 4
NWD, NCH = 4, 2
NDEV = NWD * NCH
ANY = pl.BlockSpec(memory_space=pl.ANY)
VMEM_LIMIT = 65_800_000
OWN_X, OWN_Y, OWN_P, X_P, X_Y, Y_P, Y_X, D_P = range(8)


def gelu(v):
    return 0.5 * v * (1.0 + jnp.tanh(0.7978845608028654 * (v + 0.044715 * (v * v * v))))


def sigmoid(v):
    return 1.0 / (1.0 + jnp.exp(-v))


def eight(k):
    return slice(k * SUB, (k + 1) * SUB)


def shuffle_matrix(transposed):
    rows = lax.broadcasted_iota(jnp.int32, (CHUNK, CHUNK), 0)
    cols = lax.broadcasted_iota(jnp.int32, (CHUNK, CHUNK), 1)
    out, src = (cols, rows) if transposed else (rows, cols)
    return jnp.where((out % SUB) * (CHUNK // SUB) + out // SUB == src, 1.0, 0.0).astype(BF16)


def layer(resid, seg_ref, w_y, w_x, w_o, w_g, w_u, w_d, rgate, igate, bias_x, bias_y, conv_bias, conv_w, lam_param, rgate_b, igate_b, bias_g, bias_u,
          gain_temporal, bias_o, gain_mlp, bias_d,
          out, g_y, g_x, g_o, g_g, g_u, g_d, x_far,
          v_conv, v_lam, v_chan, v_inner, v_model, n_s, acc_s, act_s, t_w, par_s, vwd_s, pos_s, u_s, h_s, prod_s, tail_s, h0_s,
          msg_out, msg_in, ssem, rsem, dssem, drsem, tsem, osem, vsem, xssem, xrsem, pssem, prsem, lsem, mssem, mrsem, xlsem, ossem, orsem, fssem, frsem, olsem):
    ch, wd = lax.axis_index("ch"), lax.axis_index("wd")
    core = lax.rem(wd, 2)
    me = ch * NWD + wd
    wx, wp = lax.rem(wd + 2, NWD), wd + 1 - 2 * core
    dev_x, dev_y, dev_p = (0, ch, wx), (0, 1 - ch, wd), (0, ch, wp)
    own, far_x, far_y, far_d = (ch, wd), (ch, wx), (1 - ch, wd), (1 - ch, wx)
    tokens, model = n_s.shape
    width = resid.shape[1]
    blocks = w_y.shape[1] // LANES
    halves = blocks * NCH
    groups = w_g.shape[1] // LANES
    steps = tokens // CHUNK
    ups = tokens // UP
    deep = w_d.shape[0] // DOWN

    def part_of(i, size):
        return pl.ds(i * size if isinstance(i, int) else pl.multiple_of(i * size, size), size)

    def cols_of(i):
        return part_of(i, LANES)

    def wide_of(k):
        return part_of(k, width)

    x_s = act_s.at[1, pl.ds(2 * LANES, CHUNK), pl.ds(0, model)]

    def gate_area(which, side):
        return act_s.at[1, pl.ds(3 * LANES, blocks * LANES), cols_of(2 * which + side)]

    def back_tile(slot):
        return act_s.at[1, cols_of(slot), pl.ds(0, model)]

    def kept(which, slot, q):
        return act_s.at[0, part_of(q, CHUNK), cols_of(2 * which + slot)]

    def remote(src, dst, device, send, recv):
        return pltpu.make_async_remote_copy(src_ref=src, dst_ref=dst, send_sem=send, recv_sem=recv, device_id=device,
                                            device_id_type=MESH)

    def first(i):
        return [(w_y, g_y, i, False), (w_x, g_x, i, False), (w_o, g_o, i, True)]

    def second(i):
        return [(w_g, g_g, i, False), (w_u, g_u, i, False)]

    def cut(unit, owner, part):
        mine, far, i, by_rows = unit
        if by_rows:
            return mine.at[cols_of(i)] if owner is None else far.at[owner[0], cols_of(i), wide_of(owner[1])]
        base, size = (0, width) if part is None else ((0, NEAR), (NEAR, width - NEAR))[part]
        if owner is None:
            return mine.at[pl.ds(base, size), cols_of(i)]
        return far.at[owner[0], pl.ds(pl.multiple_of(owner[1] * width + base, SUB), size), cols_of(i)]

    def transfer(kind, g, u, unit):
        split = not unit[-1] and unit[0] is not w_y and unit[0] is not w_x
        owner, part, device = {OWN_X: (None, None, dev_x), OWN_Y: (None, None, dev_y), OWN_P: (None, None, dev_p),
                               X_P: (far_x, None, dev_p), X_Y: (far_x, 0 if split else None, dev_y),
                               Y_P: (far_y, None, dev_p), Y_X: (far_y, 1, dev_x), D_P: (far_d, None, dev_p)}[kind]
        return remote(cut(unit, owner, part), cut(unit, owner or own, part), device, ssem.at[kind, g, u], rsem.at[kind, g, u])

    def send(g, units, kinds):
        for kind in kinds:
            for u, unit in enumerate(units):
                transfer(kind, g, u, unit).start()

    def forward(g, units):
        for u, unit in enumerate(units):
            transfer(OWN_X, g, u, unit).wait_recv()
            transfer(X_Y, g, u, unit).start()
            transfer(X_P, g, u, unit).start()
        for u, unit in enumerate(units):
            transfer(OWN_Y, g, u, unit).wait_recv()
            if len(units) == NCH:
                transfer(Y_X, g, u, unit).start()
            transfer(Y_P, g, u, unit).start()

    def relay(g, units):
        for u, unit in enumerate(units):
            transfer(X_Y, g, u, unit).wait_recv()
            if len(units) == NCH:
                transfer(Y_X, g, u, unit).wait_recv()
            transfer(D_P, g, u, unit).start()

    def ready(g, units):
        for u, unit in enumerate(units):
            for kind in (OWN_P, X_P, Y_P, D_P):
                transfer(kind, g, u, unit).wait_recv()

    def drain(g, units):
        for u, unit in enumerate(units):
            for kind in range(8):
                if len(units) == NCH or kind != Y_X:
                    transfer(kind, g, u, unit).wait_send()

    both = (OWN_X, OWN_Y, OWN_P)

    def down_piece(kind, d):
        owner, device = {OWN_X: (None, dev_x), OWN_Y: (None, dev_y), OWN_P: (None, dev_p), X_P: (far_x, dev_p),
                         Y_P: (far_y, dev_p), Y_X: (far_y, dev_x), D_P: (far_d, dev_p)}[kind]
        rows = part_of(d, deep)
        at = owner or own
        far = g_d.at[at[0], rows, wide_of(at[1])]
        return remote(w_d.at[rows] if owner is None else far, far, device, dssem.at[kind, d], drsem.at[kind, d])

    def forward_down(d):
        down_piece(OWN_Y, d).wait_recv()
        down_piece(Y_X, d).start()
        down_piece(Y_P, d).start()

    def in_tiles(j, slot):
        jj, side = j // NCH, lax.rem(j, NCH)
        return [pltpu.make_async_copy(g.at[side, :, cols_of(jj)], t_w.at[2 * u + slot, pl.ds(0, model)], tsem.at[u, slot, 0])
                for u, g in enumerate((g_y, g_x))]

    def back_tiles(j, slot):
        jj, side = j // NCH, lax.rem(j, NCH)
        return [pltpu.make_async_copy(g_o.at[side, cols_of(jj)], back_tile(slot), tsem.at[2, slot, 0])]

    def up_tiles(b, slot):
        return [pltpu.make_async_copy(g.at[c, :, cols_of(b)], t_w.at[2 * u + slot, pl.ds(c * model, model)], tsem.at[u, slot, c])
                for u, g in enumerate((g_g, g_u)) for c in range(NCH)]

    def start(copies):
        for d in copies:
            d.start()

    def wait(copies):
        for d in copies:
            d.wait()

    barrier = pltpu.get_barrier_semaphore()
    peers = (dev_x, dev_y, dev_p, (0, ch, lax.rem(wp + 2, NWD)))
    for device in peers:
        pl.semaphore_signal(barrier, device_id=device, device_id_type=MESH)
    pl.semaphore_wait(barrier, len(peers))

    send(0, first(0), both)
    send(1, first(1), (OWN_Y, OWN_P))
    chan_vectors = (bias_x, bias_y, conv_bias, rgate_b, igate_b)
    loads = [*zip(chan_vectors, v_chan), (conv_w, v_conv), (lam_param, v_lam), *zip((bias_g, bias_u), v_inner),
             *zip((gain_temporal, bias_o, gain_mlp, bias_d), v_model)]
    small_loads = [pltpu.make_async_copy(v, d, vsem.at[i]) for i, (v, d) in enumerate(loads)]
    small_own = [pltpu.make_async_copy(s, d, lsem.at[i]) for i, (s, d) in enumerate([(rgate, gate_area(0, ch)), (igate, gate_area(1, ch))])]
    start(small_loads)
    start(small_own)

    wait(small_loads)
    at = 0
    chan = [v[:] for v in v_chan]
    decay = -8.0 * jax.nn.softplus(-v_lam[:])
    for v in chan[:3] + [v_conv[k] for k in range(conv_w.shape[0])] + [decay] + chan[3:] + [v[:] for v in v_inner]:
        count = v.shape[0] // ROW
        par_s[ch, at:at + count, :] = v.astype(F32).reshape(count, ROW)
        at += count
    per = width // ROW
    for i, v in enumerate(v_model):
        vwd_s[wd, i * per:(i + 1) * per, :] = v[:].astype(F32).reshape(per, ROW)
    small_sends = [remote(par_s.at[ch], par_s.at[ch], dev_y, pssem.at[0], prsem.at[0])]
    for p in (1, 2, 3):
        small_sends.append(remote(vwd_s.at[wd], vwd_s.at[wd], (0, ch, lax.rem(wd + p, NWD)), pssem.at[p], prsem.at[p]))
    start(small_sends)

    tall = w_y.shape[1]
    stay = [(w_y, act_s.at[0, pl.ds(0, width), pl.ds(0, tall)], g_y.at[ch, wide_of(wd)]),
            (w_x, act_s.at[0, pl.ds(0, width), pl.ds(tall, tall)], g_x.at[ch, wide_of(wd)]),
            (w_o, n_s.at[pl.ds(0, tall), pl.ds(0, width)], g_o.at[ch, :, wide_of(wd)]),
            (w_g, act_s.at[0, pl.ds(width, width)], g_g.at[ch, wide_of(wd)]),
            (w_u, act_s.at[0, pl.ds(2 * width, width)], g_u.at[ch, wide_of(wd)])]
    stay_in = [pltpu.make_async_copy(s, v, lsem.at[5 + i]) for i, (s, v, _) in enumerate(stay)]
    stay_out = [pltpu.make_async_copy(v, d, lsem.at[10 + i]) for i, (_, v, d) in enumerate(stay)]
    start(stay_in)

    rows_x = tokens // NX

    def x_copy(p, q):
        peer = lax.rem(wd + p, NWD)
        return remote(resid.at[pl.ds((ch * NWD + peer) * tokens + q * rows_x, rows_x)], x_far.at[pl.ds(q * rows_x, rows_x), wide_of(wd)],
                      (0, ch, peer), xssem.at[p - 1, q], xrsem.at[p - 1, q])

    for q in range(NX):
        for p in (2, 1, 3):
            x_copy(p, q).start()
    for g in range(1, blocks):
        send(g, first(g), (OWN_X,))
    forward(0, first(0))
    for c, d in zip(stay_in, stay_out):
        c.wait()
        d.start()

    def gate_over(which):
        return remote((rgate, igate)[which], gate_area(which, ch), dev_y, pssem.at[4], prsem.at[4])

    def gate_on(which):
        return remote(gate_area(which, 1 - ch), gate_area(which, 1 - ch), dev_p, pssem.at[5], prsem.at[5])

    def by_core(do):
        for which in range(2):
            @pl.when(core == which)
            def _(which=which):
                do(which)

    by_core(lambda which: gate_over(which).start())
    for g in range(2, blocks):
        send(g, first(g), (OWN_Y, OWN_P))
    send(blocks, second(0), both)
    send(blocks + 1, second(1), (OWN_X,))
    send(blocks + 2, second(2), (OWN_X,))
    wait(small_own + small_sends + stay_out)
    relay(0, first(0))
    ready(0, first(0))
    start(in_tiles(0, 0))
    start(in_tiles(1, 1))

    def wide(i):
        return jnp.concatenate([vwd_s[k, i * per + r:i * per + r + 1, :] for k in range(NWD) for r in range(per)], axis=1)

    def narrow(side, base, i):
        return jnp.concatenate([par_s[side, pl.ds(base + 2 * i + r, 1), :] for r in range(2)], axis=1)

    def channel_row(j, k):
        return narrow(lax.rem(j, NCH), 2 * blocks * k, j // NCH)

    def inner_row(side, k, b):
        return narrow(side, 2 * blocks * 10 + 2 * groups * k, b)

    def x_load(c):
        for k in range(NWD):
            @pl.when(wd == k)
            def _(k=k):
                pltpu.make_async_copy(resid.at[pl.ds(me * tokens + c * CHUNK, CHUNK)], x_s.at[:, wide_of(k)], xlsem.at[k]).start()

            @pl.when(wd != k)
            def _(k=k):
                pltpu.make_async_copy(x_far.at[part_of(c, CHUNK), wide_of(k)], x_s.at[:, wide_of(k)], xlsem.at[k]).start()

        for k in range(NWD):
            pltpu.make_async_copy(x_far.at[part_of(c, CHUNK), wide_of(k)], x_s.at[:, wide_of(k)], xlsem.at[k]).wait()

    def message(i):
        return remote(msg_out.at[i], msg_in.at[i], dev_p, mssem.at[i], mrsem.at[i])

    def project(j, q, slot):
        vals = n_s[part_of(q, CHUNK), :]
        y = jnp.dot(vals, t_w[slot, 0:model], preferred_element_type=F32) + channel_row(j, 1)
        u = jnp.dot(vals, t_w[2 + slot, 0:model], preferred_element_type=F32) + channel_row(j, 0)
        return gelu(y).astype(BF16), u.astype(BF16)

    def gate_sums(j, q, u):
        def row(i):
            return channel_row(j, i)

        pos = pos_s[part_of(q, CHUNK), :]
        pos = jnp.concatenate([pos] * (LANES // pos.shape[1]), axis=1)
        u = u.astype(F32)
        u_s[EDGE:, :] = u
        sub = lax.broadcasted_iota(jnp.int32, (SUB, LANES), 0)
        last = u[CHUNK - EDGE:, :]
        for k in range(3):
            edge = jnp.where(sub == SUB - 1, tail_s[eight(k), :], last[eight(k), :])
            u_s[eight(k), :] = pltpu.roll(edge, 1, 0)
        tail_s[:] = last
        c = row(2) + u * row(3)
        for k in range(1, 4):
            c = c + jnp.where(pos >= k, u_s[pl.ds(EDGE - SUB * k, CHUNK), :], 0.0) * row(3 + k)
        c16 = c.astype(BF16)
        gates = [gate_area(which, lax.rem(j, NCH))[cols_of(j // NCH), :] for which in range(2)]
        return c16, [jnp.dot(c16, gate, preferred_element_type=F32) for gate in gates]

    def recur(j, q, y, c16, sums):
        def row(i):
            return channel_row(j, i)

        time = CHUNK // SUB
        sub = lax.broadcasted_iota(jnp.int32, (SUB, LANES), 0)
        pos = pos_s[part_of(q, CHUNK), :]
        pos = jnp.concatenate([pos] * (LANES // pos.shape[1]), axis=1)
        rate = sigmoid(sums[0] + row(8))
        inflow = 0.5 + 0.5 * jnp.tanh(0.5 * (sums[1] + row(9)))
        log_a = rate * row(7)
        a = jnp.exp(log_a)
        scale = jnp.tanh(-log_a) * (1.0 + a * a)
        scale = scale * lax.rsqrt(jnp.maximum(scale, 1e-37))
        reset = pos == 0
        a = jnp.where(reset, 0.0, a)
        b = jnp.where(reset, 1.0, scale) * inflow * c16.astype(F32)
        h, prod = b[eight(0), :], a[eight(0), :]
        for t in range(time):
            if t:
                h = a[eight(t), :] * h + b[eight(t), :]
                prod = a[eight(t), :] * prod
            h_s[eight(t), :] = h
            prod_s[eight(t), :] = prod
        for k in (1, 2, 4):
            far = sub >= k
            h = jnp.where(far, h + prod * pltpu.roll(h, k, 0), h)
            prod = jnp.where(far, prod * pltpu.roll(prod, k, 0), prod)
        before = h0_s[:]
        ends = h + prod * before
        carry = jnp.where(sub == 0, before, pltpu.roll(ends, 1, 0))
        h0_s[:] = jnp.broadcast_to(ends[SUB - 1:, :], (SUB, LANES))
        hid = h_s[:].reshape(time, SUB, LANES) + prod_s[:].reshape(time, SUB, LANES) * carry[None]
        return (hid.reshape(CHUNK, LANES) * y.astype(F32)).astype(BF16)

    def project_back(mixed, q, slot):
        acc_s[part_of(q, CHUNK), :] += jnp.dot(mixed, back_tile(slot)[:], preferred_element_type=F32)

    wait(in_tiles(0, 0))
    mix = shuffle_matrix(False)

    @pl.loop(0, steps)
    def _(c):
        @pl.when(lax.rem(c, steps // NX) == 0)
        def _():
            for p in (1, 2, 3):
                x_copy(p, c // (steps // NX)).wait_recv()

        x_load(c)
        rows = part_of(c, CHUNK)
        vals = jnp.dot(mix, x_s[:], preferred_element_type=F32)
        scale = lax.rsqrt(jnp.mean(vals * vals, axis=1, keepdims=True) + EPS)
        n_s[rows, :] = (vals * scale * (1.0 + wide(0))).astype(BF16)
        acc_s[rows, :] = vals + wide(1)
        seq = pl.ds(me // (seg_ref.shape[1] // tokens), 1)
        here = seg_ref[seq, pl.ds(pl.multiple_of(lax.rem(me, seg_ref.shape[1] // tokens) * tokens + c * CHUNK, CHUNK), CHUNK)]
        here = jnp.broadcast_to(here, (ROW, CHUNK))
        high, low = [jnp.einsum('rc,kc->rk', mix, v.astype(F32).astype(BF16), preferred_element_type=F32) for v in (here // 64, here % 64)]
        pos_s[rows, :] = (high * 64.0 + low).astype(jnp.int32)

        @pl.when(c == steps // 2)
        def _():
            by_core(lambda which: gate_over(which).wait_recv())
            by_core(lambda which: gate_on(which).start())

        kept(0, 0, c)[:], kept(1, 0, c)[:] = project(0, c, 0)

    by_core(lambda which: gate_on(which).wait())
    back_tile(1)[:] = jnp.zeros((LANES, model), BF16)

    @pl.loop(0, steps)
    def _(q):
        kept(2, 1, q)[:] = jnp.zeros((CHUNK, LANES), BF16)

    def came(i):
        return jnp.minimum(jnp.maximum(i - 5 - i // 8, 0), 4)

    def pass_on(low, high):
        @pl.loop(low, high)
        def _(b):
            forward(blocks + b, second(b))

            @pl.when(b < 6)
            def _():
                send(blocks + b + 3, second(b + 3), both)

            @pl.when((b > 6) & (b + 2 < groups))
            def _():
                send(blocks + b + 2, second(b + 2), both)

    @pl.loop(0, halves)
    def _(i):
        slot, other = lax.rem(i, 2), lax.rem(i + 1, 2)

        pass_on(came(i + core), came(i + core + 1))

        for g, at in ((1, 0), (2, 2), (3, 4), (4, 6)):
            @pl.when((core == 1) & (i == at))
            def _(g=g):
                if g == 1:
                    forward(g, first(g))
                relay(g, first(g))

        @pl.when((core == 1) & (i == 8))
        def _():
            relay(blocks, second(0))

        for g in range(2, blocks):
            @pl.when(i + core == g - 1)
            def _(g=g):
                forward(g, first(g))
                if g > 2:
                    send(blocks + g - 2, second(g - 2), (OWN_Y, OWN_P))

        @pl.when(i < halves - 1)
        def _():
            wait(in_tiles(i + 1, other))

        @pl.when((lax.rem(i, 2) == 1) & (i < halves - 2))
        def _():
            start(in_tiles(i + 2, slot))

        start(back_tiles(i, slot))

        def middle():
            @pl.when((core == 0) & (i == 8))
            def _():
                relay(blocks, second(0))

        @pl.when(core == 0)
        def _():
            h0_s[:] = jnp.zeros_like(h0_s)
            tail_s[:] = jnp.zeros_like(tail_s)

        @pl.when(core == 1)
        def _():
            message(i).wait_recv()
            tail_s[:] = msg_in[i, :EDGE, :]
            h0_s[:] = msg_in[i, EDGE:, :]

        @pl.loop(0, steps)
        def _(q):
            @pl.when(q == steps // 2)
            def _():
                middle()

            mixed, y, u = kept(2, other, q)[:], kept(0, slot, q)[:], kept(1, slot, q)[:]
            project_back(mixed, q, other)
            c16, sums = gate_sums(i, q, u)
            y_next, u_next = project(i + 1, q, other)
            mixed_next = recur(i, q, y, c16, sums)
            kept(2, slot, q)[:] = mixed_next
            kept(0, other, q)[:] = y_next
            kept(1, other, q)[:] = u_next

        @pl.when(core == 0)
        def _():
            msg_out[i, :EDGE, :] = tail_s[:]
            msg_out[i, EDGE:, :] = h0_s[:]
            message(i).start()

        wait(back_tiles(i, slot))

        for g in range(1, blocks):
            @pl.when(i == 2 * g - 2)
            def _(g=g):
                @pl.when(core == 0)
                def _():
                    if g == 1:
                        forward(g, first(g))
                    relay(g, first(g))

                ready(g, first(g))
                start(in_tiles(i + 2, slot))

    pass_on(4, 5)
    ready(blocks, second(0))
    start(up_tiles(0, 0))

    @pl.loop(0, steps)
    def _(c):
        project_back(kept(2, (halves - 1) % 2, c)[:], c, (halves - 1) % 2)
        rows = part_of(c, CHUNK)
        vals = acc_s[rows, :]
        scale = lax.rsqrt(jnp.mean(vals * vals, axis=1, keepdims=True) + EPS)
        n_s[rows, :] = (vals * scale * (1.0 + wide(2))).astype(BF16)
        acc_s[rows, :] = vals + wide(3)

    def rows_of(i):
        return part_of(i, UP)

    def up(i, slot, b):
        vals = n_s[rows_of(i), :]
        for c in range(NCH):
            part = slice(c * model, (c + 1) * model)
            gate = jnp.dot(vals, t_w[slot, part], preferred_element_type=F32) + inner_row(c, 0, b)
            upper = jnp.dot(vals, t_w[2 + slot, part], preferred_element_type=F32) + inner_row(c, 1, b)
            act_s[c, rows_of(i), cols_of(b)] = (gelu(gate) * upper).astype(BF16)

    def ahead(s):
        return jnp.minimum(5 + s - (s > 5).astype(jnp.int32), groups)

    @pl.loop(0, groups)
    def _(s):
        slot = lax.rem(s, 2)
        pass_on(ahead(s), ahead(s + 1))

        @pl.when(s == 7)
        def _():
            for d in range(DOWN):
                for kind in both:
                    down_piece(kind, d).start()

        wait(up_tiles(s, slot))

        @pl.loop(0, ups)
        def _(i):
            @pl.when((i == 1) & (s + 1 < groups))
            def _():
                relay(blocks + s + 1, second(s + 1))

            @pl.when((i == 3) & (s + 1 < groups))
            def _():
                ready(blocks + s + 1, second(s + 1))
                start(up_tiles(s + 1, 1 - slot))

            up(i, slot, s)

    base = me * tokens

    def col_block(b):
        return lax.rem(wd + lax.rem(b, 2) * (1 - 2 * core) + 2 * (b // 2) + NWD, NWD)

    def wide_cols(b):
        return wide_of(col_block(b))

    def there(q):
        return part_of(q, CHUNK), out.at[pl.ds(base + q * CHUNK, CHUNK)]

    def across(q):
        rows, place = there(q)
        return remote(n_s.at[rows, wide_cols(0)], place, dev_y, fssem.at[0, q], frsem.at[0, q])

    def keep(q):
        rows, place = there(q)
        return pltpu.make_async_copy(n_s.at[rows, wide_cols(0)], place, olsem.at[q])

    def direct(b, q):
        rows, place = there(q)
        return remote(n_s.at[rows, wide_cols(b)], place, (0, ch, col_block(b)), ossem.at[b - 1, q], orsem.at[b - 1, q])

    def onward(b, q):
        here = out.at[pl.ds((ch * NWD + col_block(b)) * tokens + q * CHUNK, CHUNK)]
        return remote(here, here, dev_y, fssem.at[b, q], frsem.at[b, q])

    def load_down(b, p):
        side = lax.rem(ch + p // DOWN, NCH)
        rows = part_of(lax.rem(p, DOWN), deep)
        for half in range(2):
            cols = pl.ds(pl.multiple_of(col_block(b) * width + half * LANES, LANES), LANES)
            buf = t_w.at[p, pl.ds(half * deep, deep)]
            mine = (b == 0) & (p < DOWN)

            @pl.when(mine)
            def _():
                pltpu.make_async_copy(w_d.at[rows, cols_of(half)], buf, osem.at[p, half]).start()

            @pl.when(jnp.logical_not(mine))
            def _():
                pltpu.make_async_copy(g_d.at[side, rows, cols], buf, osem.at[p, half]).start()

    def wait_down(p):
        for half in range(2):
            pltpu.make_async_copy(w_d.at[pl.ds(0, deep), cols_of(half)], t_w.at[p, pl.ds(half * deep, deep)], osem.at[p, half]).wait()

    def down(b, p, i):
        side = lax.rem(ch + p // DOWN, NCH)
        vals = act_s[side, rows_of(i), part_of(lax.rem(p, DOWN), deep)]
        both = [jnp.dot(vals, t_w[p, half * deep:(half + 1) * deep], preferred_element_type=F32) for half in range(2)]
        acc_s[rows_of(i), wide_cols(b)] += jnp.concatenate(both, axis=1)

    def next_piece(b, p):
        d = lax.rem(p, DOWN)
        near = p < DOWN
        for at, kind_near, kind_far in ((0, OWN_P, Y_P), (1, OWN_X, Y_X), (2, X_P, D_P)):
            for kind, here in ((kind_near, near), (kind_far, jnp.logical_not(near))):
                @pl.when((b == at) & here)
                def _(kind=kind):
                    down_piece(kind, d).wait_recv()
                    if kind in (OWN_X, Y_X):
                        down_piece(X_P if kind == OWN_X else D_P, d).start()

        @pl.when(b < NWD - 1)
        def _():
            load_down(b + 1, p)

    def hand_out(b, i):
        back = shuffle_matrix(True)
        for c in range(UP // CHUNK):
            q = i * (UP // CHUNK) + c
            rows = part_of(q, CHUNK)
            n_s[rows, wide_cols(b)] = jnp.dot(back, acc_s[rows, wide_cols(b)].astype(BF16), preferred_element_type=F32).astype(BF16)

            @pl.when(b == 0)
            def _():
                across(q).start()
                keep(q).start()

            @pl.when(b > 0)
            def _():
                direct(b, q).start()

    def pass_results(b, low, high):
        @pl.loop(low, high)
        def _(q):
            direct(b, q).wait_recv()
            onward(b, q).start()

    load_down(0, 0)
    load_down(0, 1)

    @pl.loop(0, NWD)
    def _(b):
        @pl.loop(0, 2 * DOWN)
        def _(p):
            @pl.when((b == 0) & (p >= DOWN))
            def _():
                forward_down(p - DOWN)
                load_down(0, p)

            wait_down(p)

            @pl.loop(0, ups)
            def _(i):
                down(b, p, i)

                @pl.when(p == 2 * DOWN - 1)
                def _():
                    hand_out(b, i)

            @pl.when(b != 1)
            def _():
                next_piece(b, p)

            @pl.when((b == 1) & (p == 2 * DOWN - 1))
            def _():
                pass_results(b, 0, steps)

                @pl.loop(0, p)
                def _(k):
                    next_piece(b, k)

            @pl.when((b == NWD - 1) & (p < DOWN))
            def _():
                pass_results(2, p * 2, p * 2 + 2)

            @pl.when((b == 2) & (p == 2 * DOWN - 2))
            def _():
                next_piece(b - 1, p + 1)

    pass_results(2, 2 * DOWN, steps)
    pass_results(3, 0, steps)
    for g in range(blocks):
        drain(g, first(g))

    @pl.loop(0, groups)
    def _(b):
        drain(blocks + b, second(b))

    for d in range(DOWN):
        for kind in (OWN_X, OWN_Y, OWN_P, X_P, Y_P, Y_X, D_P):
            down_piece(kind, d).wait_send()
    by_core(lambda which: gate_over(which).wait_send())
    for q in range(NX):
        for p in (1, 2, 3):
            x_copy(p, q).wait_send()

    @pl.when(core == 0)
    def _():
        @pl.loop(0, halves)
        def _(i):
            message(i).wait_send()

    @pl.loop(0, steps)
    def _(q):
        keep(q).wait()
        across(q).wait()
        for b in range(1, NWD):
            direct(b, q).wait_send()
            onward(b, q).wait()


def put_out(src, dst, buf, isem, osem):
    part = src.shape[0] // SUB
    ins = [pltpu.make_async_copy(src.at[pl.ds(k * part, part)], buf.at[pl.ds(k * part, part)], isem.at[k]) for k in range(SUB)]
    outs = [pltpu.make_async_copy(buf.at[pl.ds(k * part, part)], dst.at[pl.ds(k * part, part)], osem.at[k]) for k in range(SUB)]
    for c in ins:
        c.start()
    for c, d in zip(ins, outs):
        c.wait()
        d.start()
    for d in outs:
        d.wait()


def solution(mesh):
    row_spec = P("dp", "wd")
    specs = (row_spec, P("dp"), P("wd"), P("wd", "ch"), P("ch"), P("wd", "ch"), P("ch"), P(None, "ch"), P("ch"), P("ch"), P("ch"), P("ch"), P("ch"), P("ch"), P("ch", "wd"), P("wd"), P("wd"), P("wd", "ch"), P("ch"), P("wd", "ch"), P("ch"), P("ch", "wd"), P("wd"))

    def local_layer(resid_in, seg_pos, gain_temporal, w_x, bias_x, w_y, bias_y, conv_w, conv_bias, lam_param, rgate_w, rgate_b, igate_w, igate_b, w_o, bias_o, gain_mlp, w_g, bias_g, w_u, bias_u, w_d, bias_d):
        tokens, width = resid_in.shape
        model = width * NWD
        rows = tokens // NDEV
        blocks = w_x.shape[1] // LANES
        groups = w_g.shape[1] // LANES
        total = NCH * blocks
        vectors = (bias_x, bias_y, conv_bias, conv_w, lam_param, rgate_b, igate_b, bias_g, bias_u, gain_temporal, bias_o, gain_mlp, bias_d)
        chan, inner = w_x.shape[1], w_g.shape[1]
        shared = (10 * chan + 2 * inner) // ROW
        lead = -(-shared // SUB) * SUB

        def like(w, by_rows):
            return jax.ShapeDtypeStruct((NCH, w.shape[0] * (1 if by_rows else NWD), w.shape[1] * (NWD if by_rows else 1)), BF16)

        dma = pltpu.SemaphoreType.DMA
        steps = rows // CHUNK
        kinds = (8, blocks + groups, 3)
        outs = pl.pallas_call(
            layer,
            out_shape=[jax.ShapeDtypeStruct((tokens, width), BF16), like(w_y, False), like(w_x, False), like(w_o, True), like(w_g, False), like(w_u, False), like(w_d, True),
                       jax.ShapeDtypeStruct((rows, model), BF16)],
            in_specs=[ANY, pl.BlockSpec(memory_space=pltpu.VMEM)] + [ANY] * (8 + len(vectors)),
            out_specs=[ANY] * 8,
            scratch_shapes=[pltpu.VMEM(conv_w.shape, BF16), pltpu.VMEM((chan,), F32), [pltpu.VMEM((chan,), BF16)] * 5, [pltpu.VMEM((inner,), BF16)] * 2, [pltpu.VMEM((width,), BF16)] * 4,
                            pltpu.VMEM((rows, model), BF16), pltpu.VMEM((rows, model), F32),
                            pltpu.VMEM((NCH, rows, w_g.shape[1]), BF16), pltpu.VMEM((4, NCH * model, LANES), BF16),
                            pltpu.VMEM((NCH, lead, ROW), F32), pltpu.VMEM((NWD, 4 * width // ROW, ROW), F32), pltpu.VMEM((rows, ROW), jnp.int32),
                            pltpu.VMEM((CHUNK + EDGE, LANES), F32), pltpu.VMEM((CHUNK, LANES), F32), pltpu.VMEM((CHUNK, LANES), F32),
                            pltpu.VMEM((EDGE, LANES), F32), pltpu.VMEM((SUB, LANES), F32),
                            pltpu.VMEM((total, EDGE + SUB, LANES), F32), pltpu.VMEM((total, EDGE + SUB, LANES), F32),
                            dma(kinds), dma(kinds), dma((8, DOWN)), dma((8, DOWN)), dma((3, 2, NCH)), dma((2 * DOWN, 2)), dma((len(vectors),)), dma((3, NX)), dma((3, NX)), dma((7,)), dma((7,)), dma((15,)),
                            dma((total,)), dma((total,)), dma((NWD,)), dma((3, steps)), dma((3, steps)), dma((4, steps)), dma((4, steps)), dma((steps,))],
            compiler_params=pltpu.CompilerParams(collective_id=0, has_side_effects=True, vmem_limit_bytes=VMEM_LIMIT),
            name="layer",
        )(resid_in, seg_pos, w_y, w_x, w_o, w_g, w_u, w_d, rgate_w.reshape(-1, LANES), igate_w.reshape(-1, LANES), *vectors)
        return pl.pallas_call(
            put_out, out_shape=jax.ShapeDtypeStruct((tokens, width), BF16), in_specs=[ANY], out_specs=ANY,
            scratch_shapes=[pltpu.VMEM((tokens, width), BF16), dma((SUB,)), dma((SUB,))],
            compiler_params=pltpu.CompilerParams(vmem_limit_bytes=VMEM_LIMIT), name="put_out",
        )(outs[0])

    return jax.shard_map(local_layer, mesh=mesh, in_specs=specs, out_specs=row_spec, check_vma=False)
```

```python
import jax
import jax.numpy as jnp
from jax import lax
from jax.experimental import pallas as pl
from jax.experimental.pallas import tpu as pltpu
from jax.sharding import PartitionSpec as P

MESH = pl.DeviceIdType.MESH
F32, BF16 = jnp.float32, jnp.bfloat16
EPS = 1e-6
LANES = 256
CHUNK = 256
SUB = 8
EDGE = 24
ROW = 128
UP = 512
DOWN = 2
NEAR = 216
NX = 4
NWD, NCH = 4, 2
NDEV = NWD * NCH
ANY = pl.BlockSpec(memory_space=pl.ANY)
VMEM_LIMIT = 65_800_000
OWN_X, OWN_Y, OWN_P, X_P, X_Y, Y_P, Y_X, D_P = range(8)


def gelu(v):
    return 0.5 * v * (1.0 + jnp.tanh(0.7978845608028654 * (v + 0.044715 * (v * v * v))))


def sigmoid(v):
    return 1.0 / (1.0 + jnp.exp(-v))


def eight(k):
    return slice(k * SUB, (k + 1) * SUB)


def shuffle_matrix(transposed):
    rows = lax.broadcasted_iota(jnp.int32, (CHUNK, CHUNK), 0)
    cols = lax.broadcasted_iota(jnp.int32, (CHUNK, CHUNK), 1)
    out, src = (cols, rows) if transposed else (rows, cols)
    return jnp.where((out % SUB) * (CHUNK // SUB) + out // SUB == src, 1.0, 0.0).astype(BF16)


def layer(resid, seg_ref, w_y, w_x, w_o, w_g, w_u, w_d, rgate, igate, bias_x, bias_y, conv_bias, conv_w, lam_param, rgate_b, igate_b, bias_g, bias_u,
          gain_temporal, bias_o, gain_mlp, bias_d,
          out, g_y, g_x, g_o, g_g, g_u, g_d, x_far,
          v_conv, v_lam, v_chan, v_inner, v_model, n_s, acc_s, act_s, t_w, par_s, vwd_s, pos_s, u_s, h_s, prod_s, tail_s, h0_s,
          msg_out, msg_in, ssem, rsem_t, rsem_u, dssem, drsem, tsem, osem, vsem, xssem, xrsem, pssem, prsem, lsem, mssem, mrsem, xlsem, ossem, orsem, fssem, frsem, olsem):
    ch, wd = lax.axis_index("ch"), lax.axis_index("wd")
    core = lax.rem(wd, 2)
    me = ch * NWD + wd
    wx, wp = lax.rem(wd + 2, NWD), wd + 1 - 2 * core
    dev_x, dev_y, dev_p = (0, ch, wx), (0, 1 - ch, wd), (0, ch, wp)
    own, far_x, far_y, far_d = (ch, wd), (ch, wx), (1 - ch, wd), (1 - ch, wx)
    tokens, model = n_s.shape
    width = resid.shape[1]
    blocks = w_y.shape[1] // LANES
    halves = blocks * NCH
    groups = w_g.shape[1] // LANES
    steps = tokens // CHUNK
    ups = tokens // UP
    deep = w_d.shape[0] // DOWN

    def part_of(i, size):
        return pl.ds(i * size if isinstance(i, int) else pl.multiple_of(i * size, size), size)

    def cols_of(i):
        return part_of(i, LANES)

    def wide_of(k):
        return part_of(k, width)

    x_s = act_s.at[1, pl.ds(2 * LANES, CHUNK), pl.ds(0, model)]

    def gate_area(which, side):
        return act_s.at[1, pl.ds(3 * LANES, blocks * LANES), cols_of(2 * which + side)]

    def back_tile(slot):
        return act_s.at[1, cols_of(slot), pl.ds(0, model)]

    def kept(which, slot, q):
        return act_s.at[0, part_of(q, CHUNK), cols_of(2 * which + slot)]

    def remote(src, dst, device, send, recv):
        return pltpu.make_async_remote_copy(src_ref=src, dst_ref=dst, send_sem=send, recv_sem=recv, device_id=device,
                                            device_id_type=MESH)

    def first(i):
        return [(w_y, g_y, i, False), (w_x, g_x, i, False), (w_o, g_o, i, True)]

    def second(i):
        return [(w_g, g_g, i, False), (w_u, g_u, i, False)]

    def cut(unit, owner, part):
        mine, far, i, by_rows = unit
        if by_rows:
            return mine.at[cols_of(i)] if owner is None else far.at[owner[0], cols_of(i), wide_of(owner[1])]
        base, size = (0, width) if part is None else ((0, NEAR), (NEAR, width - NEAR))[part]
        if owner is None:
            return mine.at[pl.ds(base, size), cols_of(i)]
        return far.at[owner[0], pl.ds(pl.multiple_of(owner[1] * width + base, SUB), size), cols_of(i)]

    def transfer(kind, g, u, unit):
        split = not unit[-1] and unit[0] is not w_y and unit[0] is not w_x
        owner, part, device = {OWN_X: (None, None, dev_x), OWN_Y: (None, None, dev_y), OWN_P: (None, None, dev_p),
                               X_P: (far_x, None, dev_p), X_Y: (far_x, 0 if split else None, dev_y),
                               Y_P: (far_y, None, dev_p), Y_X: (far_y, 1, dev_x), D_P: (far_d, None, dev_p)}[kind]
        return remote(cut(unit, owner, part), cut(unit, owner or own, part), device, ssem.at[g], rsem_u.at[kind, g - blocks, u] if unit[0] is w_g or unit[0] is w_u else rsem_t.at[kind, g, u])

    def send(g, units, kinds):
        for kind in kinds:
            for u, unit in enumerate(units):
                transfer(kind, g, u, unit).start()

    def forward(g, units):
        for u, unit in enumerate(units):
            transfer(OWN_X, g, u, unit).wait_recv()
            transfer(X_Y, g, u, unit).start()
            transfer(X_P, g, u, unit).start()
        for u, unit in enumerate(units):
            transfer(OWN_Y, g, u, unit).wait_recv()
            if len(units) == NCH:
                transfer(Y_X, g, u, unit).start()
            transfer(Y_P, g, u, unit).start()

    def relay(g, units):
        for u, unit in enumerate(units):
            transfer(X_Y, g, u, unit).wait_recv()
            if len(units) == NCH:
                transfer(Y_X, g, u, unit).wait_recv()
            transfer(D_P, g, u, unit).start()

    def ready(g, units):
        for u, unit in enumerate(units):
            for kind in (OWN_P, X_P, Y_P, D_P):
                transfer(kind, g, u, unit).wait_recv()

    def sent(sem, *shape):
        bytes_of_all = g_g.at[tuple(pl.ds(0, n) for n in shape)] if len(shape) > 2 else g_g.at[0, pl.ds(0, shape[0]), pl.ds(0, shape[1])]
        remote(bytes_of_all, bytes_of_all, dev_y, sem, drsem.at[0, 0]).wait_send()

    both = (OWN_X, OWN_Y, OWN_P)

    def down_piece(kind, d):
        owner, device = {OWN_X: (None, dev_x), OWN_Y: (None, dev_y), OWN_P: (None, dev_p), X_P: (far_x, dev_p),
                         Y_P: (far_y, dev_p), Y_X: (far_y, dev_x), D_P: (far_d, dev_p)}[kind]
        rows = part_of(d, deep)
        at = owner or own
        far = g_d.at[at[0], rows, wide_of(at[1])]
        return remote(w_d.at[rows] if owner is None else far, far, device, dssem.at[0], drsem.at[kind, d])

    def forward_down(d):
        down_piece(OWN_Y, d).wait_recv()
        down_piece(Y_X, d).start()
        down_piece(Y_P, d).start()

    def in_tiles(j, slot):
        jj, side = j // NCH, lax.rem(j, NCH)
        return [pltpu.make_async_copy(g.at[side, :, cols_of(jj)], t_w.at[2 * u + slot, pl.ds(0, model)], tsem.at[u, slot, 0])
                for u, g in enumerate((g_y, g_x))]

    def back_tiles(j, slot):
        jj, side = j // NCH, lax.rem(j, NCH)
        return [pltpu.make_async_copy(g_o.at[side, cols_of(jj)], back_tile(slot), tsem.at[2, slot, 0])]

    def up_tiles(b, slot):
        return [pltpu.make_async_copy(g.at[c, :, cols_of(b)], t_w.at[2 * u + slot, pl.ds(c * model, model)], tsem.at[u, slot, c])
                for u, g in enumerate((g_g, g_u)) for c in range(NCH)]

    def start(copies):
        for d in copies:
            d.start()

    def wait(copies):
        for d in copies:
            d.wait()

    barrier = pltpu.get_barrier_semaphore()
    peers = (dev_x, dev_y, dev_p, (0, ch, lax.rem(wp + 2, NWD)))
    for device in peers:
        pl.semaphore_signal(barrier, device_id=device, device_id_type=MESH)
    pl.semaphore_wait(barrier, len(peers))

    send(0, first(0), both)
    send(1, first(1), (OWN_Y, OWN_P))
    chan_vectors = (bias_x, bias_y, conv_bias, rgate_b, igate_b)
    loads = [*zip(chan_vectors, v_chan), (conv_w, v_conv), (lam_param, v_lam), *zip((bias_g, bias_u), v_inner),
             *zip((gain_temporal, bias_o, gain_mlp, bias_d), v_model)]
    small_loads = [pltpu.make_async_copy(v, d, vsem.at[i]) for i, (v, d) in enumerate(loads)]
    small_own = [pltpu.make_async_copy(s, d, lsem.at[i]) for i, (s, d) in enumerate([(rgate, gate_area(0, ch)), (igate, gate_area(1, ch))])]
    start(small_loads)
    start(small_own)

    wait(small_loads)
    at = 0
    chan = [v[:] for v in v_chan]
    decay = -8.0 * jax.nn.softplus(-v_lam[:])
    for v in chan[:3] + [v_conv[k] for k in range(conv_w.shape[0])] + [decay] + chan[3:] + [v[:] for v in v_inner]:
        count = v.shape[0] // ROW
        par_s[ch, at:at + count, :] = v.astype(F32).reshape(count, ROW)
        at += count
    per = width // ROW
    for i, v in enumerate(v_model):
        vwd_s[wd, i * per:(i + 1) * per, :] = v[:].astype(F32).reshape(per, ROW)
    small_sends = [remote(par_s.at[ch], par_s.at[ch], dev_y, pssem.at[0], prsem.at[0])]
    for p in (1, 2, 3):
        small_sends.append(remote(vwd_s.at[wd], vwd_s.at[wd], (0, ch, lax.rem(wd + p, NWD)), pssem.at[p], prsem.at[p]))
    start(small_sends)

    tall = w_y.shape[1]
    stay = [(w_y, act_s.at[0, pl.ds(0, width), pl.ds(0, tall)], g_y.at[ch, wide_of(wd)]),
            (w_x, act_s.at[0, pl.ds(0, width), pl.ds(tall, tall)], g_x.at[ch, wide_of(wd)]),
            (w_o, n_s.at[pl.ds(0, tall), pl.ds(0, width)], g_o.at[ch, :, wide_of(wd)]),
            (w_g, act_s.at[0, pl.ds(width, width)], g_g.at[ch, wide_of(wd)]),
            (w_u, act_s.at[0, pl.ds(2 * width, width)], g_u.at[ch, wide_of(wd)])]
    stay_in = [pltpu.make_async_copy(s, v, lsem.at[5 + i]) for i, (s, v, _) in enumerate(stay)]
    stay_out = [pltpu.make_async_copy(v, d, lsem.at[10 + i]) for i, (_, v, d) in enumerate(stay)]
    start(stay_in)

    rows_x = tokens // NX

    def x_copy(p, q):
        peer = lax.rem(wd + p, NWD)
        return remote(resid.at[pl.ds((ch * NWD + peer) * tokens + q * rows_x, rows_x)], x_far.at[pl.ds(q * rows_x, rows_x), wide_of(wd)],
                      (0, ch, peer), xssem.at[0], xrsem.at[p - 1, q])

    for q in range(NX):
        for p in (2, 1, 3):
            x_copy(p, q).start()
    for g in range(1, blocks):
        send(g, first(g), (OWN_X,))
    forward(0, first(0))
    for c, d in zip(stay_in, stay_out):
        c.wait()
        d.start()

    def gate_over(which):
        return remote((rgate, igate)[which], gate_area(which, ch), dev_y, pssem.at[4], prsem.at[4])

    def gate_on(which):
        return remote(gate_area(which, 1 - ch), gate_area(which, 1 - ch), dev_p, pssem.at[5], prsem.at[5])

    def by_core(do):
        for which in range(2):
            @pl.when(core == which)
            def _(which=which):
                do(which)

    by_core(lambda which: gate_over(which).start())
    for g in range(2, blocks):
        send(g, first(g), (OWN_Y, OWN_P))
    send(blocks, second(0), both)
    send(blocks + 1, second(1), (OWN_X,))
    send(blocks + 2, second(2), (OWN_X,))
    wait(small_own + small_sends + stay_out)
    relay(0, first(0))
    ready(0, first(0))
    start(in_tiles(0, 0))
    start(in_tiles(1, 1))

    def wide(i):
        return jnp.concatenate([vwd_s[k, i * per + r:i * per + r + 1, :] for k in range(NWD) for r in range(per)], axis=1)

    def narrow(side, base, i):
        return jnp.concatenate([par_s[side, pl.ds(base + 2 * i + r, 1), :] for r in range(2)], axis=1)

    def channel_row(j, k):
        return narrow(lax.rem(j, NCH), 2 * blocks * k, j // NCH)

    def inner_row(side, k, b):
        return narrow(side, 2 * blocks * 10 + 2 * groups * k, b)

    def x_load(c):
        for k in range(NWD):
            @pl.when(wd == k)
            def _(k=k):
                pltpu.make_async_copy(resid.at[pl.ds(me * tokens + c * CHUNK, CHUNK)], x_s.at[:, wide_of(k)], xlsem.at[k]).start()

            @pl.when(wd != k)
            def _(k=k):
                pltpu.make_async_copy(x_far.at[part_of(c, CHUNK), wide_of(k)], x_s.at[:, wide_of(k)], xlsem.at[k]).start()

        for k in range(NWD):
            pltpu.make_async_copy(x_far.at[part_of(c, CHUNK), wide_of(k)], x_s.at[:, wide_of(k)], xlsem.at[k]).wait()

    def message(i):
        return remote(msg_out.at[i], msg_in.at[i], dev_p, mssem.at[i], mrsem.at[i])

    def project(j, q, slot):
        vals = n_s[part_of(q, CHUNK), :]
        y = jnp.dot(vals, t_w[slot, 0:model], preferred_element_type=F32) + channel_row(j, 1)
        u = jnp.dot(vals, t_w[2 + slot, 0:model], preferred_element_type=F32) + channel_row(j, 0)
        return gelu(y).astype(BF16), u.astype(BF16)

    def gate_sums(j, q, u):
        def row(i):
            return channel_row(j, i)

        pos = pos_s[part_of(q, CHUNK), :]
        pos = jnp.concatenate([pos] * (LANES // pos.shape[1]), axis=1)
        u = u.astype(F32)
        u_s[EDGE:, :] = u
        sub = lax.broadcasted_iota(jnp.int32, (SUB, LANES), 0)
        last = u[CHUNK - EDGE:, :]
        for k in range(3):
            edge = jnp.where(sub == SUB - 1, tail_s[eight(k), :], last[eight(k), :])
            u_s[eight(k), :] = pltpu.roll(edge, 1, 0)
        tail_s[:] = last
        c = row(2) + u * row(3)
        for k in range(1, 4):
            c = c + jnp.where(pos >= k, u_s[pl.ds(EDGE - SUB * k, CHUNK), :], 0.0) * row(3 + k)
        c16 = c.astype(BF16)
        gates = [gate_area(which, lax.rem(j, NCH))[cols_of(j // NCH), :] for which in range(2)]
        return c16, [jnp.dot(c16, gate, preferred_element_type=F32) for gate in gates]

    def recur(j, q, y, c16, sums):
        def row(i):
            return channel_row(j, i)

        time = CHUNK // SUB
        sub = lax.broadcasted_iota(jnp.int32, (SUB, LANES), 0)
        pos = pos_s[part_of(q, CHUNK), :]
        pos = jnp.concatenate([pos] * (LANES // pos.shape[1]), axis=1)
        rate = sigmoid(sums[0] + row(8))
        inflow = 0.5 + 0.5 * jnp.tanh(0.5 * (sums[1] + row(9)))
        log_a = rate * row(7)
        a = jnp.exp(log_a)
        scale = jnp.tanh(-log_a) * (1.0 + a * a)
        scale = scale * lax.rsqrt(jnp.maximum(scale, 1e-37))
        reset = pos == 0
        a = jnp.where(reset, 0.0, a)
        b = jnp.where(reset, 1.0, scale) * inflow * c16.astype(F32)
        h, prod = b[eight(0), :], a[eight(0), :]
        for t in range(time):
            if t:
                h = a[eight(t), :] * h + b[eight(t), :]
                prod = a[eight(t), :] * prod
            h_s[eight(t), :] = h
            prod_s[eight(t), :] = prod
        for k in (1, 2, 4):
            far = sub >= k
            h = jnp.where(far, h + prod * pltpu.roll(h, k, 0), h)
            prod = jnp.where(far, prod * pltpu.roll(prod, k, 0), prod)
        before = h0_s[:]
        ends = h + prod * before
        carry = jnp.where(sub == 0, before, pltpu.roll(ends, 1, 0))
        h0_s[:] = jnp.broadcast_to(ends[SUB - 1:, :], (SUB, LANES))
        hid = h_s[:].reshape(time, SUB, LANES) + prod_s[:].reshape(time, SUB, LANES) * carry[None]
        return (hid.reshape(CHUNK, LANES) * y.astype(F32)).astype(BF16)

    def project_back(mixed, q, slot):
        acc_s[part_of(q, CHUNK), :] += jnp.dot(mixed, back_tile(slot)[:], preferred_element_type=F32)

    wait(in_tiles(0, 0))
    mix = shuffle_matrix(False)

    @pl.loop(0, steps)
    def _(c):
        @pl.when(lax.rem(c, steps // NX) == 0)
        def _():
            for p in (1, 2, 3):
                x_copy(p, c // (steps // NX)).wait_recv()

        x_load(c)
        rows = part_of(c, CHUNK)
        vals = jnp.dot(mix, x_s[:], preferred_element_type=F32)
        scale = lax.rsqrt(jnp.mean(vals * vals, axis=1, keepdims=True) + EPS)
        n_s[rows, :] = (vals * scale * (1.0 + wide(0))).astype(BF16)
        acc_s[rows, :] = vals + wide(1)
        seq = pl.ds(me // (seg_ref.shape[1] // tokens), 1)
        here = seg_ref[seq, pl.ds(pl.multiple_of(lax.rem(me, seg_ref.shape[1] // tokens) * tokens + c * CHUNK, CHUNK), CHUNK)]
        here = jnp.broadcast_to(here, (ROW, CHUNK))
        high, low = [jnp.einsum('rc,kc->rk', mix, v.astype(F32).astype(BF16), preferred_element_type=F32) for v in (here // 64, here % 64)]
        pos_s[rows, :] = (high * 64.0 + low).astype(jnp.int32)

        @pl.when(c == steps // 2)
        def _():
            by_core(lambda which: gate_over(which).wait_recv())
            by_core(lambda which: gate_on(which).start())

        kept(0, 0, c)[:], kept(1, 0, c)[:] = project(0, c, 0)

    by_core(lambda which: gate_on(which).wait())
    back_tile(1)[:] = jnp.zeros((LANES, model), BF16)

    @pl.loop(0, steps)
    def _(q):
        kept(2, 1, q)[:] = jnp.zeros((CHUNK, LANES), BF16)

    def came(i):
        return jnp.minimum(jnp.maximum(i - 5 - i // 8, 0), 4)

    def pass_on(low, high):
        @pl.loop(low, high)
        def _(b):
            forward(blocks + b, second(b))

            @pl.when(b < 6)
            def _():
                send(blocks + b + 3, second(b + 3), both)

            @pl.when((b > 6) & (b + 2 < groups))
            def _():
                send(blocks + b + 2, second(b + 2), both)

    @pl.loop(0, halves)
    def _(i):
        slot, other = lax.rem(i, 2), lax.rem(i + 1, 2)

        pass_on(came(i + core), came(i + core + 1))

        for g, at in ((1, 0), (2, 2), (3, 4), (4, 6)):
            @pl.when((core == 1) & (i == at))
            def _(g=g):
                if g == 1:
                    forward(g, first(g))
                relay(g, first(g))

        @pl.when((core == 1) & (i == 8))
        def _():
            relay(blocks, second(0))

        for g in range(2, blocks):
            @pl.when(i + core == g - 1)
            def _(g=g):
                forward(g, first(g))
                if g > 2:
                    send(blocks + g - 2, second(g - 2), (OWN_Y, OWN_P))

        @pl.when(i < halves - 1)
        def _():
            wait(in_tiles(i + 1, other))

        @pl.when((lax.rem(i, 2) == 1) & (i < halves - 2))
        def _():
            start(in_tiles(i + 2, slot))

        start(back_tiles(i, slot))

        def middle():
            @pl.when((core == 0) & (i == 8))
            def _():
                relay(blocks, second(0))

        @pl.when(core == 0)
        def _():
            h0_s[:] = jnp.zeros_like(h0_s)
            tail_s[:] = jnp.zeros_like(tail_s)

        @pl.when(core == 1)
        def _():
            message(i).wait_recv()
            tail_s[:] = msg_in[i, :EDGE, :]
            h0_s[:] = msg_in[i, EDGE:, :]

        @pl.loop(0, steps)
        def _(q):
            @pl.when(q == steps // 2)
            def _():
                middle()

            mixed, y, u = kept(2, other, q)[:], kept(0, slot, q)[:], kept(1, slot, q)[:]
            project_back(mixed, q, other)
            c16, sums = gate_sums(i, q, u)
            y_next, u_next = project(i + 1, q, other)
            mixed_next = recur(i, q, y, c16, sums)
            kept(2, slot, q)[:] = mixed_next
            kept(0, other, q)[:] = y_next
            kept(1, other, q)[:] = u_next

        @pl.when(core == 0)
        def _():
            msg_out[i, :EDGE, :] = tail_s[:]
            msg_out[i, EDGE:, :] = h0_s[:]
            message(i).start()

        wait(back_tiles(i, slot))

        for g in range(1, blocks):
            @pl.when(i == 2 * g - 2)
            def _(g=g):
                @pl.when(core == 0)
                def _():
                    if g == 1:
                        forward(g, first(g))
                    relay(g, first(g))

                ready(g, first(g))
                start(in_tiles(i + 2, slot))

    pass_on(4, 5)
    ready(blocks, second(0))
    start(up_tiles(0, 0))

    @pl.loop(0, steps)
    def _(c):
        project_back(kept(2, (halves - 1) % 2, c)[:], c, (halves - 1) % 2)
        rows = part_of(c, CHUNK)
        vals = acc_s[rows, :]
        scale = lax.rsqrt(jnp.mean(vals * vals, axis=1, keepdims=True) + EPS)
        n_s[rows, :] = (vals * scale * (1.0 + wide(2))).astype(BF16)
        acc_s[rows, :] = vals + wide(3)

    def rows_of(i):
        return part_of(i, UP)

    def up(i, slot, b):
        vals = n_s[rows_of(i), :]
        for c in range(NCH):
            part = slice(c * model, (c + 1) * model)
            gate = jnp.dot(vals, t_w[slot, part], preferred_element_type=F32) + inner_row(c, 0, b)
            upper = jnp.dot(vals, t_w[2 + slot, part], preferred_element_type=F32) + inner_row(c, 1, b)
            act_s[c, rows_of(i), cols_of(b)] = (gelu(gate) * upper).astype(BF16)

    def ahead(s):
        return jnp.minimum(5 + s - (s > 5).astype(jnp.int32), groups)

    @pl.loop(0, groups)
    def _(s):
        slot = lax.rem(s, 2)
        pass_on(ahead(s), ahead(s + 1))

        @pl.when(s == 7)
        def _():
            for d in range(DOWN):
                for kind in both:
                    down_piece(kind, d).start()

        wait(up_tiles(s, slot))

        @pl.loop(0, ups)
        def _(i):
            @pl.when((i == 1) & (s + 1 < groups))
            def _():
                relay(blocks + s + 1, second(s + 1))

            @pl.when((i == 3) & (s + 1 < groups))
            def _():
                ready(blocks + s + 1, second(s + 1))
                start(up_tiles(s + 1, 1 - slot))

            up(i, slot, s)

    base = me * tokens

    def col_block(b):
        return lax.rem(wd + lax.rem(b, 2) * (1 - 2 * core) + 2 * (b // 2) + NWD, NWD)

    def wide_cols(b):
        return wide_of(col_block(b))

    def there(q):
        return part_of(q, CHUNK), out.at[pl.ds(base + q * CHUNK, CHUNK)]

    def across(q):
        rows, place = there(q)
        return remote(n_s.at[rows, wide_cols(0)], place, dev_y, fssem.at[0], frsem.at[0, q])

    def keep(q):
        rows, place = there(q)
        return pltpu.make_async_copy(n_s.at[rows, wide_cols(0)], place, olsem.at[q])

    def direct(b, q):
        rows, place = there(q)
        return remote(n_s.at[rows, wide_cols(b)], place, (0, ch, col_block(b)), ossem.at[0], orsem.at[b - 1, q])

    def onward(b, q):
        here = out.at[pl.ds((ch * NWD + col_block(b)) * tokens + q * CHUNK, CHUNK)]
        return remote(here, here, dev_y, fssem.at[0], frsem.at[b, q])

    def load_down(b, p):
        side = lax.rem(ch + p // DOWN, NCH)
        rows = part_of(lax.rem(p, DOWN), deep)
        for half in range(2):
            cols = pl.ds(pl.multiple_of(col_block(b) * width + half * LANES, LANES), LANES)
            buf = t_w.at[p, pl.ds(half * deep, deep)]
            mine = (b == 0) & (p < DOWN)

            @pl.when(mine)
            def _():
                pltpu.make_async_copy(w_d.at[rows, cols_of(half)], buf, osem.at[p, half]).start()

            @pl.when(jnp.logical_not(mine))
            def _():
                pltpu.make_async_copy(g_d.at[side, rows, cols], buf, osem.at[p, half]).start()

    def wait_down(p):
        for half in range(2):
            pltpu.make_async_copy(w_d.at[pl.ds(0, deep), cols_of(half)], t_w.at[p, pl.ds(half * deep, deep)], osem.at[p, half]).wait()

    def down(b, p, i):
        side = lax.rem(ch + p // DOWN, NCH)
        vals = act_s[side, rows_of(i), part_of(lax.rem(p, DOWN), deep)]
        both = [jnp.dot(vals, t_w[p, half * deep:(half + 1) * deep], preferred_element_type=F32) for half in range(2)]
        acc_s[rows_of(i), wide_cols(b)] += jnp.concatenate(both, axis=1)

    def next_piece(b, p):
        d = lax.rem(p, DOWN)
        near = p < DOWN
        for at, kind_near, kind_far in ((0, OWN_P, Y_P), (1, OWN_X, Y_X), (2, X_P, D_P)):
            for kind, here in ((kind_near, near), (kind_far, jnp.logical_not(near))):
                @pl.when((b == at) & here)
                def _(kind=kind):
                    down_piece(kind, d).wait_recv()
                    if kind in (OWN_X, Y_X):
                        down_piece(X_P if kind == OWN_X else D_P, d).start()

        @pl.when(b < NWD - 1)
        def _():
            load_down(b + 1, p)

    def hand_out(b, i):
        back = shuffle_matrix(True)
        for c in range(UP // CHUNK):
            q = i * (UP // CHUNK) + c
            rows = part_of(q, CHUNK)
            n_s[rows, wide_cols(b)] = jnp.dot(back, acc_s[rows, wide_cols(b)].astype(BF16), preferred_element_type=F32).astype(BF16)

            @pl.when(b == 0)
            def _():
                across(q).start()
                keep(q).start()

            @pl.when(b > 0)
            def _():
                direct(b, q).start()

    def pass_results(b, low, high):
        @pl.loop(low, high)
        def _(q):
            direct(b, q).wait_recv()
            onward(b, q).start()

    load_down(0, 0)
    load_down(0, 1)

    @pl.loop(0, NWD)
    def _(b):
        @pl.loop(0, 2 * DOWN)
        def _(p):
            @pl.when((b == 0) & (p >= DOWN))
            def _():
                forward_down(p - DOWN)
                load_down(0, p)

            wait_down(p)

            @pl.loop(0, ups)
            def _(i):
                down(b, p, i)

                @pl.when(p == 2 * DOWN - 1)
                def _():
                    hand_out(b, i)

            @pl.when(b != 1)
            def _():
                next_piece(b, p)

            @pl.when((b == 1) & (p == 2 * DOWN - 1))
            def _():
                pass_results(b, 0, steps)

                @pl.loop(0, p)
                def _(k):
                    next_piece(b, k)

            @pl.when((b == NWD - 1) & (p < DOWN))
            def _():
                pass_results(2, p * 2, p * 2 + 2)

            @pl.when((b == 2) & (p == 2 * DOWN - 2))
            def _():
                next_piece(b - 1, p + 1)

    pass_results(2, 2 * DOWN, steps)
    pass_results(3, 0, steps)
    unit_rows = 7 * LANES
    for g in range(blocks):
        sent(ssem.at[g], unit_rows, 3 * width)

    @pl.loop(0, groups)
    def _(b):
        sent(ssem.at[blocks + b], unit_rows, 2 * width)

    sent(dssem.at[0], NCH, tokens, DOWN * 7 * deep * width // (NCH * tokens))
    sent(xssem.at[0], tokens, 3 * width)
    by_core(lambda which: gate_over(which).wait_send())
    sent(ossem.at[0], tokens, 3 * width)

    @pl.when(core == 0)
    def _():
        @pl.loop(0, halves)
        def _(i):
            message(i).wait_send()

    @pl.loop(0, steps)
    def _(q):
        keep(q).wait()
        across(q).wait_recv()
        for b in range(1, NWD):
            onward(b, q).wait_recv()

    sent(fssem.at[0], tokens, NWD * width)


def put_out(src, dst, buf, isem, osem):
    part = src.shape[0] // SUB
    ins = [pltpu.make_async_copy(src.at[pl.ds(k * part, part)], buf.at[pl.ds(k * part, part)], isem.at[k]) for k in range(SUB)]
    outs = [pltpu.make_async_copy(buf.at[pl.ds(k * part, part)], dst.at[pl.ds(k * part, part)], osem.at[k]) for k in range(SUB)]
    for c in ins:
        c.start()
    for c, d in zip(ins, outs):
        c.wait()
        d.start()
    for d in outs:
        d.wait()


def solution(mesh):
    row_spec = P("dp", "wd")
    specs = (row_spec, P("dp"), P("wd"), P("wd", "ch"), P("ch"), P("wd", "ch"), P("ch"), P(None, "ch"), P("ch"), P("ch"), P("ch"), P("ch"), P("ch"), P("ch"), P("ch", "wd"), P("wd"), P("wd"), P("wd", "ch"), P("ch"), P("wd", "ch"), P("ch"), P("ch", "wd"), P("wd"))

    def local_layer(resid_in, seg_pos, gain_temporal, w_x, bias_x, w_y, bias_y, conv_w, conv_bias, lam_param, rgate_w, rgate_b, igate_w, igate_b, w_o, bias_o, gain_mlp, w_g, bias_g, w_u, bias_u, w_d, bias_d):
        tokens, width = resid_in.shape
        model = width * NWD
        rows = tokens // NDEV
        blocks = w_x.shape[1] // LANES
        groups = w_g.shape[1] // LANES
        total = NCH * blocks
        vectors = (bias_x, bias_y, conv_bias, conv_w, lam_param, rgate_b, igate_b, bias_g, bias_u, gain_temporal, bias_o, gain_mlp, bias_d)
        chan, inner = w_x.shape[1], w_g.shape[1]
        shared = (10 * chan + 2 * inner) // ROW
        lead = -(-shared // SUB) * SUB

        def like(w, by_rows):
            return jax.ShapeDtypeStruct((NCH, w.shape[0] * (1 if by_rows else NWD), w.shape[1] * (NWD if by_rows else 1)), BF16)

        dma = pltpu.SemaphoreType.DMA
        steps = rows // CHUNK
        outs = pl.pallas_call(
            layer,
            out_shape=[jax.ShapeDtypeStruct((tokens, width), BF16), like(w_y, False), like(w_x, False), like(w_o, True), like(w_g, False), like(w_u, False), like(w_d, True),
                       jax.ShapeDtypeStruct((rows, model), BF16)],
            in_specs=[ANY, pl.BlockSpec(memory_space=pltpu.VMEM)] + [ANY] * (8 + len(vectors)),
            out_specs=[ANY] * 8,
            scratch_shapes=[pltpu.VMEM(conv_w.shape, BF16), pltpu.VMEM((chan,), F32), [pltpu.VMEM((chan,), BF16)] * 5, [pltpu.VMEM((inner,), BF16)] * 2, [pltpu.VMEM((width,), BF16)] * 4,
                            pltpu.VMEM((rows, model), BF16), pltpu.VMEM((rows, model), F32),
                            pltpu.VMEM((NCH, rows, w_g.shape[1]), BF16), pltpu.VMEM((4, NCH * model, LANES), BF16),
                            pltpu.VMEM((NCH, lead, ROW), F32), pltpu.VMEM((NWD, 4 * width // ROW, ROW), F32), pltpu.VMEM((rows, ROW), jnp.int32),
                            pltpu.VMEM((CHUNK + EDGE, LANES), F32), pltpu.VMEM((CHUNK, LANES), F32), pltpu.VMEM((CHUNK, LANES), F32),
                            pltpu.VMEM((EDGE, LANES), F32), pltpu.VMEM((SUB, LANES), F32),
                            pltpu.VMEM((total, EDGE + SUB, LANES), F32), pltpu.VMEM((total, EDGE + SUB, LANES), F32),
                            dma((blocks + groups,)), dma((8, blocks, 3)), dma((8, groups, 2)), dma((1,)), dma((8, DOWN)), dma((3, 2, NCH)), dma((2 * DOWN, 2)), dma((len(vectors),)), dma((1,)), dma((3, NX)), dma((6,)), dma((6,)), dma((15,)),
                            dma((total,)), dma((total,)), dma((NWD,)), dma((1,)), dma((3, steps)), dma((1,)), dma((4, steps)), dma((steps,))],
            compiler_params=pltpu.CompilerParams(collective_id=0, has_side_effects=True, vmem_limit_bytes=VMEM_LIMIT),
            name="layer",
        )(resid_in, seg_pos, w_y, w_x, w_o, w_g, w_u, w_d, rgate_w.reshape(-1, LANES), igate_w.reshape(-1, LANES), *vectors)
        return pl.pallas_call(
            put_out, out_shape=jax.ShapeDtypeStruct((tokens, width), BF16), in_specs=[ANY], out_specs=ANY,
            scratch_shapes=[pltpu.VMEM((tokens, width), BF16), dma((SUB,)), dma((SUB,))],
            compiler_params=pltpu.CompilerParams(vmem_limit_bytes=VMEM_LIMIT), name="put_out",
        )(outs[0])

    return jax.shard_map(local_layer, mesh=mesh, in_specs=specs, out_specs=row_spec, check_vma=False)
```
